8 devices in a mesh: dp: 2 (over y, z), sp: 4 (over x, core).
Axes of the slice: x: 2, y: 2, z: 1, core: 2. Of those that a mesh axis runs over, the one named last changes fastest.
Arguments:
- x: bfloat16 [4096, 2048], P(('dp', 'sp')), parts along dimension 0
- gain: bfloat16 [2048], replicated
- wq: bfloat16 [2048, 4096], replicated
- wk: bfloat16 [2048, 2048], replicated
- wv: bfloat16 [2048, 2048], replicated
- wo: bfloat16 [4096, 2048], replicated
Outputs:
- output: bfloat16 [4096, 2048], P(('dp', 'sp')), parts along dimension 0
There are 2 independent parts. The reference program is written for one: setup_inputs(seed, part) draws one part's arguments, and reference() takes and returns one part's arrays. A program takes and returns all parts, laid end to end along the dimension named above; an argument that names none is the same for every part.
All inputs are finite; a program needn't handle non-finite values.
Results may differ from the reference program's by a relative error of at most 0.012.
Values are sent between devices in bfloat16 or wider.
A program may use at most 2 GiB of HBM per device.

```python
import jax
import jax.numpy as jnp
from jax import lax

ROWS = 2048
D = 2048
HEADS = 32
KV_HEADS = 16
HEAD = 128
THETA = 10000


def setup_inputs(seed: int = 0, part: int = 0) -> dict:
    kx, kn, kq, kk, kv, ko = jax.random.split(jax.random.key(seed), 6)

    def weights(key, rows, columns):
        return jax.random.normal(key, (rows, columns), jnp.float32) * rows**-0.5

    drawn = {
        "x": jax.random.normal(jax.random.fold_in(kx, part), (ROWS, D), jnp.float32),
        "gain": 1 + 0.1 * jax.random.normal(kn, (D,), jnp.float32),
        "wq": 2 * weights(kq, D, HEADS * HEAD),
        "wk": 2 * weights(kk, D, KV_HEADS * HEAD),
        "wv": 4 * weights(kv, D, KV_HEADS * HEAD),
        "wo": weights(ko, HEADS * HEAD, D),
    }
    return {k: v.astype(jnp.bfloat16) for k, v in drawn.items()}


def normed(x, gain):
    wide = x.astype(jnp.float32)
    scale = lax.rsqrt(jnp.mean(wide * wide, -1, keepdims=True) + 1e-6)
    return (wide * scale * gain.astype(jnp.float32)).astype(jnp.bfloat16)


def turned(t, place, theta):
    half = t.shape[-1] // 2
    angle = place.astype(jnp.float32)[:, None] * theta ** (-jnp.arange(half, dtype=jnp.float32) / half)
    cos, sin = jnp.cos(angle)[:, None], jnp.sin(angle)[:, None]
    a, b = t[..., :half].astype(jnp.float32), t[..., half:].astype(jnp.float32)
    return jnp.concatenate([a * cos - b * sin, b * cos + a * sin], -1).astype(jnp.bfloat16)


def matmul(a, w):
    return jnp.dot(a, w, preferred_element_type=jnp.float32).astype(jnp.bfloat16)


def einsum(form, a, b):
    return jnp.einsum(form, a.astype(jnp.float32), b.astype(jnp.float32))


def attention(q, k, v):
    scores = einsum("tgsd,ugd->gstu", q, k) * q.shape[-1] ** -0.5
    token = jnp.arange(q.shape[0])
    scores = jnp.where(token[:, None] >= token, scores, -jnp.inf)
    weights = jax.nn.softmax(scores, -1).astype(jnp.bfloat16)
    return einsum("gstu,ugd->tgsd", weights, v).astype(jnp.bfloat16)


def reference(x, gain, wq, wk, wv, wo):
    a, place = normed(x, gain), jnp.arange(ROWS)
    q = turned(matmul(a, wq).reshape(ROWS, HEADS, HEAD), place, THETA).reshape(ROWS, KV_HEADS, -1, HEAD)
    k = turned(matmul(a, wk).reshape(ROWS, KV_HEADS, HEAD), place, THETA)
    v = matmul(a, wv).reshape(ROWS, KV_HEADS, HEAD)
    seen = attention(q, k, v).reshape(ROWS, HEADS * HEAD)
    return (x.astype(jnp.float32) + jnp.dot(seen, wo, preferred_element_type=jnp.float32)).astype(jnp.bfloat16)
```

```python
import functools

import jax
import jax.numpy as jnp
from jax import lax
from jax.experimental import pallas as pl
from jax.experimental.pallas import tpu as pltpu
from jax.sharding import PartitionSpec as P

NEG = -1e30
HIDDEN = 2 * NEG
LOG2E = 1.4426950408889634
VMEM = 60 * 2**20
HEAD = 128
THETA = 10000
COLS = 512


def _dot(a, b, ca, cb):
    return lax.dot_general(a, b, (((ca,), (cb,)), ((), ())), preferred_element_type=jnp.float32)


def _project(pos_ref, a_ref, cos_ref, sin_ref, *rest, steps):
    n = sum(s > 0 for s in steps)
    weights, outs = rest[:n], rest[-n:]
    j = pl.program_id(0)
    heads = COLS // HEAD

    def turned(w_ref):
        t = jnp.dot(a_ref[...], w_ref[...], preferred_element_type=jnp.float32).astype(jnp.bfloat16).astype(jnp.float32)
        for h in range(heads):
            part = t[:, h * HEAD : (h + 1) * HEAD]
            yield h, (part * cos_ref[...] + pltpu.roll(part, HEAD // 2, 1) * sin_ref[...]).astype(jnp.bfloat16)

    sq, sk, sv = steps
    if sq:

        @pl.when(j < sq)
        def _():
            for h, t in turned(weights[0]):
                outs[0][h // 2, h % 2] = t

    @pl.when((j >= sq) & (j < sq + sk))
    def _():
        for h, t in turned(weights[-2]):
            outs[-2][h] = t

    @pl.when(j >= sq + sk)
    def _():
        t = jnp.dot(a_ref[...], weights[-1][...], preferred_element_type=jnp.float32).astype(jnp.bfloat16)
        for h in range(heads):
            outs[-1][h] = t[:, h * HEAD : (h + 1) * HEAD].T


def project(a, tables, core, half, wq, wk, wv, into=None):
    rows, depth = a.shape
    tokens = 2 * rows
    ws = [w for w in (wq, wk, wv) if w is not None]
    steps = (0 if wq is None else wq.shape[1] // 2 // COLS, wk.shape[1] // 2 // COLS, wv.shape[1] // 2 // COLS)
    starts = (0, steps[0], steps[0] + steps[1])
    heads = COLS // HEAD
    kv = wk.shape[1] // 2 // HEAD

    def at(i):
        return lambda j: jnp.clip(j - starts[i], 0, steps[i] - 1)

    idx = [i for i in range(3) if steps[i]]
    specs = [pl.BlockSpec((rows, depth), lambda j, p: (0, 0)), *[pl.BlockSpec((rows, HEAD), lambda j, p: (0, 0))] * 2]
    specs += [pl.BlockSpec((depth, COLS), lambda j, p, i=i: (0, p[0] * steps[i] + at(i)(j))) for i in idx]
    out_specs = [
        pl.BlockSpec((heads // 2, 2, rows, HEAD), lambda j, p: (at(0)(j), 0, p[1], 0)),
        pl.BlockSpec((heads, rows, HEAD), lambda j, p: (at(1)(j), p[1], 0)),
        pl.BlockSpec((heads, HEAD, rows), lambda j, p: (at(2)(j), 0, p[1])),
    ]
    shapes = [(kv, 2, tokens, HEAD), (kv, tokens, HEAD), (kv, HEAD, tokens)]
    args = [a, *tables, *ws]
    aliases = {}
    if into is not None:
        aliases = {1 + len(args) + n: n for n in range(len(idx))}
        args += into
        specs += [pl.BlockSpec(memory_space=pl.ANY)] * len(idx)
    cols = sum(steps) * COLS
    return pl.pallas_call(
        functools.partial(_project, steps=steps),
        grid_spec=pltpu.PrefetchScalarGridSpec(
            num_scalar_prefetch=1, grid=(sum(steps),), in_specs=specs, out_specs=[out_specs[i] for i in idx]
        ),
        out_shape=[jax.ShapeDtypeStruct(shapes[i], a.dtype) for i in idx],
        input_output_aliases=aliases,
        compiler_params=pltpu.CompilerParams(dimension_semantics=("arbitrary",), vmem_limit_bytes=VMEM),
        cost_estimate=pl.CostEstimate(flops=2 * rows * depth * cols, transcendentals=0, bytes_accessed=2 * depth * cols + 4 * rows * depth),
        name="project_q" if steps[0] else "project_kv",
    )(jnp.stack([core, half]).astype(jnp.int32), *args)


def _attend(pos_ref, q_ref, k_ref, v_ref, *rest, causal, scale, bk, carried, final):
    top_in, mix_in = rest[:2] if carried else (None, None)
    outs = rest[2 * carried : 2 * carried + (1 if final else 2)]
    top_s, mix_s = rest[-2:] if final else outs
    kb, g, bq, d = q_ref.shape
    cols = g * bq
    iq = pl.program_id(0)
    e = scale * LOG2E

    if carried:
        top_s[...] = top_in[...]
        mix_s[...] = mix_in[...]
    else:
        top_s[...] = jnp.full_like(top_s, NEG)
        mix_s[...] = jnp.zeros_like(mix_s)

    ones = jnp.ones((8, bk), k_ref.dtype)
    gap = lax.rem(lax.broadcasted_iota(jnp.int32, (bk, cols), 1), bq) - lax.broadcasted_iota(jnp.int32, (bk, cols), 0)

    def block(j, masked):
        here = pl.ds(pl.multiple_of(j * bk, bk), bk)
        scores = [_dot(k_ref[i, here, :], q_ref[i].reshape(cols, d), 1, 1) for i in range(kb)]
        weights, keeps = [], []
        for i, s in enumerate(scores):
            if masked:
                s = jnp.where(gap >= j * bk - iq * bq, s, HIDDEN)
            old = top_s[0, i : i + 1, :]
            top = jnp.maximum(old, s.max(axis=0, keepdims=True))
            top_s[0, i : i + 1, :] = top
            weights.append(jnp.exp2((s - top) * e).astype(k_ref.dtype))
            keeps.append(jnp.exp2((old - top) * e))
        for i, (p, keep) in enumerate(zip(weights, keeps)):
            values = jnp.concatenate([v_ref[i, :, here], ones], axis=0)
            mix_s[0, i] = mix_s[0, i] * keep + _dot(values, p, 1, 0)

    if causal:
        whole, last = lax.div(iq * bq, bk), lax.div(iq * bq + bq - 1, bk) + 1
        lax.fori_loop(0, whole, lambda j, _: block(j, False), None)
        lax.fori_loop(whole, last, lambda j, _: block(j, True), None)
    else:
        lax.fori_loop(0, lax.div(pos_ref[1], bk), lambda j, _: block(j, False), None)

    if final:
        for i in range(kb):
            out = (mix_s[0, i, :d, :] * (1 / mix_s[0, i, d : d + 1, :])).T
            for n in range(g):
                outs[0][:, (i * g + n) * d : (i * g + n + 1) * d] = out[n * bq : (n + 1) * bq, :].astype(outs[0].dtype)


def attend(q, k, v, pos, *, causal, state=None, rows=None, bq=256, bk=512):
    kv, g, tokens, d = q.shape
    keys = k.shape[1]
    blocks = (rows or tokens) // bq
    final = rows is not None
    whole = lambda *shape: pl.BlockSpec(shape, lambda iq, p: (0,) * len(shape))
    specs = [pl.BlockSpec((kv, g, bq, d), lambda iq, p: (0, 0, p[0] + iq, 0)), whole(kv, keys, d), whole(kv, d, keys)]
    args = [q, k, v]
    shapes = [(tokens // bq, kv, g * bq), (tokens // bq, kv, d + 8, g * bq)]
    if state is not None:
        args += state
        specs += [pl.BlockSpec((1, *shapes[0][1:]), lambda iq, p: (p[0] + iq, 0, 0)), pl.BlockSpec((1, *shapes[1][1:]), lambda iq, p: (p[0] + iq, 0, 0, 0))]
    if final:
        out_specs = [pl.BlockSpec((bq, kv * g * d), lambda iq, p: (iq, 0))]
        out_shape = [jax.ShapeDtypeStruct((rows, kv * g * d), q.dtype)]
        scratch = [pltpu.VMEM((1, *s[1:]), jnp.float32) for s in shapes]
    else:
        out_specs = [pl.BlockSpec((1, *shapes[0][1:]), lambda iq, p: (iq, 0, 0)), pl.BlockSpec((1, *shapes[1][1:]), lambda iq, p: (iq, 0, 0, 0))]
        out_shape = [jax.ShapeDtypeStruct(s, jnp.float32) for s in shapes]
        scratch = []
    work = kv * g * blocks * bq * keys // (2 if causal else 1)
    got = pl.pallas_call(
        functools.partial(_attend, causal=causal, scale=d**-0.5, bk=bk, carried=state is not None, final=final),
        grid_spec=pltpu.PrefetchScalarGridSpec(num_scalar_prefetch=1, grid=(blocks,), in_specs=specs, out_specs=out_specs, scratch_shapes=scratch),
        out_shape=out_shape,
        compiler_params=pltpu.CompilerParams(dimension_semantics=("arbitrary",), vmem_limit_bytes=VMEM),
        cost_estimate=pl.CostEstimate(flops=8 * work * d, transcendentals=work, bytes_accessed=4 * k.size),
        name="attend_end" if final else "attend",
    )(jnp.stack(pos).astype(jnp.int32), *args)
    return got[0] if final else got


def _output(pos_ref, x_ref, own_ref, other_ref, w_own, w_other, y_ref):
    y = jnp.dot(own_ref[...], w_own[...], preferred_element_type=jnp.float32)
    y += jnp.dot(other_ref[...], w_other[...], preferred_element_type=jnp.float32)
    y_ref[...] = (x_ref[...].astype(jnp.float32) + y).astype(y_ref.dtype)


def output(x, own, other, wo, core, cols=512):
    rows, depth = own.shape
    width = wo.shape[1]
    block = pl.BlockSpec((rows, cols), lambda j, p: (0, j))
    whole = pl.BlockSpec((rows, depth), lambda j, p: (0, 0))
    return pl.pallas_call(
        _output,
        grid_spec=pltpu.PrefetchScalarGridSpec(
            num_scalar_prefetch=1,
            grid=(width // cols,),
            in_specs=[block, whole, whole, pl.BlockSpec((depth, cols), lambda j, p: (p[0], j)), pl.BlockSpec((depth, cols), lambda j, p: (1 - p[0], j))],
            out_specs=block,
        ),
        out_shape=jax.ShapeDtypeStruct(x.shape, x.dtype),
        compiler_params=pltpu.CompilerParams(dimension_semantics=("arbitrary",), vmem_limit_bytes=VMEM),
        cost_estimate=pl.CostEstimate(flops=4 * rows * depth * width, transcendentals=0, bytes_accessed=4 * depth * width),
        name="output",
    )(core[None].astype(jnp.int32), x, own, other, wo, wo)


def normed(x, gain):
    wide = x.astype(jnp.float32)
    scale = lax.rsqrt(jnp.mean(wide * wide, -1, keepdims=True) + 1e-6)
    return (wide * scale * gain.astype(jnp.float32)).astype(jnp.bfloat16)


def tables(first, rows):
    half = HEAD // 2
    angle = (first + jnp.arange(rows)).astype(jnp.float32)[:, None] * THETA ** (-jnp.arange(half, dtype=jnp.float32) / half)
    cos, sin = jnp.cos(angle), jnp.sin(angle)
    return jnp.concatenate([cos, cos], -1), jnp.concatenate([-sin, sin], -1)


SWAP = [(0, 1), (1, 0), (2, 3), (3, 2)]


def solution(mesh):
    def step(x, gain, wq, wk, wv, wo):
        rows = x.shape[0]
        sp = lax.axis_index("sp")
        core, late = lax.rem(sp, 2), lax.div(sp, 2)
        a = normed(x, gain)
        far_own = lax.ppermute(a, "sp", [(0, 2), (1, 3)])
        a_other = lax.ppermute(a, "sp", SWAP)
        far_other = lax.ppermute(far_own, "sp", SWAP)
        here = late * 2 * rows
        local = project(a, tables(here + core * rows, rows), core, core, wq, wk, wv)
        q, k, v = project(a_other, tables(here + (1 - core) * rows, rows), core, 1 - core, wq, wk, wv, local)
        state = attend(q, k, v, (0 * core, 0 * core), causal=True, bk=256)
        far = project(far_own, tables(core * rows, rows), core, core, None, wk, wv)
        fk, fv = project(far_other, tables((1 - core) * rows, rows), core, 1 - core, None, wk, wv, far)
        blocks = rows // 256
        given = attend(q, fk, fv, ((1 - core) * blocks, late * 2 * rows), causal=False, state=state, rows=rows)
        got = lax.ppermute(given, "sp", SWAP)
        kept = attend(q, fk, fv, (core * blocks, late * 2 * rows), causal=False, state=state, rows=rows)
        return output(x, kept, got, wo, core)

    tokens, whole = P(("dp", "sp"), None), P(None, None)
    return jax.shard_map(
        step,
        mesh=mesh,
        in_specs=(tokens, P(None), whole, whole, whole, whole),
        out_specs=tokens,
        check_vma=False,
    )
```

```python
import functools

import jax
import jax.numpy as jnp
import numpy as np
from jax import lax
from jax.experimental import pallas as pl
from jax.experimental.pallas import tpu as pltpu
from jax.sharding import PartitionSpec as P

NEG = -1e30
HIDDEN = 2 * NEG
LOG2E = 1.4426950408889634
VMEM = 63 * 2**20
HEAD = 128
THETA = 10000

ROWS = 512
CHIP = 1024
DEPTH = 2048
COLS = 512
KV = 8
GROUP = 2
BQ = 256
BK = 512
AT_ONCE = 4
PIECE = 128
SLOTS = 7

MESH = pl.DeviceIdType.MESH


def _dot(a, b, ca, cb):
    return lax.dot_general(a, b, (((ca,), (cb,)), ((), ())), preferred_element_type=jnp.float32)


def _rows(start, size):
    return pl.ds(pl.multiple_of(start, size), size)


def _kernel(x, gain, table, wq, wk, wv, wo, y, a_loc, a_far, qk, v, fk, fv, top, mix, wbuf, xbuf, tab, ybuf,
            x_sem, tab_sem, w_sem, y_sem, swap_out, swap_in, far_out, far_in, pass_out, pass_in, seen_out, seen_in, ready):
    sp = lax.axis_index("sp")
    core, chip = lax.rem(sp, 2), lax.div(sp, 2)
    late = chip == 1
    partner, across = {"sp": chip * 2 + 1 - core}, {"sp": (1 - chip) * 2 + core}
    mine, theirs = core * ROWS, (1 - core) * ROWS
    kv_cols = KV * HEAD
    q_cols = GROUP * kv_cols

    def x_copy(r):
        return pltpu.make_async_copy(x.at[pl.ds(r * PIECE, PIECE)], xbuf.at[pl.ds(r * PIECE, PIECE)], x_sem.at[r])

    def w_copy(w, row, column, slot):
        return pltpu.make_async_copy(w.at[_rows(row, DEPTH), _rows(column, COLS)], wbuf.at[slot], w_sem.at[slot])

    def q_copy(c):
        return w_copy(wq, 0, core * q_cols + c * COLS, 4 + c % 3)

    def o_copy(u):
        return w_copy(wo, (core if u % 2 == 0 else 1 - core) * DEPTH, u // 2 * COLS, (5 + u) % SLOTS)

    def w_wait(slot):
        pltpu.make_async_copy(wq.at[pl.ds(0, DEPTH), pl.ds(0, COLS)], wbuf.at[slot], w_sem.at[slot]).wait()

    def remote(src, dst, out, got, device):
        return pltpu.make_async_remote_copy(src_ref=src, dst_ref=dst, send_sem=out, recv_sem=got, device_id=device, device_id_type=MESH)

    def swap(r):
        rows = a_loc.at[_rows(mine + r * PIECE, PIECE)]
        return remote(rows, rows, swap_out.at[r], swap_in.at[r], partner)

    def far_rows(c, r):
        return a_far.at[_rows(r // 2 * ROWS + c * BQ + r % 2 * PIECE, PIECE)]

    def far(r):
        return remote(a_loc.at[_rows(mine + r * PIECE, PIECE)], far_rows(core, r), far_out.at[r], far_in.at[r], across)

    def hand(r):
        return remote(far_rows(core, r), far_rows(core, r), pass_out.at[r], pass_in.at[r], partner)

    def seen(i):
        return remote(a_loc.at[_rows(theirs + i * BQ, BQ)], a_far.at[pl.ds(i * BQ, BQ)], seen_out.at[i], seen_in.at[i], partner)

    def y_copy(n):
        return pltpu.make_async_copy(ybuf.at[lax.rem(n, 2)], y.at[:, _rows(n * COLS, COLS)], y_sem.at[lax.rem(n, 2)])

    for r in range(4):
        x_copy(r).start()
    table_copy = pltpu.make_async_copy(table, tab, tab_sem)
    table_copy.start()
    for c in range(3):
        q_copy(c).start()
    for c in range(2):
        w_copy(wk, 0, core * kv_cols + c * COLS, c).start()
    for c in range(2):
        w_copy(wv, 0, core * kv_cols + c * COLS, 2 + c).start()

    barrier = pltpu.get_barrier_semaphore()
    for device in (partner, across):
        pl.semaphore_signal(barrier, inc=1, device_id=device, device_id_type=MESH)
    pl.semaphore_wait(barrier, 2)

    def send(r):
        swap(r).start()

        @pl.when(chip == 0)
        def _():
            far(r).start()

    for r in range(4):
        x_copy(r).wait()
        wide = xbuf[r * PIECE : (r + 1) * PIECE, :].astype(jnp.float32)
        scale = lax.rsqrt(jnp.mean(wide * wide, -1, keepdims=True) + 1e-6)
        a_loc[_rows(mine + r * PIECE, PIECE), :] = (wide * scale * gain[...].astype(jnp.float32)).astype(a_loc.dtype)
        if r:
            send(r - 1)
    table_copy.wait()
    send(3)
    for r in range(4):
        swap(r).wait_recv()

    def turned(t, place):
        rows = t.shape[0]
        both = tab[_rows(place, rows), :]
        back = pltpu.roll(both, HEAD // 2, 1)
        first = lax.broadcasted_iota(jnp.int32, both.shape, 1) < HEAD // 2
        cos, sin = jnp.where(first, both, back), jnp.where(first, -back, both)
        t = t.astype(qk.dtype).astype(jnp.float32)
        for h in range(COLS // HEAD):
            part = t[:, h * HEAD : (h + 1) * HEAD]
            yield h, (part * cos + pltpu.roll(part, HEAD // 2, 1) * sin).astype(qk.dtype)

    def project(a, row, slot):
        return jnp.dot(a[_rows(row, BQ), :], wbuf[slot], preferred_element_type=jnp.float32)

    def project_v(out, c, a, row):
        t = project(a, row, 2 + c).astype(out.dtype)
        for h in range(COLS // HEAD):
            out[c * 4 + h, :, _rows(row, BQ)] = t[:, h * HEAD : (h + 1) * HEAD].T

    def local_qk(c, _):
        slot = jnp.where(c < 4, 4 + lax.rem(c, 3), c - 4)
        w_wait(slot)
        for b in range(CHIP // BQ):
            for h, t in turned(project(a_loc, b * BQ, slot), chip * CHIP + b * BQ):
                qk[c * 4 + h, b * BQ : (b + 1) * BQ, :] = t
        for at, copy in enumerate((q_copy(3), o_copy(0), o_copy(1), o_copy(6))):
            pl.when(c == at)(copy.start)

    lax.fori_loop(0, 6, local_qk, None)

    def local_v(c, _):
        w_wait(2 + c)
        for b in range(CHIP // BQ):
            project_v(v, c, a_loc, b * BQ)

    lax.fori_loop(0, 2, local_v, None)

    e = HEAD**-0.5 * LOG2E
    cols = GROUP * BQ

    def block(iq, keys, values, k0, at, size, ahead=None):
        here, queries = _rows(at, size), _rows(iq * BQ, BQ)
        ones = jnp.ones((8, size), values.dtype)
        if ahead is not None:
            ok = lax.rem(lax.broadcasted_iota(jnp.int32, (size, cols), 1), BQ) + ahead >= lax.broadcasted_iota(jnp.int32, (size, cols), 0)

        def some(hb, _):
            heads = [hb * AT_ONCE + i for i in range(AT_ONCE)]
            scores = [_dot(keys[k0 + h, here, :], qk[pl.ds(GROUP * h, GROUP), queries, :].reshape(cols, HEAD), 1, 1) for h in heads]
            weights, keeps = [], []
            for h, s in zip(heads, scores):
                if ahead is not None:
                    s = jnp.where(ok, s, HIDDEN)
                old = top[iq, pl.ds(h, 1), :]
                new = jnp.maximum(old, s.max(axis=0, keepdims=True))
                top[iq, pl.ds(h, 1), :] = new
                weights.append(jnp.exp2((s - new) * e).astype(values.dtype))
                keeps.append(jnp.exp2((old - new) * e))
            for h, p, keep in zip(heads, weights, keeps):
                mix[iq, h] = mix[iq, h] * keep + _dot(jnp.concatenate([values[h, :, here], ones], axis=0), p, 1, 0)

        lax.fori_loop(0, KV // AT_ONCE, some, None)

    def hand_on(r):
        @pl.when(late)
        def _():
            far(r).wait_recv()
            hand(r).start()

    top[...] = jnp.full_like(top, NEG)
    mix[...] = jnp.zeros_like(mix)
    hand_on(0)

    def local(p, _):
        for odd in range(2):
            iq = 2 * p + odd
            lax.fori_loop(0, p, lambda j, _: block(iq, qk, v, 2 * KV, j * BK, BK), None)
            block(iq, qk, v, 2 * KV, p * BK, BQ * (1 + odd), odd * BQ)
        pl.when(p == 0)(lambda: hand_on(1))
        pl.when(p == 1)(lambda: hand_on(2))

    lax.fori_loop(0, 2, local, None)

    def order(i):
        return lax.rem((1 - core) * 2 + i, 4)

    def far_project(h):
        for r in (0, 1):
            hand(2 * h + r).wait_recv()

        def k_step(c, _):
            for b in range(2):
                for n, t in turned(project(a_far, h * ROWS + b * BQ, c), b * ROWS + h * BQ):
                    fk[c * 4 + n, h * ROWS + b * BQ : h * ROWS + (b + 1) * BQ, :] = t

        def v_step(c, _):
            for b in range(2):
                project_v(fv, c, a_far, h * ROWS + b * BQ)

        lax.fori_loop(0, 2, k_step, None)
        lax.fori_loop(0, 2, v_step, None)

    @pl.when(late)
    def _():
        far_project(0)

        def first(i, _):
            block(order(i), fk, fv, 0, 0, BK)
            pl.when(i == 1)(lambda: hand_on(3))

        lax.fori_loop(0, 4, first, None)
        far_project(1)
        for r in range(4):
            hand(r).wait_send()

    for u in range(2, 6):
        o_copy(u).start()
    pl.semaphore_signal(ready, inc=1, device_id=partner, device_id_type=MESH)
    for r in range(4):
        swap(r).wait_send()
        pl.when(chip == 0)(far(r).wait_send)

    def last(i, _):
        iq = order(i)
        pl.when(late)(lambda: block(iq, fk, fv, 0, BK, BK))
        for h in range(KV):
            out = (mix[iq, h, :HEAD, :] * (1 / mix[iq, h, HEAD : HEAD + 1, :])).astype(a_loc.dtype).T
            for n in range(GROUP):
                a_loc[_rows(iq * BQ, BQ), (GROUP * h + n) * HEAD : (GROUP * h + n + 1) * HEAD] = out[n * BQ : (n + 1) * BQ, :]

        @pl.when(i == 1)
        def _():
            pl.semaphore_wait(ready, 1)
            seen(0).start()

        pl.when(i == 2)(seen(1).start)

    lax.fori_loop(0, 4, last, None)

    for i in range(2):
        seen(i).wait_recv()

    def output(n, _):
        slots = [lax.rem(5 + 2 * n + i, SLOTS) for i in range(2)]
        for slot in slots:
            w_wait(slot)
        pl.when(n >= 2)(y_copy(n).wait)
        for b in range(ROWS // BQ):
            rows = slice(b * BQ, (b + 1) * BQ)
            t = project(a_loc, mine + b * BQ, slots[0]) + project(a_far, b * BQ, slots[1])
            ybuf[lax.rem(n, 2), rows, :] = (xbuf[rows, _rows(n * COLS, COLS)].astype(jnp.float32) + t).astype(ybuf.dtype)
        y_copy(n).start()
        pl.when(n == 0)(o_copy(7).start)

    lax.fori_loop(0, 4, output, None)
    for n in (2, 3):
        y_copy(n).wait()
    for i in range(2):
        seen(i).wait_send()


def rotary():
    half = HEAD // 2
    places = np.arange(2 * CHIP, dtype=np.float32)
    angle = places[:, None] * (np.float32(THETA) ** (-np.arange(half, dtype=np.float32) / np.float32(half)))
    return np.concatenate([np.cos(angle.astype(np.float64)), np.sin(angle.astype(np.float64))], -1).astype(np.float32)


def solution(mesh):
    def step(x, gain, wq, wk, wv, wo):
        bf, f32 = jnp.bfloat16, jnp.float32
        dma = pltpu.SemaphoreType.DMA
        hbm = pl.BlockSpec(memory_space=pl.ANY)
        return pl.pallas_call(
            _kernel,
            out_shape=jax.ShapeDtypeStruct(x.shape, x.dtype),
            in_specs=[hbm, pl.BlockSpec(memory_space=pltpu.VMEM), *[hbm] * 5],
            out_specs=hbm,
            scratch_shapes=[
                pltpu.VMEM((CHIP, DEPTH), bf),
                pltpu.VMEM((CHIP, DEPTH), bf),
                pltpu.VMEM((3 * KV, CHIP, HEAD), bf),
                pltpu.VMEM((KV, HEAD, CHIP), bf),
                pltpu.VMEM((KV, CHIP, HEAD), bf),
                pltpu.VMEM((KV, HEAD, CHIP), bf),
                pltpu.VMEM((CHIP // BQ, KV, GROUP * BQ), f32),
                pltpu.VMEM((CHIP // BQ, KV, HEAD + 8, GROUP * BQ), f32),
                pltpu.VMEM((SLOTS, DEPTH, COLS), bf),
                pltpu.VMEM((ROWS, DEPTH), bf),
                pltpu.VMEM((2 * CHIP, HEAD), f32),
                pltpu.VMEM((2, ROWS, COLS), bf),
                dma((4,)), dma, dma((SLOTS,)), dma((2,)),
                *[dma((4,))] * 6, dma((2,)), dma((2,)),
                pltpu.SemaphoreType.REGULAR,
            ],
            compiler_params=pltpu.CompilerParams(collective_id=0, has_side_effects=True, vmem_limit_bytes=VMEM),
            name="layer",
        )(x, gain[None], jnp.asarray(rotary()), wq, wk, wv, wo)

    tokens, whole = P(("dp", "sp"), None), P(None, None)
    return jax.shard_map(
        step,
        mesh=mesh,
        in_specs=(tokens, P(None), whole, whole, whole, whole),
        out_specs=tokens,
        check_vma=False,
    )
```

```python
import functools

import jax
import jax.numpy as jnp
import numpy as np
from jax import lax
from jax.experimental import pallas as pl
from jax.experimental.pallas import tpu as pltpu
from jax.sharding import PartitionSpec as P

HIDDEN = -jnp.inf
LOG2E = 1.4426950408889634
VMEM = 63 * 2**20
HEAD = 128
THETA = 10000

ROWS = 512
CHIP = 1024
DEPTH = 2048
COLS = 512
KV = 8
GROUP = 2
BQ = 256
BK = 512
AT_ONCE = 4
PIECE = 128
SLOTS = 7

MESH = pl.DeviceIdType.MESH


def _dot(a, b, ca, cb):
    return lax.dot_general(a, b, (((ca,), (cb,)), ((), ())), preferred_element_type=jnp.float32)


def _rows(start, size):
    return pl.ds(pl.multiple_of(start, size), size)


def _kernel(x, gain, table, wq, wk, wv, wo, y, a_loc, a_far, qk, v, fk, fv, top, mix, wbuf, xbuf, tab, ybuf,
            x_sem, tab_sem, w_sem, y_sem, swap_out, swap_in, far_out, far_in, pass_out, pass_in, seen_out, seen_in, ready):
    sp = lax.axis_index("sp")
    core, chip = lax.rem(sp, 2), lax.div(sp, 2)
    late = chip == 1
    partner, across = {"sp": chip * 2 + 1 - core}, {"sp": (1 - chip) * 2 + core}
    mine, theirs = core * ROWS, (1 - core) * ROWS
    kv_cols = KV * HEAD
    q_cols = GROUP * kv_cols

    def x_copy(r):
        return pltpu.make_async_copy(x.at[pl.ds(r * PIECE, PIECE)], xbuf.at[pl.ds(r * PIECE, PIECE)], x_sem.at[r])

    def w_copy(w, row, column, slot):
        return pltpu.make_async_copy(w.at[_rows(row, DEPTH), _rows(column, COLS)], wbuf.at[slot], w_sem.at[slot])

    def q_copy(c):
        return w_copy(wq, 0, core * q_cols + c * COLS, 4 + c % 3)

    def o_copy(u):
        return w_copy(wo, (core if u % 2 == 0 else 1 - core) * DEPTH, u // 2 * COLS, (5 + u) % SLOTS)

    def w_wait(slot):
        pltpu.make_async_copy(wq.at[pl.ds(0, DEPTH), pl.ds(0, COLS)], wbuf.at[slot], w_sem.at[slot]).wait()

    def remote(src, dst, out, got, device):
        return pltpu.make_async_remote_copy(src_ref=src, dst_ref=dst, send_sem=out, recv_sem=got, device_id=device, device_id_type=MESH)

    def swap(r):
        rows = a_loc.at[_rows(mine + r * PIECE, PIECE)]
        return remote(rows, rows, swap_out.at[r], swap_in.at[r], partner)

    def far_rows(c, r):
        return a_far.at[_rows(r // 2 * ROWS + c * BQ + r % 2 * PIECE, PIECE)]

    def far(r):
        return remote(a_loc.at[_rows(mine + r * PIECE, PIECE)], far_rows(core, r), far_out.at[r], far_in.at[r], across)

    def hand(r):
        return remote(far_rows(core, r), far_rows(core, r), pass_out.at[r], pass_in.at[r], partner)

    def seen(i):
        return remote(a_loc.at[_rows(theirs + i * BQ, BQ)], a_far.at[pl.ds(i * BQ, BQ)], seen_out.at[i], seen_in.at[i], partner)

    def y_copy(n):
        return pltpu.make_async_copy(ybuf.at[lax.rem(n, 2)], y.at[:, _rows(n * COLS, COLS)], y_sem.at[lax.rem(n, 2)])

    for r in range(4):
        x_copy(r).start()
    table_copy = pltpu.make_async_copy(table, tab, tab_sem)
    table_copy.start()

    barrier = pltpu.get_barrier_semaphore()
    for device in (partner, across):
        pl.semaphore_signal(barrier, inc=1, device_id=device, device_id_type=MESH)
    pl.semaphore_wait(barrier, 2)

    def send(r):
        swap(r).start()

        @pl.when(chip == 0)
        def _():
            far(r).start()

    for r in range(4):
        x_copy(r).wait()
        if r == 1:
            q_copy(0).start()
        if r == 3:
            for c in (1, 2):
                q_copy(c).start()
            for c in range(2):
                w_copy(wk, 0, core * kv_cols + c * COLS, c).start()
            for c in range(2):
                w_copy(wv, 0, core * kv_cols + c * COLS, 2 + c).start()
        wide = xbuf[r * PIECE : (r + 1) * PIECE, :].astype(jnp.float32)
        scale = lax.rsqrt(jnp.mean(wide * wide, -1, keepdims=True) + 1e-6)
        a_loc[_rows(mine + r * PIECE, PIECE), :] = (wide * scale * gain[...].astype(jnp.float32)[None, :]).astype(a_loc.dtype)
        if r:
            send(r - 1)
    table_copy.wait()
    send(3)

    def turned(t, place):
        rows = t.shape[0]
        both = tab[_rows(place, rows), :]
        back = pltpu.roll(both, HEAD // 2, 1)
        first = lax.broadcasted_iota(jnp.int32, both.shape, 1) < HEAD // 2
        cos, sin = jnp.where(first, both, back), jnp.where(first, -back, both)
        t = t.astype(qk.dtype).astype(jnp.float32)
        for h in range(COLS // HEAD):
            part = t[:, h * HEAD : (h + 1) * HEAD]
            yield h, (part * cos + pltpu.roll(part, HEAD // 2, 1) * sin).astype(qk.dtype)

    def project(a, row, slot):
        return jnp.dot(a[_rows(row, BQ), :], wbuf[slot], preferred_element_type=jnp.float32)

    def project_v(out, c, a, row):
        t = project(a, row, 2 + c).astype(out.dtype)
        for h in range(COLS // HEAD):
            out[c * 4 + h, :, _rows(row, BQ)] = t[:, h * HEAD : (h + 1) * HEAD].T

    def local_qk(c, slot, parts):
        for row in parts:
            for h, t in turned(project(a_loc, row, slot), chip * CHIP + row):
                qk[c * 4 + h, _rows(row, BQ), :] = t

    w_wait(4)
    local_qk(0, 4, (mine, mine + BQ))
    for r in range(4):
        swap(r).wait_recv()
    local_qk(0, 4, (theirs, theirs + BQ))
    q_copy(3).start()

    def more_qk(c, _):
        slot = jnp.where(c < 4, 4 + lax.rem(c, 3), c - 4)
        w_wait(slot)
        local_qk(c, slot, range(0, CHIP, BQ))
        for at, copy in ((1, o_copy(0)), (2, o_copy(1)), (3, o_copy(6))):
            pl.when(c == at)(copy.start)

    lax.fori_loop(1, 6, more_qk, None)

    def local_v(c, _):
        w_wait(2 + c)
        for b in range(CHIP // BQ):
            project_v(v, c, a_loc, b * BQ)

    lax.fori_loop(0, 2, local_v, None)

    e = HEAD**-0.5 * LOG2E
    cols = GROUP * BQ

    def block(iq, keys, values, k0, at, size, ahead=None):
        begin = ahead is not None
        here, queries = _rows(at, size), _rows(iq * BQ, BQ)
        ones = jnp.ones((8, size), values.dtype)
        if begin:
            ok = lax.rem(lax.broadcasted_iota(jnp.int32, (size, cols), 1), BQ) + ahead >= lax.broadcasted_iota(jnp.int32, (size, cols), 0)

        def some(hb, _):
            heads = [hb * AT_ONCE + i for i in range(AT_ONCE)]
            scores = [_dot(keys[k0 + h, here, :], qk[pl.ds(GROUP * h, GROUP), queries, :].reshape(cols, HEAD), 1, 1) for h in heads]
            weights, keeps = [], []
            for h, s in zip(heads, scores):
                if begin:
                    s = jnp.where(ok, s, HIDDEN)
                    new = s.max(axis=0, keepdims=True)
                else:
                    old = top[iq, pl.ds(h, 1), :]
                    new = jnp.maximum(old, s.max(axis=0, keepdims=True))
                    keeps.append(jnp.exp2((old - new) * e))
                top[iq, pl.ds(h, 1), :] = new
                weights.append(jnp.exp2((s - new) * e).astype(values.dtype))
            for i, (h, p) in enumerate(zip(heads, weights)):
                got = _dot(jnp.concatenate([values[h, :, here], ones], axis=0), p, 1, 0)
                mix[iq, h] = got if begin else mix[iq, h] * keeps[i] + got

        lax.fori_loop(0, KV // AT_ONCE, some, None)

    def hand_on(r):
        @pl.when(late)
        def _():
            far(r).wait_recv()
            hand(r).start()

    hand_on(0)

    def local(p, _):
        for odd in range(2):
            iq = 2 * p + odd
            block(iq, qk, v, 2 * KV, p * BK, BQ * (1 + odd), odd * BQ)
            lax.fori_loop(0, p, lambda j, _: block(iq, qk, v, 2 * KV, j * BK, BK), None)
        pl.when(p == 0)(lambda: hand_on(1))
        pl.when(p == 1)(lambda: hand_on(2))

    lax.fori_loop(0, 2, local, None)

    def order(i):
        return lax.rem((1 - core) * 2 + i, 4)

    def far_project(h):
        for r in (0, 1):
            hand(2 * h + r).wait_recv()

        def k_step(c, _):
            for b in range(2):
                for n, t in turned(project(a_far, h * ROWS + b * BQ, c), b * ROWS + h * BQ):
                    fk[c * 4 + n, h * ROWS + b * BQ : h * ROWS + (b + 1) * BQ, :] = t

        def v_step(c, _):
            for b in range(2):
                project_v(fv, c, a_far, h * ROWS + b * BQ)

        lax.fori_loop(0, 2, k_step, None)
        lax.fori_loop(0, 2, v_step, None)

    @pl.when(late)
    def _():
        far_project(0)

        def first(i, _):
            block(order(i), fk, fv, 0, 0, BK)
            pl.when(i == 1)(lambda: hand_on(3))

        lax.fori_loop(0, 4, first, None)
        far_project(1)
        for r in range(4):
            hand(r).wait_send()

    for u in range(2, 6):
        o_copy(u).start()
    pl.semaphore_signal(ready, inc=1, device_id=partner, device_id_type=MESH)
    for r in range(4):
        swap(r).wait_send()
        pl.when(chip == 0)(far(r).wait_send)

    def last(i, _):
        iq = order(i)
        pl.when(late)(lambda: block(iq, fk, fv, 0, BK, BK))
        for h in range(KV):
            out = (mix[iq, h, :HEAD, :] * (1 / mix[iq, h, HEAD : HEAD + 1, :])).astype(a_loc.dtype).T
            for n in range(GROUP):
                a_loc[_rows(iq * BQ, BQ), (GROUP * h + n) * HEAD : (GROUP * h + n + 1) * HEAD] = out[n * BQ : (n + 1) * BQ, :]

        @pl.when(i == 1)
        def _():
            pl.semaphore_wait(ready, 1)
            seen(0).start()

        pl.when(i == 2)(seen(1).start)

    lax.fori_loop(0, 4, last, None)

    for i in range(2):
        seen(i).wait_recv()

    def output(n, _):
        slots = [lax.rem(5 + 2 * n + i, SLOTS) for i in range(2)]
        for slot in slots:
            w_wait(slot)
        pl.when(n >= 2)(y_copy(n).wait)
        for b in range(ROWS // BQ):
            rows = slice(b * BQ, (b + 1) * BQ)
            t = project(a_loc, mine + b * BQ, slots[0]) + project(a_far, b * BQ, slots[1])
            ybuf[lax.rem(n, 2), rows, :] = (xbuf[rows, _rows(n * COLS, COLS)].astype(jnp.float32) + t).astype(ybuf.dtype)
        y_copy(n).start()
        pl.when(n == 0)(o_copy(7).start)

    lax.fori_loop(0, 4, output, None)
    for n in (2, 3):
        y_copy(n).wait()
    for i in range(2):
        seen(i).wait_send()


def rotary():
    half = HEAD // 2
    places = np.arange(2 * CHIP, dtype=np.float32)
    angle = places[:, None] * (np.float32(THETA) ** (-np.arange(half, dtype=np.float32) / np.float32(half)))
    return np.concatenate([np.cos(angle.astype(np.float64)), np.sin(angle.astype(np.float64))], -1).astype(np.float32)


def solution(mesh):
    def step(x, gain, wq, wk, wv, wo):
        bf, f32 = jnp.bfloat16, jnp.float32
        dma = pltpu.SemaphoreType.DMA
        hbm = pl.BlockSpec(memory_space=pl.ANY)
        return pl.pallas_call(
            _kernel,
            out_shape=jax.ShapeDtypeStruct(x.shape, x.dtype),
            in_specs=[hbm, pl.BlockSpec(memory_space=pltpu.VMEM), *[hbm] * 5],
            out_specs=hbm,
            scratch_shapes=[
                pltpu.VMEM((CHIP, DEPTH), bf),
                pltpu.VMEM((CHIP, DEPTH), bf),
                pltpu.VMEM((3 * KV, CHIP, HEAD), bf),
                pltpu.VMEM((KV, HEAD, CHIP), bf),
                pltpu.VMEM((KV, CHIP, HEAD), bf),
                pltpu.VMEM((KV, HEAD, CHIP), bf),
                pltpu.VMEM((CHIP // BQ, KV, GROUP * BQ), f32),
                pltpu.VMEM((CHIP // BQ, KV, HEAD + 8, GROUP * BQ), f32),
                pltpu.VMEM((SLOTS, DEPTH, COLS), bf),
                pltpu.VMEM((ROWS, DEPTH), bf),
                pltpu.VMEM((2 * CHIP, HEAD), f32),
                pltpu.VMEM((2, ROWS, COLS), bf),
                dma((4,)), dma, dma((SLOTS,)), dma((2,)),
                *[dma((4,))] * 6, dma((2,)), dma((2,)),
                pltpu.SemaphoreType.REGULAR,
            ],
            compiler_params=pltpu.CompilerParams(collective_id=0, has_side_effects=True, vmem_limit_bytes=VMEM),
            name="layer",
        )(x, gain, jnp.asarray(rotary()), wq, wk, wv, wo)

    tokens, whole = P(("dp", "sp"), None), P(None, None)
    return jax.shard_map(
        step,
        mesh=mesh,
        in_specs=(tokens, P(None), whole, whole, whole, whole),
        out_specs=tokens,
        check_vma=False,
    )
```

```python
import functools

import jax
import jax.numpy as jnp
import numpy as np
from jax import lax
from jax.experimental import pallas as pl
from jax.experimental.pallas import tpu as pltpu
from jax.sharding import PartitionSpec as P

HIDDEN = -jnp.inf
LOG2E = 1.4426950408889634
VMEM = 63 * 2**20
HEAD = 128
THETA = 10000

ROWS = 512
CHIP = 1024
DEPTH = 2048
COLS = 512
KV = 8
GROUP = 2
BQ = 256
BK = 512
AT_ONCE = 4
PIECE = 128
MOVED = 256
SLOTS = 7

MESH = pl.DeviceIdType.MESH


def _dot(a, b, ca, cb):
    return lax.dot_general(a, b, (((ca,), (cb,)), ((), ())), preferred_element_type=jnp.float32)


def _rows(start, size):
    return pl.ds(pl.multiple_of(start, size), size)


def _kernel(x, gain, table, wq, wk, wv, wo, y, a_loc, a_far, qk, v, fk, fv, top, mix, wbuf, xbuf, tab, ybuf, xm, ym,
            x_sem, tab_sem, w_sem, y_sem, swap_out, swap_in, far_out, far_in, pass_out, pass_in, seen_out, seen_in,
            back_out, back_in, xb_out, xb_in, yb_out, yb_in, ready):
    sp = lax.axis_index("sp")
    core, chip = lax.rem(sp, 2), lax.div(sp, 2)
    early, late = chip == 0, chip == 1
    giver = sp == 2
    partner, across = {"sp": chip * 2 + 1 - core}, {"sp": (1 - chip) * 2 + core}
    mine, theirs = core * ROWS, (1 - core) * ROWS
    kv_cols = KV * HEAD
    q_cols = GROUP * kv_cols

    def x_copy(r):
        return pltpu.make_async_copy(x.at[pl.ds(r * PIECE, PIECE)], xbuf.at[pl.ds(r * PIECE, PIECE)], x_sem.at[r])

    def w_copy(w, row, column, slot):
        return pltpu.make_async_copy(w.at[_rows(row, DEPTH), _rows(column, COLS)], wbuf.at[slot], w_sem.at[slot])

    def q_slot(c):
        return 4 + lax.rem(c, 3)

    def q_copy(c):
        return w_copy(wq, 0, core * q_cols + lax.rem(c, 4) * COLS, q_slot(c))

    def o_slot(u):
        return lax.rem(5 + u, SLOTS)

    def o_copy(u):
        return w_copy(wo, jnp.where(lax.rem(u, 2) == 0, core, 1 - core) * DEPTH, lax.div(lax.rem(u, 8), 2) * COLS, o_slot(u))

    def w_wait(slot):
        pltpu.make_async_copy(wq.at[pl.ds(0, DEPTH), pl.ds(0, COLS)], wbuf.at[slot], w_sem.at[slot]).wait()

    def remote(src, dst, out, got, device):
        return pltpu.make_async_remote_copy(src_ref=src, dst_ref=dst, send_sem=out, recv_sem=got, device_id=device, device_id_type=MESH)

    def swap(r):
        rows = a_loc.at[_rows(mine + r * PIECE, PIECE)]
        return remote(rows, rows, swap_out.at[r], swap_in.at[r], partner)

    def far_rows(c, r):
        return a_far.at[_rows(r // 2 * ROWS + c * BQ + r % 2 * PIECE, PIECE)]

    def far(r):
        return remote(a_loc.at[_rows(mine + r * PIECE, PIECE)], far_rows(core, r), far_out.at[r], far_in.at[r], across)

    def hand(r):
        return remote(far_rows(core, r), far_rows(core, r), pass_out.at[r], pass_in.at[r], partner)

    def moved_rows(r):
        return a_loc.at[pl.ds(CHIP + r * PIECE, PIECE)]

    def back(r):
        return remote(a_loc.at[pl.ds(r * PIECE, PIECE)], moved_rows(r), back_out.at[r], back_in.at[r], {"sp": 0})

    def hand_moved(r):
        return remote(moved_rows(r), moved_rows(r), pass_out.at[r], pass_in.at[r], partner)

    def x_back(c):
        return remote(xbuf.at[pl.ds(c * PIECE, PIECE)], xm, xb_out.at[c], xb_in, {"sp": c})

    def y_back(c):
        return remote(ym, y.at[_rows(c * PIECE, PIECE)], yb_out, yb_in.at[c], {"sp": 2})

    def seen(i):
        return remote(a_loc.at[_rows(theirs + i * BQ, BQ)], a_far.at[pl.ds(i * BQ, BQ)], seen_out.at[i], seen_in.at[i], partner)

    def seen_moved():
        rows = a_loc.at[_rows(CHIP + (1 - core) * PIECE, PIECE)]
        return remote(rows, a_far.at[pl.ds(ROWS, PIECE)], seen_out.at[2], seen_in.at[2], partner)

    def y_copy(n, b):
        slot, rows = lax.rem(n, 2), pl.ds(b * BQ, BQ)
        return pltpu.make_async_copy(ybuf.at[slot, rows], y.at[rows, _rows(n * COLS, COLS)], y_sem.at[slot, b])

    for r in range(4):
        x_copy(r).start()
    table_copy = pltpu.make_async_copy(table, tab, tab_sem)
    table_copy.start()

    barrier = pltpu.get_barrier_semaphore()
    for other in range(1, 4):
        pl.semaphore_signal(barrier, inc=1, device_id={"sp": lax.rem(sp + other, 4)}, device_id_type=MESH)
    pl.semaphore_wait(barrier, 3)

    def send(r):
        swap(r).start()
        pl.when(early)(far(r).start)
        if r < 2:
            pl.when(giver)(back(r).start)

    for r in range(4):
        x_copy(r).wait()
        if r == 1:
            w_copy(wk, 0, core * kv_cols, 0).start()
        if r == 3:
            w_copy(wk, 0, core * kv_cols + COLS, 1).start()
            for c in range(2):
                w_copy(wv, 0, core * kv_cols + c * COLS, 2 + c).start()
            for c in range(3):
                q_copy(c).start()
        wide = xbuf[r * PIECE : (r + 1) * PIECE, :].astype(jnp.float32)
        scale = lax.rsqrt(jnp.mean(wide * wide, -1, keepdims=True) + 1e-6)
        a_loc[_rows(mine + r * PIECE, PIECE), :] = (wide * scale * gain[...].astype(jnp.float32)[None, :]).astype(a_loc.dtype)
        if r:
            send(r - 1)
    table_copy.wait()
    send(3)

    @pl.when(giver)
    def _():
        for c in range(2):
            x_back(c).start()

    def turned(t, place):
        rows = t.shape[0]
        both = tab[_rows(place, rows), :]
        back = pltpu.roll(both, HEAD // 2, 1)
        first = lax.broadcasted_iota(jnp.int32, both.shape, 1) < HEAD // 2
        cos, sin = jnp.where(first, both, back), jnp.where(first, -back, both)
        t = t.astype(qk.dtype).astype(jnp.float32)
        for h in range(COLS // HEAD):
            part = t[:, h * HEAD : (h + 1) * HEAD]
            yield h, (part * cos + pltpu.roll(part, HEAD // 2, 1) * sin).astype(qk.dtype)

    def project(a, row, slot, rows=BQ):
        return jnp.dot(a[_rows(row, rows), :], wbuf[slot], preferred_element_type=jnp.float32)

    def project_qk(c, slot, parts):
        for row in parts:
            for h, t in turned(project(a_loc, row, slot), chip * CHIP + row):
                qk[c * 4 + h, _rows(row, BQ), :] = t

    def project_v(out, c, a, row):
        t = project(a, row, 2 + c).astype(out.dtype)
        for h in range(COLS // HEAD):
            out[c * 4 + h, :, _rows(row, BQ)] = t[:, h * HEAD : (h + 1) * HEAD].T

    w_wait(0)
    project_qk(4, 0, (mine, mine + BQ))
    for r in range(4):
        swap(r).wait_recv()
    project_qk(4, 0, (theirs, theirs + BQ))

    def local_v(c, _):
        w_wait(2 + c)
        for b in range(CHIP // BQ):
            project_v(v, c, a_loc, b * BQ)

    w_wait(1)

    def local_qk(i, _):
        c = jnp.where(i == 0, 5, i - 1)
        slot = jnp.where(i == 0, 1, q_slot(i + 2))
        pl.when(i > 0)(lambda: w_wait(slot))
        pl.when((i == 0) | early)(lambda: project_qk(c, slot, (0,)))
        project_qk(c, slot, range(BQ, CHIP, BQ))
        pl.when((i == 1) | (i > 1) & early)(q_copy(i + 2).start)

        @pl.when((i == 4) & (sp == 0))
        def _():
            for r in range(2):
                back(r).wait_recv()
                hand_moved(r).start()

    lax.fori_loop(0, 1, local_qk, None)
    lax.fori_loop(0, 2, local_v, None)
    lax.fori_loop(1, 5, local_qk, None)

    @pl.when(early)
    def _():
        @pl.when(core == 1)
        def _():
            for r in range(2):
                hand_moved(r).wait_recv()

        def moved_qk(i, _):
            c = jnp.where(i < 4, i, i)
            slot = jnp.where(i < 4, q_slot(i + 4), i - 4)
            pl.when(i < 4)(lambda: w_wait(slot))
            project_qk(c, slot, (CHIP,))
            pl.when(i < 1)(q_copy(i + 7).start)

        lax.fori_loop(0, 6, moved_qk, None)
        lax.fori_loop(0, 2, lambda c, _: project_v(v, c, a_loc, CHIP), None)
        for u in range(2, 6):
            o_copy(u).start()

    for u in (0, 1, 6):
        o_copy(u).start()

    e = HEAD**-0.5 * LOG2E
    cols = GROUP * BQ

    def block(iq, keys, values, k0, at, size, ahead=None):
        here, queries = _rows(at, size), _rows(iq * BQ, BQ)
        state = lax.rem(iq, 4)
        ones = jnp.ones((8, size), values.dtype)
        begin = ahead is not None
        if begin:
            ok = lax.rem(lax.broadcasted_iota(jnp.int32, (size, cols), 1), BQ) + ahead >= lax.broadcasted_iota(jnp.int32, (size, cols), 0)

        def some(hb, _):
            heads = [hb * AT_ONCE + i for i in range(AT_ONCE)]
            scores = [_dot(keys[k0 + h, here, :], qk[pl.ds(GROUP * h, GROUP), queries, :].reshape(cols, HEAD), 1, 1) for h in heads]
            weights, keeps = [], []
            for h, s in zip(heads, scores):
                if begin:
                    s = jnp.where(ok, s, HIDDEN)
                    new = s.max(axis=0, keepdims=True)
                else:
                    old = top[state, pl.ds(h, 1), :]
                    new = jnp.maximum(old, s.max(axis=0, keepdims=True))
                    keeps.append(jnp.exp2((old - new) * e))
                top[state, pl.ds(h, 1), :] = new
                weights.append(jnp.exp2((s - new) * e).astype(values.dtype))
            for i, (h, p) in enumerate(zip(heads, weights)):
                got = _dot(jnp.concatenate([values[h, :, here], ones], axis=0), p, 1, 0)
                mix[state, h] = got if begin else mix[state, h] * keeps[i] + got

        lax.fori_loop(0, KV // AT_ONCE, some, None)

    def finish(iq):
        state = lax.rem(iq, 4)
        for h in range(KV):
            out = (mix[state, h, :HEAD, :] * (1 / mix[state, h, HEAD : HEAD + 1, :])).astype(a_loc.dtype).T
            for n in range(GROUP):
                a_loc[_rows(iq * BQ, BQ), (GROUP * h + n) * HEAD : (GROUP * h + n + 1) * HEAD] = out[n * BQ : (n + 1) * BQ, :]

    def hand_on(r):
        @pl.when(late)
        def _():
            far(r).wait_recv()
            hand(r).start()

    def moved_output():
        seen_moved().wait_recv()
        x_back(0).wait_recv()

        def output(n, _):
            u = 2 * n
            for i in range(2):
                w_wait(o_slot(u + i))
            t = project(a_loc, CHIP + core * PIECE, o_slot(u), PIECE) + project(a_far, ROWS, o_slot(u + 1), PIECE)
            here = _rows(n * COLS, COLS)
            ym[:, here] = (xm[:, here].astype(jnp.float32) + t).astype(ym.dtype)
            for i in range(2):
                o_copy(u + i + SLOTS).start()

        lax.fori_loop(0, 4, output, None)

    hand_on(0)

    def local(s, _):
        iq = jnp.where(early, lax.rem(s + 4, 5), s + 1)
        p = lax.div(iq, 2)
        pl.when(lax.rem(iq, 2) == 0)(lambda: block(iq, qk, v, 2 * KV, p * BK, BQ, 0))
        pl.when(lax.rem(iq, 2) == 1)(lambda: block(iq, qk, v, 2 * KV, p * BK, BK, BQ))
        lax.fori_loop(0, p, lambda j, _: block(iq, qk, v, 2 * KV, j * BK, BK), None)

        @pl.when(early)
        def _():
            @pl.when(s == 0)
            def _():
                @pl.when(core == 0)
                def _():
                    for r in range(2):
                        hand_moved(r).wait_send()

                finish(4)

            pl.when(s == 1)(seen_moved().start)
            pl.when(s == 2)(moved_output)
            pl.when(s == 3)(y_back(core).start)

        pl.when(s == 1)(lambda: hand_on(1))

    lax.fori_loop(0, jnp.where(early, 5, 3), local, None)

    def far_project(h):
        for r in (0, 1):
            hand(2 * h + r).wait_recv()

        def k_step(c, _):
            for b in range(2):
                for n, t in turned(project(a_far, h * ROWS + b * BQ, c), b * ROWS + h * BQ):
                    fk[c * 4 + n, h * ROWS + b * BQ : h * ROWS + (b + 1) * BQ, :] = t

        def v_step(c, _):
            for b in range(2):
                project_v(fv, c, a_far, h * ROWS + b * BQ)

        lax.fori_loop(0, 2, k_step, None)
        lax.fori_loop(0, 2, v_step, None)

    def order(i):
        return jnp.where(early, lax.rem((1 - core) * 2 + i, 4), 1 + lax.rem(i + 1 - core, 3))

    @pl.when(late)
    def _():
        far_project(0)

        def first(i, _):
            block(order(i), fk, fv, 0, 0, BK)
            pl.when(i == 0)(lambda: hand_on(2))
            pl.when(i == 2)(lambda: hand_on(3))

        lax.fori_loop(0, 3, first, None)
        far_project(1)
        for r in range(4):
            hand(r).wait_send()
        pl.semaphore_signal(ready, inc=1, device_id=partner, device_id_type=MESH)
        for u in range(2, 6):
            o_copy(u).start()

    for r in range(4):
        swap(r).wait_send()
        pl.when(early)(far(r).wait_send)

    def last(i, _):
        iq = order(i)
        pl.when(late)(lambda: block(iq, fk, fv, 0, BK, BK))
        finish(iq)

        @pl.when(i == 1)
        def _():
            pl.when(late)(lambda: pl.semaphore_wait(ready, 1))
            pl.when(sp != 3)(seen(0).start)
            pl.when(sp == 3)(seen(1).start)

        pl.when((i == 2) & (sp != 3))(seen(1).start)

    lax.fori_loop(0, jnp.where(early, 4, 3), last, None)

    pl.when(sp != 2)(seen(0).wait_recv)
    seen(1).wait_recv()
    begin = jnp.where(early, 8, 0)

    def output(n, _):
        u = begin + 2 * n
        for i in range(2):
            w_wait(o_slot(u + i))

        def part(b):
            pl.when(n >= 2)(y_copy(n, b).wait)
            t = project(a_loc, mine + b * BQ, o_slot(u)) + project(a_far, b * BQ, o_slot(u + 1))
            rows = pl.ds(b * BQ, BQ)
            ybuf[lax.rem(n, 2), rows, :] = (xbuf[rows, _rows(n * COLS, COLS)].astype(jnp.float32) + t).astype(ybuf.dtype)
            y_copy(n, b).start()

        pl.when(sp != 2)(lambda: part(0))
        part(1)
        pl.when(n == 0)(o_copy(u + SLOTS).start)

    lax.fori_loop(0, 4, output, None)
    for n in (2, 3):
        pl.when(sp != 2)(y_copy(n, 0).wait)
        y_copy(n, 1).wait()
    pl.when(sp != 3)(seen(0).wait_send)
    seen(1).wait_send()

    @pl.when(early)
    def _():
        seen_moved().wait_send()
        y_back(core).wait_send()

    @pl.when(giver)
    def _():
        for c in range(2):
            back(c).wait_send()
            x_back(c).wait_send()
            y_back(c).wait_recv()


def rotary():
    half = HEAD // 2
    places = np.arange(2 * CHIP, dtype=np.float32)
    angle = places[:, None] * (np.float32(THETA) ** (-np.arange(half, dtype=np.float32) / np.float32(half)))
    return np.concatenate([np.cos(angle.astype(np.float64)), np.sin(angle.astype(np.float64))], -1).astype(np.float32)


def solution(mesh):
    def step(x, gain, wq, wk, wv, wo):
        bf, f32 = jnp.bfloat16, jnp.float32
        dma = pltpu.SemaphoreType.DMA
        hbm = pl.BlockSpec(memory_space=pl.ANY)
        return pl.pallas_call(
            _kernel,
            out_shape=jax.ShapeDtypeStruct(x.shape, x.dtype),
            in_specs=[hbm, pl.BlockSpec(memory_space=pltpu.VMEM), *[hbm] * 5],
            out_specs=hbm,
            scratch_shapes=[
                pltpu.VMEM((CHIP + MOVED, DEPTH), bf),
                pltpu.VMEM((CHIP, DEPTH), bf),
                pltpu.VMEM((3 * KV, CHIP + MOVED, HEAD), bf),
                pltpu.VMEM((KV, HEAD, CHIP + MOVED), bf),
                pltpu.VMEM((KV, CHIP, HEAD), bf),
                pltpu.VMEM((KV, HEAD, CHIP), bf),
                pltpu.VMEM((CHIP // BQ, KV, GROUP * BQ), f32),
                pltpu.VMEM((CHIP // BQ, KV, HEAD + 8, GROUP * BQ), f32),
                pltpu.VMEM((SLOTS, DEPTH, COLS), bf),
                pltpu.VMEM((ROWS, DEPTH), bf),
                pltpu.VMEM((2 * CHIP, HEAD), f32),
                pltpu.VMEM((2, ROWS, COLS), bf),
                pltpu.VMEM((PIECE, DEPTH), bf),
                pltpu.VMEM((PIECE, DEPTH), bf),
                dma((4,)), dma, dma((SLOTS,)), dma((2, 2)),
                *[dma((4,))] * 6, dma((3,)), dma((3,)),
                dma((2,)), dma((2,)), dma((2,)), dma, dma, dma((2,)),
                pltpu.SemaphoreType.REGULAR,
            ],
            compiler_params=pltpu.CompilerParams(collective_id=0, has_side_effects=True, vmem_limit_bytes=VMEM),
            name="layer",
        )(x, gain, jnp.asarray(rotary()), wq, wk, wv, wo)

    tokens, whole = P(("dp", "sp"), None), P(None, None)
    return jax.shard_map(
        step,
        mesh=mesh,
        in_specs=(tokens, P(None), whole, whole, whole, whole),
        out_specs=tokens,
        check_vma=False,
    )
```

```python
import functools

import jax
import jax.numpy as jnp
import numpy as np
from jax import lax
from jax.experimental import pallas as pl
from jax.experimental.pallas import tpu as pltpu
from jax.sharding import PartitionSpec as P

HIDDEN = -jnp.inf
LOG2E = 1.4426950408889634
VMEM = 61 * 2**20
HEAD = 128
THETA = 10000

ROWS = 512
CHIP = 1024
DEPTH = 2048
COLS = 512
KV = 8
GROUP = 2
BQ = 256
BK = 512
PIECE = 128
MOVED = 256
SLOTS = 7

MESH = pl.DeviceIdType.MESH


def _dot(a, b, ca, cb):
    return lax.dot_general(a, b, (((ca,), (cb,)), ((), ())), preferred_element_type=jnp.float32)


def _rows(start, size):
    return pl.ds(pl.multiple_of(start, size), size)


def _kernel(x, gain, table, wq, wk, wv, wo, y, a_loc, a_far, q, k, v, top, mix, wbuf, xbuf, tab, xm, ym,
            x_sem, tab_sem, w_sem, swap_out, swap_in, far_out, far_in, pass_out, pass_in, seen_out, seen_in,
            back_out, back_in, xb_out, xb_in, yb_out, yb_in, share_out, share_in, ready):
    sp = lax.axis_index("sp")
    core, chip = lax.rem(sp, 2), lax.div(sp, 2)
    early, late = chip == 0, chip == 1
    giver = sp == 2
    partner, across = {"sp": chip * 2 + 1 - core}, {"sp": (1 - chip) * 2 + core}
    mine, theirs = core * ROWS, (1 - core) * ROWS
    kv_cols = KV * HEAD
    q_cols = GROUP * kv_cols

    def x_copy(r):
        return pltpu.make_async_copy(x.at[pl.ds(r * PIECE, PIECE)], xbuf.at[pl.ds(r * PIECE, PIECE)], x_sem.at[r])

    def w_copy(w, row, column, slot):
        return pltpu.make_async_copy(w.at[_rows(row, DEPTH), _rows(column, COLS)], wbuf.at[slot], w_sem.at[slot])

    def q_slot(c):
        return 4 + lax.rem(c, 3)

    def q_copy(c):
        return w_copy(wq, 0, core * q_cols + lax.rem(c, 4) * COLS, q_slot(c))

    def o_slot(u):
        return lax.rem(5 + u, SLOTS)

    def o_copy(u):
        return w_copy(wo, jnp.where(lax.rem(u, 2) == 0, core, 1 - core) * DEPTH, lax.div(lax.rem(u, 8), 2) * COLS, o_slot(u))

    def w_wait(slot):
        pltpu.make_async_copy(wq.at[pl.ds(0, DEPTH), pl.ds(0, COLS)], wbuf.at[slot], w_sem.at[slot]).wait()

    def remote(src, dst, out, got, device):
        return pltpu.make_async_remote_copy(src_ref=src, dst_ref=dst, send_sem=out, recv_sem=got, device_id=device, device_id_type=MESH)

    def swap(r):
        rows = a_loc.at[_rows(mine + r * PIECE, PIECE)]
        return remote(rows, rows, swap_out.at[r], swap_in.at[r], partner)

    def far_rows(c, r):
        return a_far.at[_rows(r // 2 * ROWS + c * BQ + r % 2 * PIECE, PIECE)]

    def far(r):
        return remote(a_loc.at[_rows(mine + r * PIECE, PIECE)], far_rows(core, r), far_out.at[r], far_in.at[r], across)

    def hand(r):
        return remote(far_rows(core, r), far_rows(core, r), pass_out.at[r], pass_in.at[r], partner)

    def moved_rows(r):
        return a_loc.at[pl.ds(CHIP + r * PIECE, PIECE)]

    def back(r):
        return remote(a_loc.at[pl.ds(r * PIECE, PIECE)], moved_rows(r), back_out.at[r], back_in.at[r], {"sp": 0})

    def hand_moved(r):
        return remote(moved_rows(r), moved_rows(r), pass_out.at[r], pass_in.at[r], partner)

    def x_back(c):
        return remote(xbuf.at[pl.ds(c * PIECE, PIECE)], xm, xb_out.at[c], xb_in, {"sp": c})

    def y_back(c):
        return remote(ym, y.at[_rows(c * PIECE, PIECE)], yb_out, yb_in.at[c], {"sp": 2})

    def seen(i):
        return remote(a_loc.at[_rows(theirs + i * BQ, BQ)], a_far.at[pl.ds(i * BQ, BQ)], seen_out.at[i], seen_in.at[i], partner)

    def seen_more():
        rows = a_loc.at[_rows(jnp.where(early, CHIP + (1 - core) * PIECE, ROWS), PIECE)]
        return remote(rows, a_far.at[pl.ds(ROWS, PIECE)], seen_out.at[2], seen_in.at[2], partner)

    def x_share():
        return remote(xbuf.at[pl.ds(0, PIECE)], xm, xb_out.at[0], xb_in, {"sp": 2})

    def y_share(n):
        here = _rows(n * COLS, COLS)
        return remote(ym.at[:, here], y.at[pl.ds(0, PIECE), here], share_out.at[n], share_in.at[n], {"sp": 3})

    for r in range(4):
        x_copy(r).start()
    table_copy = pltpu.make_async_copy(table, tab, tab_sem)
    table_copy.start()

    barrier = pltpu.get_barrier_semaphore()
    for other in range(1, 4):
        pl.semaphore_signal(barrier, inc=1, device_id={"sp": lax.rem(sp + other, 4)}, device_id_type=MESH)
    pl.semaphore_wait(barrier, 3)

    def send(r):
        swap(r).start()
        pl.when(early)(far(r).start)
        if r < 2:
            pl.when(giver)(back(r).start)

    for r in range(4):
        x_copy(r).wait()
        if r == 1:
            w_copy(wk, 0, core * kv_cols, 0).start()
        if r == 3:
            w_copy(wk, 0, core * kv_cols + COLS, 1).start()
            for c in range(2):
                w_copy(wv, 0, core * kv_cols + c * COLS, 2 + c).start()
            for c in range(3):
                q_copy(c).start()
        wide = xbuf[r * PIECE : (r + 1) * PIECE, :].astype(jnp.float32)
        scale = lax.rsqrt(jnp.mean(wide * wide, -1, keepdims=True) + 1e-6)
        a_loc[_rows(mine + r * PIECE, PIECE), :] = (wide * scale * gain[...].astype(jnp.float32)[None, :]).astype(a_loc.dtype)
        if r:
            send(r - 1)
    table_copy.wait()
    send(3)

    pl.when(sp == 3)(x_share().start)

    @pl.when(giver)
    def _():
        for c in range(2):
            x_back(c).start()

    def turned(t, place):
        rows = t.shape[0]
        both = tab[_rows(place, rows), :]
        back = pltpu.roll(both, HEAD // 2, 1)
        first = lax.broadcasted_iota(jnp.int32, both.shape, 1) < HEAD // 2
        cos, sin = jnp.where(first, both, back), jnp.where(first, -back, both)
        t = t.astype(q.dtype).astype(jnp.float32)
        for h in range(COLS // HEAD):
            part = t[:, h * HEAD : (h + 1) * HEAD]
            yield h, (part * cos + pltpu.roll(part, HEAD // 2, 1) * sin).astype(q.dtype)

    def project(a, row, slot, rows=BQ):
        return jnp.dot(a[_rows(row, rows), :], wbuf[slot], preferred_element_type=jnp.float32)

    def project_q(c, row):
        for h, t in turned(project(a_loc, row, q_slot(c)), chip * CHIP + row):
            q[lax.rem(c, 4) * 4 + h, _rows(row, BQ), :] = t

    def project_k(c, a, row, place, key):
        for h, t in turned(project(a, row, c), place):
            k[c * 4 + h, _rows(key, BQ), :] = t

    def project_v(c, a, row, key):
        t = project(a, row, 2 + c).astype(v.dtype)
        for h in range(COLS // HEAD):
            v[c * 4 + h, :, _rows(key, BQ)] = t[:, h * HEAD : (h + 1) * HEAD].T

    for c in range(2):
        w_wait(c)

    def local_k(part, _):
        @pl.when(part == 1)
        def _():
            for r in range(4):
                swap(r).wait_recv()

        for c in range(2):
            for b in range(2):
                row = jnp.where(part == 0, mine, theirs) + b * BQ
                project_k(c, a_loc, row, chip * CHIP + row, row)

    lax.fori_loop(0, 2, local_k, None)

    def local_v(c, _):
        w_wait(2 + c)
        for b in range(CHIP // BQ):
            project_v(c, a_loc, b * BQ, b * BQ)

    lax.fori_loop(0, 2, local_v, None)

    def local_q(c, _):
        w_wait(q_slot(c))
        pl.when(early)(lambda: project_q(c, 0))
        for b in range(1, CHIP // BQ):
            project_q(c, b * BQ)
        pl.when((c == 0) | early)(q_copy(c + 3).start)

        @pl.when((c == 3) & (sp == 0))
        def _():
            for r in range(2):
                back(r).wait_recv()
                hand_moved(r).start()

    lax.fori_loop(0, 4, local_q, None)

    @pl.when(early)
    def _():
        @pl.when(core == 1)
        def _():
            for r in range(2):
                hand_moved(r).wait_recv()

        def moved_q(c, _):
            w_wait(q_slot(c))
            project_q(c, CHIP)
            pl.when(c == 4)(q_copy(7).start)

        lax.fori_loop(4, 8, moved_q, None)
        for c in range(2):
            project_k(c, a_loc, CHIP, CHIP, CHIP)
            project_v(c, a_loc, CHIP, CHIP)
        for u in range(2, 6):
            o_copy(u).start()

    for u in (0, 1, 6):
        o_copy(u).start()

    e = HEAD**-0.5 * LOG2E
    cols = GROUP * BQ

    def block(iq, state, at, size, ahead=None):
        here, queries = _rows(at, size), _rows(iq * BQ, BQ)
        ones = jnp.ones((8, size), v.dtype)
        begin = ahead is not None
        if begin:
            ok = lax.rem(lax.broadcasted_iota(jnp.int32, (size, cols), 1), BQ) + ahead >= lax.broadcasted_iota(jnp.int32, (size, cols), 0)

        def scores(h):
            return _dot(k[h, here, :], q[GROUP * h : GROUP * (h + 1), queries, :].reshape(cols, HEAD), 1, 1)

        def weights(h, s):
            if begin:
                s = jnp.where(ok, s, HIDDEN)
                new, keep = s.max(axis=0, keepdims=True), None
            else:
                old = top[state, h : h + 1, :]
                new = jnp.maximum(old, s.max(axis=0, keepdims=True))
                keep = jnp.exp2((old - new) * e)
            top[state, h : h + 1, :] = new
            return jnp.exp2((s - new) * e).astype(v.dtype), keep

        def add(h, p, keep):
            got = _dot(jnp.concatenate([v[h, :, here], ones], axis=0), p, 1, 0)
            mix[state, h] = got if begin else mix[state, h] * keep + got

        ready_s, ready_p = [scores(0), scores(1)], []
        for h in range(KV):
            if h + 2 < KV:
                ready_s.append(scores(h + 2))
            ready_p.append(weights(h, ready_s[h]))
            if h:
                add(h - 1, *ready_p[h - 1])
        add(KV - 1, *ready_p[-1])

    def finish(iq, state):
        for h in range(KV):
            out = (mix[state, h, :HEAD, :] * (1 / mix[state, h, HEAD : HEAD + 1, :])).astype(a_loc.dtype).T
            for n in range(GROUP):
                a_loc[_rows(iq * BQ, BQ), (GROUP * h + n) * HEAD : (GROUP * h + n + 1) * HEAD] = out[n * BQ : (n + 1) * BQ, :]

    def hand_on(r):
        @pl.when(late)
        def _():
            far(r).wait_recv()
            hand(r).start()

    def moved_output():
        seen_more().wait_recv()
        x_back(0).wait_recv()

        def output(n, _):
            u = 2 * n
            for i in range(2):
                w_wait(o_slot(u + i))
            t = project(a_loc, CHIP + core * PIECE, o_slot(u), PIECE) + project(a_far, ROWS, o_slot(u + 1), PIECE)
            here = _rows(n * COLS, COLS)
            ym[:, here] = (xm[:, here].astype(jnp.float32) + t).astype(ym.dtype)
            for i in range(2):
                o_copy(u + i + SLOTS).start()

        lax.fori_loop(0, 4, output, None)

    hand_on(0)

    def far_project(half):
        def part(i, _):
            c = jnp.where(i == 0, core, 1 - core)

            @pl.when(i == 1)
            def _():
                for r in range(2):
                    hand(2 * half + r).wait_recv()

            row = half * ROWS + c * BQ
            for n in range(2):
                project_k(n, a_far, row, c * ROWS + half * BQ, CHIP + row)
                project_v(n, a_far, row, CHIP + row)

        lax.fori_loop(0, 2, part, None)

    def step(s, _):
        far_step = late & (s >= 3)
        half, i = lax.div(s, 3) - 1, lax.rem(s, 3)
        iq_early = jnp.where(s == 0, 4, lax.rem((1 - core) * 2 + s + 3, 4))
        iq_late = jnp.where(s < 3, s + 1, 1 + lax.rem(i + 1 - core, 3))
        iq = jnp.where(early, iq_early, iq_late)
        state = jnp.where(early, 0, iq - 1)
        p = lax.div(iq, 2)

        pl.when(far_step & (i == 0))(lambda: far_project(half))

        @pl.when(late & (s == 6))
        def _():
            for r in range(4):
                hand(r).wait_send()
            pl.semaphore_signal(ready, inc=1, device_id=partner, device_id_type=MESH)
            for u in range(2, 6):
                o_copy(u).start()

        @pl.when((late & (s == 6)) | (early & (s == 3)))
        def _():
            for r in range(4):
                swap(r).wait_send()
                pl.when(early)(far(r).wait_send)

        @pl.when(late & (s == 7))
        def _():
            pl.semaphore_wait(ready, 1)
            pl.when(core == 0)(seen(0).start)
            pl.when(core == 1)(seen(1).start)

        @pl.when(late & (s == 8))
        def _():
            pl.when(core == 0)(seen(1).start)
            pl.when(core == 1)(seen_more().start)

        even = lax.rem(iq, 2) == 0
        pl.when(jnp.logical_not(far_step) & even)(lambda: block(iq, state, p * BK, BQ, 0))
        pl.when(jnp.logical_not(far_step) & jnp.logical_not(even))(lambda: block(iq, state, p * BK, BK, BQ))

        @pl.when(early)
        def _():
            pl.when(s == 1)(seen_more().start)
            pl.when(s == 2)(seen(0).start)
            pl.when(s == 3)(seen(1).start)

        start = jnp.where(far_step, CHIP + half * BK, 0)
        lax.fori_loop(0, jnp.where(far_step, 1, p), lambda j, _: block(iq, state, start + j * BK, BK), None)

        @pl.when((s == 0) & (sp == 0))
        def _():
            for r in range(2):
                hand_moved(r).wait_send()

        pl.when(early | (s >= 6))(lambda: finish(iq, state))

        @pl.when(early)
        def _():
            pl.when(s == 1 + core)(moved_output)
            pl.when(s == 2 + core)(y_back(core).start)

        for at, r in ((1, 1), (3, 2), (5, 3)):
            pl.when(s == at)(functools.partial(hand_on, r))

    lax.fori_loop(0, jnp.where(early, 5, 9), step, None)

    pl.when(sp != 2)(seen(0).wait_recv)
    seen(1).wait_recv()

    @pl.when(sp == 2)
    def _():
        seen_more().wait_recv()
        x_share().wait_recv()

    begin = jnp.where(early, 8, 0)

    def output(n, _):
        u = begin + 2 * n
        for i in range(2):
            w_wait(o_slot(u + i))
        here = _rows(n * COLS, COLS)

        def both(own, other, rows):
            return project(a_loc, own, o_slot(u), rows) + project(a_far, other, o_slot(u + 1), rows)

        def part(row, rows):
            which = pl.ds(row, rows)
            y[which, here] = (xbuf[which, here].astype(jnp.float32) + both(mine + row, row, rows)).astype(y.dtype)

        @pl.when(sp == 2)
        def _():
            ym[:, here] = (xm[:, here].astype(jnp.float32) + both(ROWS, ROWS, PIECE)).astype(ym.dtype)

        pl.when(sp == 3)(lambda: part(PIECE, PIECE))
        pl.when(early)(lambda: part(0, BQ))
        part(BQ, BQ)
        pl.when(sp == 2)(y_share(n).start)
        pl.when(n == 0)(o_copy(u + SLOTS).start)

    lax.fori_loop(0, 4, output, None)
    pl.when(sp != 3)(seen(0).wait_send)
    seen(1).wait_send()
    pl.when(sp != 2)(seen_more().wait_send)
    pl.when(early)(y_back(core).wait_send)

    @pl.when(giver)
    def _():
        for c in range(2):
            back(c).wait_send()
            x_back(c).wait_send()
            y_back(c).wait_recv()
        for n in range(4):
            y_share(n).wait_send()

    @pl.when(sp == 3)
    def _():
        x_share().wait_send()
        for n in range(4):
            y_share(n).wait_recv()


def rotary():
    half = HEAD // 2
    places = np.arange(2 * CHIP, dtype=np.float32)
    angle = places[:, None] * (np.float32(THETA) ** (-np.arange(half, dtype=np.float32) / np.float32(half)))
    return np.concatenate([np.cos(angle.astype(np.float64)), np.sin(angle.astype(np.float64))], -1).astype(np.float32)


def solution(mesh):
    def step(x, gain, wq, wk, wv, wo):
        bf, f32 = jnp.bfloat16, jnp.float32
        dma = pltpu.SemaphoreType.DMA
        hbm = pl.BlockSpec(memory_space=pl.ANY)
        return pl.pallas_call(
            _kernel,
            out_shape=pltpu.VMEM(x.shape, x.dtype),
            in_specs=[hbm, pl.BlockSpec(memory_space=pltpu.VMEM), *[hbm] * 5],
            out_specs=pl.BlockSpec(memory_space=pltpu.VMEM),
            scratch_shapes=[
                pltpu.VMEM((CHIP + MOVED, DEPTH), bf),
                pltpu.VMEM((CHIP, DEPTH), bf),
                pltpu.VMEM((GROUP * KV, CHIP + MOVED, HEAD), bf),
                pltpu.VMEM((KV, 2 * CHIP, HEAD), bf),
                pltpu.VMEM((KV, HEAD, 2 * CHIP), bf),
                pltpu.VMEM((3, KV, GROUP * BQ), f32),
                pltpu.VMEM((3, KV, HEAD + 8, GROUP * BQ), f32),
                pltpu.VMEM((SLOTS, DEPTH, COLS), bf),
                pltpu.VMEM((ROWS, DEPTH), bf),
                pltpu.VMEM((2 * CHIP, HEAD), f32),
                pltpu.VMEM((PIECE, DEPTH), bf),
                pltpu.VMEM((PIECE, DEPTH), bf),
                dma((4,)), dma, dma((SLOTS,)),
                *[dma((4,))] * 6, dma((3,)), dma((3,)),
                dma((2,)), dma((2,)), dma((2,)), dma, dma, dma((2,)), dma((4,)), dma((4,)),
                pltpu.SemaphoreType.REGULAR,
            ],
            compiler_params=pltpu.CompilerParams(collective_id=0, has_side_effects=True, vmem_limit_bytes=VMEM),
            name="layer",
        )(x, gain, jnp.asarray(rotary()), wq, wk, wv, wo)

    tokens, whole = P(("dp", "sp"), None), P(None, None)
    return jax.shard_map(
        step,
        mesh=mesh,
        in_specs=(tokens, P(None), whole, whole, whole, whole),
        out_specs=tokens,
        check_vma=False,
    )
```

```python
import functools

import jax
import jax.numpy as jnp
import numpy as np
from jax import lax
from jax.experimental import pallas as pl
from jax.experimental.pallas import tpu as pltpu
from jax.sharding import PartitionSpec as P

HIDDEN = -jnp.inf
LOG2E = 1.4426950408889634
VMEM = 61 * 2**20
HEAD = 128
THETA = 10000

ROWS = 512
CHIP = 1024
DEPTH = 2048
COLS = 512
KV = 8
GROUP = 2
BQ = 256
BK = 512
PIECE = 128
MOVED = 256
SLOTS = 7

MESH = pl.DeviceIdType.MESH


def _dot(a, b, ca, cb):
    return lax.dot_general(a, b, (((ca,), (cb,)), ((), ())), preferred_element_type=jnp.float32)


def _rows(start, size):
    return pl.ds(pl.multiple_of(start, size), size)


def _kernel(x, gain, table, wq, wk, wv, wo, y, a_loc, a_far, q, k, v, top, mix, wbuf, xbuf, tab, xm, ym,
            x_sem, tab_sem, w_sem, swap_out, swap_in, far_out, far_in, pass_out, pass_in, seen_out, seen_in,
            back_out, back_in, xb_out, xb_in, yb_out, yb_in, share_out, share_in, ready):
    sp = lax.axis_index("sp")
    core, chip = lax.rem(sp, 2), lax.div(sp, 2)
    early, late = chip == 0, chip == 1
    giver = sp == 2
    partner, across = {"sp": chip * 2 + 1 - core}, {"sp": (1 - chip) * 2 + core}
    mine, theirs = core * ROWS, (1 - core) * ROWS
    kv_cols = KV * HEAD
    q_cols = GROUP * kv_cols

    def x_copy(r):
        return pltpu.make_async_copy(x.at[pl.ds(r * PIECE, PIECE)], xbuf.at[pl.ds(r * PIECE, PIECE)], x_sem.at[r])

    def w_copy(w, row, column, slot):
        return pltpu.make_async_copy(w.at[_rows(row, DEPTH), _rows(column, COLS)], wbuf.at[slot], w_sem.at[slot])

    def q_slot(c):
        return 4 + lax.rem(c, 3)

    def q_copy(c):
        return w_copy(wq, 0, core * q_cols + lax.rem(c, 4) * COLS, q_slot(c))

    def o_slot(u):
        return lax.rem(5 + u, SLOTS)

    def o_copy(u):
        return w_copy(wo, jnp.where(lax.rem(u, 2) == 0, core, 1 - core) * DEPTH, lax.div(lax.rem(u, 8), 2) * COLS, o_slot(u))

    def w_wait(slot):
        pltpu.make_async_copy(wq.at[pl.ds(0, DEPTH), pl.ds(0, COLS)], wbuf.at[slot], w_sem.at[slot]).wait()

    def remote(src, dst, out, got, device):
        return pltpu.make_async_remote_copy(src_ref=src, dst_ref=dst, send_sem=out, recv_sem=got, device_id=device, device_id_type=MESH)

    def swap(r):
        rows = a_loc.at[_rows(mine + r * PIECE, PIECE)]
        return remote(rows, rows, swap_out.at[r], swap_in.at[r], partner)

    def far_rows(c, r):
        return a_far.at[_rows(r // 2 * ROWS + c * BQ + r % 2 * PIECE, PIECE)]

    def far(r):
        return remote(a_loc.at[_rows(mine + r * PIECE, PIECE)], far_rows(core, r), far_out.at[r], far_in.at[r], across)

    def hand(r):
        return remote(far_rows(core, r), far_rows(core, r), pass_out.at[r], pass_in.at[r], partner)

    def moved_rows(r):
        return a_loc.at[pl.ds(CHIP + r * PIECE, PIECE)]

    def back(r):
        return remote(a_loc.at[pl.ds(r * PIECE, PIECE)], moved_rows(r), back_out.at[r], back_in.at[r], {"sp": 0})

    def hand_moved(r):
        return remote(moved_rows(r), moved_rows(r), pass_out.at[r], pass_in.at[r], partner)

    def x_back(c):
        return remote(xbuf.at[pl.ds(c * PIECE, PIECE)], xm, xb_out.at[c], xb_in, {"sp": c})

    def y_back(c):
        return remote(ym, y.at[_rows(c * PIECE, PIECE)], yb_out, yb_in.at[c], {"sp": 2})

    def seen(i):
        return remote(a_loc.at[_rows(theirs + i * BQ, BQ)], a_far.at[pl.ds(i * BQ, BQ)], seen_out.at[i], seen_in.at[i], partner)

    def seen_more():
        rows = a_loc.at[_rows(jnp.where(early, CHIP + (1 - core) * PIECE, ROWS), PIECE)]
        return remote(rows, a_far.at[pl.ds(ROWS, PIECE)], seen_out.at[2], seen_in.at[2], partner)

    def x_share():
        return remote(xbuf.at[pl.ds(0, PIECE)], xm, xb_out.at[0], xb_in, {"sp": 2})

    def y_share(n):
        here = _rows(n * COLS, COLS)
        return remote(ym.at[:, here], y.at[pl.ds(0, PIECE), here], share_out.at[n], share_in.at[n], {"sp": 3})

    for r in range(4):
        x_copy(r).start()
    table_copy = pltpu.make_async_copy(table, tab, tab_sem)
    table_copy.start()

    for c in range(2):
        w_copy(wk, 0, core * kv_cols + c * COLS, c).start()

    barrier = pltpu.get_barrier_semaphore()
    for other in range(1, 4):
        pl.semaphore_signal(barrier, inc=1, device_id={"sp": lax.rem(sp + other, 4)}, device_id_type=MESH)

    for r in range(4):
        x_copy(r).wait()
        wide = xbuf[r * PIECE : (r + 1) * PIECE, :].astype(jnp.float32)
        scale = lax.rsqrt(jnp.mean(wide * wide, -1, keepdims=True) + 1e-6)
        a_loc[_rows(mine + r * PIECE, PIECE), :] = (wide * scale * gain[...].astype(jnp.float32)[None, :]).astype(a_loc.dtype)

    pl.semaphore_wait(barrier, 3)
    for r in range(4):
        pl.when(early)(far(r).start)
        swap(r).start()
        if r < 2:
            pl.when(giver)(back(r).start)
    table_copy.wait()
    pl.when(sp == 3)(x_share().start)

    @pl.when(giver)
    def _():
        for c in range(2):
            x_back(c).start()

    def turned(t, place):
        rows = t.shape[0]
        both = tab[_rows(place, rows), :]
        back = pltpu.roll(both, HEAD // 2, 1)
        first = lax.broadcasted_iota(jnp.int32, both.shape, 1) < HEAD // 2
        cos, sin = jnp.where(first, both, back), jnp.where(first, -back, both)
        t = t.astype(q.dtype).astype(jnp.float32)
        for h in range(COLS // HEAD):
            part = t[:, h * HEAD : (h + 1) * HEAD]
            yield h, (part * cos + pltpu.roll(part, HEAD // 2, 1) * sin).astype(q.dtype)

    def project(a, row, slot, rows=BQ):
        return jnp.dot(a[_rows(row, rows), :], wbuf[slot], preferred_element_type=jnp.float32)

    def project_q(c, row):
        for h, t in turned(project(a_loc, row, q_slot(c)), chip * CHIP + row):
            q[lax.rem(c, 4) * 4 + h, _rows(row, BQ), :] = t

    def project_k(c, a, row, place, key):
        for h, t in turned(project(a, row, c), place):
            k[c * 4 + h, _rows(key, BQ), :] = t

    def project_v(c, a, row, key):
        t = project(a, row, 2 + c).astype(v.dtype)
        for h in range(COLS // HEAD):
            v[c * 4 + h, :, _rows(key, BQ)] = t[:, h * HEAD : (h + 1) * HEAD].T

    for c in range(2):
        w_wait(c)
    for c in range(2):
        w_copy(wv, 0, core * kv_cols + c * COLS, 2 + c).start()
    for c in range(3):
        q_copy(c).start()

    def local_k(part, _):
        @pl.when(part == 1)
        def _():
            for r in range(4):
                swap(r).wait_recv()

        for c in range(2):
            for b in range(2):
                row = jnp.where(part == 0, mine, theirs) + b * BQ
                project_k(c, a_loc, row, chip * CHIP + row, row)

    lax.fori_loop(0, 2, local_k, None)

    def local_v(c, _):
        w_wait(2 + c)
        for b in range(CHIP // BQ):
            project_v(c, a_loc, b * BQ, b * BQ)

    lax.fori_loop(0, 2, local_v, None)

    def local_q(c, _):
        w_wait(q_slot(c))
        pl.when(early)(lambda: project_q(c, 0))
        for b in range(1, CHIP // BQ):
            project_q(c, b * BQ)
        pl.when((c == 0) | early)(q_copy(c + 3).start)

        @pl.when((c == 1) & (sp == 0))
        def _():
            for r in range(2):
                back(r).wait_recv()
                hand_moved(r).start()

    lax.fori_loop(0, 4, local_q, None)

    @pl.when(early)
    def _():
        @pl.when(core == 1)
        def _():
            for r in range(2):
                hand_moved(r).wait_recv()

        def moved_q(c, _):
            w_wait(q_slot(c))
            project_q(c, CHIP)
            pl.when(c == 4)(q_copy(7).start)

        lax.fori_loop(4, 8, moved_q, None)
        for c in range(2):
            project_k(c, a_loc, CHIP, CHIP, CHIP)
            project_v(c, a_loc, CHIP, CHIP)
        for u in range(2, 6):
            o_copy(u).start()

    for u in (0, 1, 6):
        o_copy(u).start()

    e = HEAD**-0.5 * LOG2E
    cols = GROUP * BQ

    def block(iq, state, at, size, ahead=None):
        here, queries = _rows(at, size), _rows(iq * BQ, BQ)
        ones = jnp.ones((8, size), v.dtype)
        begin = ahead is not None
        if begin:
            ok = lax.rem(lax.broadcasted_iota(jnp.int32, (size, cols), 1), BQ) + ahead >= lax.broadcasted_iota(jnp.int32, (size, cols), 0)

        def scores(h):
            return _dot(k[h, here, :], q[GROUP * h : GROUP * (h + 1), queries, :].reshape(cols, HEAD), 1, 1)

        def weights(h, s):
            if begin:
                s = jnp.where(ok, s, HIDDEN)
                new, keep = s.max(axis=0, keepdims=True), None
            else:
                old = top[state, h : h + 1, :]
                new = jnp.maximum(old, s.max(axis=0, keepdims=True))
                keep = jnp.exp2((old - new) * e)
            top[state, h : h + 1, :] = new
            return jnp.exp2((s - new) * e).astype(v.dtype), keep

        def add(h, p, keep):
            got = _dot(jnp.concatenate([v[h, :, here], ones], axis=0), p, 1, 0)
            mix[state, h] = got if begin else mix[state, h] * keep + got

        ready_s, ready_p = [scores(0), scores(1)], []
        for h in range(KV):
            if h + 2 < KV:
                ready_s.append(scores(h + 2))
            ready_p.append(weights(h, ready_s[h]))
            if h:
                add(h - 1, *ready_p[h - 1])
        add(KV - 1, *ready_p[-1])

    def finish(iq, state):
        for h in range(KV):
            out = (mix[state, h, :HEAD, :] * (1 / mix[state, h, HEAD : HEAD + 1, :])).astype(a_loc.dtype).T
            for n in range(GROUP):
                a_loc[_rows(iq * BQ, BQ), (GROUP * h + n) * HEAD : (GROUP * h + n + 1) * HEAD] = out[n * BQ : (n + 1) * BQ, :]

    def hand_on(r):
        @pl.when(late)
        def _():
            far(r).wait_recv()
            hand(r).start()

    def moved_output():
        seen_more().wait_recv()
        x_back(0).wait_recv()

        def output(n, _):
            u = 2 * n
            for i in range(2):
                w_wait(o_slot(u + i))
            t = project(a_loc, CHIP + core * PIECE, o_slot(u), PIECE) + project(a_far, ROWS, o_slot(u + 1), PIECE)
            here = _rows(n * COLS, COLS)
            ym[:, here] = (xm[:, here].astype(jnp.float32) + t).astype(ym.dtype)
            for i in range(2):
                o_copy(u + i + SLOTS).start()

        lax.fori_loop(0, 4, output, None)

    hand_on(0)

    def far_project(half):
        def part(i, _):
            c = jnp.where(i == 0, core, 1 - core)

            @pl.when(i == 1)
            def _():
                for r in range(2):
                    hand(2 * half + r).wait_recv()

            row = half * ROWS + c * BQ
            for n in range(2):
                project_k(n, a_far, row, c * ROWS + half * BQ, CHIP + row)
                project_v(n, a_far, row, CHIP + row)

        lax.fori_loop(0, 2, part, None)

    def step(s, _):
        far_step = late & (s >= 3)
        half, i = lax.div(s, 3) - 1, lax.rem(s, 3)
        iq_early = jnp.where(s == 0, 4, lax.rem((1 - core) * 2 + s + 3, 4))
        iq_late = jnp.where(s < 3, s + 1, 1 + lax.rem(i + 1 - core, 3))
        iq = jnp.where(early, iq_early, iq_late)
        state = jnp.where(early, 0, iq - 1)
        p = lax.div(iq, 2)

        pl.when(far_step & (i == 0))(lambda: far_project(half))

        @pl.when(late & (s == 6))
        def _():
            for r in range(4):
                hand(r).wait_send()
            pl.semaphore_signal(ready, inc=1, device_id=partner, device_id_type=MESH)
            for u in range(2, 6):
                o_copy(u).start()

        @pl.when((late & (s == 6)) | (early & (s == 3)))
        def _():
            for r in range(4):
                swap(r).wait_send()
                pl.when(early)(far(r).wait_send)

        @pl.when(late & (s == 7))
        def _():
            pl.semaphore_wait(ready, 1)
            pl.when(core == 0)(seen(0).start)
            pl.when(core == 1)(seen(1).start)

        @pl.when(late & (s == 8))
        def _():
            pl.when(core == 0)(seen(1).start)
            pl.when(core == 1)(seen_more().start)

        even = lax.rem(iq, 2) == 0
        pl.when(jnp.logical_not(far_step) & even)(lambda: block(iq, state, p * BK, BQ, 0))
        pl.when(jnp.logical_not(far_step) & jnp.logical_not(even))(lambda: block(iq, state, p * BK, BK, BQ))

        @pl.when(early)
        def _():
            pl.when(s == 1)(seen_more().start)
            pl.when(s == 2)(seen(0).start)
            pl.when(s == 3)(seen(1).start)

        start = jnp.where(far_step, CHIP + half * BK, 0)
        lax.fori_loop(0, jnp.where(far_step, 1, p), lambda j, _: block(iq, state, start + j * BK, BK), None)

        @pl.when((s == 0) & (sp == 0))
        def _():
            for r in range(2):
                hand_moved(r).wait_send()

        pl.when(early | (s >= 6))(lambda: finish(iq, state))

        @pl.when(early)
        def _():
            pl.when(s == 1 + core)(moved_output)
            pl.when(s == 2 + core)(y_back(core).start)

        for at, r in ((1, 1), (3, 2), (5, 3)):
            pl.when(s == at)(functools.partial(hand_on, r))

    lax.fori_loop(0, jnp.where(early, 5, 9), step, None)

    pl.when(sp != 2)(seen(0).wait_recv)
    seen(1).wait_recv()

    @pl.when(sp == 2)
    def _():
        seen_more().wait_recv()
        x_share().wait_recv()

    begin = jnp.where(early, 8, 0)

    def output(n, _):
        u = begin + 2 * n
        for i in range(2):
            w_wait(o_slot(u + i))
        here = _rows(n * COLS, COLS)

        def both(own, other, rows):
            return project(a_loc, own, o_slot(u), rows) + project(a_far, other, o_slot(u + 1), rows)

        def part(row, rows):
            which = pl.ds(row, rows)
            y[which, here] = (xbuf[which, here].astype(jnp.float32) + both(mine + row, row, rows)).astype(y.dtype)

        @pl.when(early)
        def _():
            part(0, BQ)
            part(BQ, BQ)

        @pl.when(sp == 3)
        def _():
            part(PIECE, PIECE)
            part(BQ, BQ)

        @pl.when(sp == 2)
        def _():
            ym[:, here] = (xm[:, here].astype(jnp.float32) + both(ROWS, ROWS, PIECE)).astype(ym.dtype)

        @pl.when(sp == 2)
        def _():
            y_share(n).start()
            part(BQ, BQ)

        pl.when(n == 0)(o_copy(u + SLOTS).start)

    lax.fori_loop(0, 4, output, None)
    pl.when(sp != 3)(seen(0).wait_send)
    seen(1).wait_send()
    pl.when(sp != 2)(seen_more().wait_send)
    pl.when(early)(y_back(core).wait_send)

    @pl.when(giver)
    def _():
        for c in range(2):
            back(c).wait_send()
            x_back(c).wait_send()
            y_back(c).wait_recv()
        for n in range(4):
            y_share(n).wait_send()

    @pl.when(sp == 3)
    def _():
        x_share().wait_send()
        for n in range(4):
            y_share(n).wait_recv()


def rotary():
    half = HEAD // 2
    places = np.arange(2 * CHIP, dtype=np.float32)
    angle = places[:, None] * (np.float32(THETA) ** (-np.arange(half, dtype=np.float32) / np.float32(half)))
    return np.concatenate([np.cos(angle.astype(np.float64)), np.sin(angle.astype(np.float64))], -1).astype(np.float32)


def solution(mesh):
    def step(x, gain, wq, wk, wv, wo):
        bf, f32 = jnp.bfloat16, jnp.float32
        dma = pltpu.SemaphoreType.DMA
        hbm = pl.BlockSpec(memory_space=pl.ANY)
        return pl.pallas_call(
            _kernel,
            out_shape=pltpu.VMEM(x.shape, x.dtype),
            in_specs=[hbm, pl.BlockSpec(memory_space=pltpu.VMEM), *[hbm] * 5],
            out_specs=pl.BlockSpec(memory_space=pltpu.VMEM),
            scratch_shapes=[
                pltpu.VMEM((CHIP + MOVED, DEPTH), bf),
                pltpu.VMEM((CHIP, DEPTH), bf),
                pltpu.VMEM((GROUP * KV, CHIP + MOVED, HEAD), bf),
                pltpu.VMEM((KV, 2 * CHIP, HEAD), bf),
                pltpu.VMEM((KV, HEAD, 2 * CHIP), bf),
                pltpu.VMEM((3, KV, GROUP * BQ), f32),
                pltpu.VMEM((3, KV, HEAD + 8, GROUP * BQ), f32),
                pltpu.VMEM((SLOTS, DEPTH, COLS), bf),
                pltpu.VMEM((ROWS, DEPTH), bf),
                pltpu.VMEM((2 * CHIP, HEAD), f32),
                pltpu.VMEM((PIECE, DEPTH), bf),
                pltpu.VMEM((PIECE, DEPTH), bf),
                dma((4,)), dma, dma((SLOTS,)),
                *[dma((4,))] * 6, dma((3,)), dma((3,)),
                dma((2,)), dma((2,)), dma((2,)), dma, dma, dma((2,)), dma((4,)), dma((4,)),
                pltpu.SemaphoreType.REGULAR,
            ],
            compiler_params=pltpu.CompilerParams(collective_id=0, has_side_effects=True, vmem_limit_bytes=VMEM),
            name="layer",
        )(x, gain, jnp.asarray(rotary()), wq, wk, wv, wo)

    tokens, whole = P(("dp", "sp"), None), P(None, None)
    return jax.shard_map(
        step,
        mesh=mesh,
        in_specs=(tokens, P(None), whole, whole, whole, whole),
        out_specs=tokens,
        check_vma=False,
    )
```

```python
import functools

import jax
import jax.numpy as jnp
import numpy as np
from jax import lax
from jax.experimental import pallas as pl
from jax.experimental.pallas import tpu as pltpu
from jax.sharding import PartitionSpec as P

HIDDEN = -jnp.inf
LOG2E = 1.4426950408889634
VMEM = 61 * 2**20
HEAD = 128
THETA = 10000

ROWS = 512
CHIP = 1024
DEPTH = 2048
COLS = 512
KV = 8
GROUP = 2
BQ = 256
BK = 512
PIECE = 128
MOVED = 256
SLOTS = 7

MESH = pl.DeviceIdType.MESH


def _dot(a, b, ca, cb):
    return lax.dot_general(a, b, (((ca,), (cb,)), ((), ())), preferred_element_type=jnp.float32)


def _rows(start, size):
    return pl.ds(pl.multiple_of(start, size), size)


def _kernel(x, gain, table, wq, wk, wv, wo, y, a_loc, a_far, q, k, v, top, mix, wbuf, xbuf, tab, xm, ym,
            x_sem, tab_sem, w_sem, swap_out, swap_in, far_out, far_in, pass_out, pass_in, seen_out, seen_in,
            back_out, back_in, xb_out, xb_in, yb_out, yb_in, share_out, share_in, ready):
    sp = lax.axis_index("sp")
    core, chip = lax.rem(sp, 2), lax.div(sp, 2)
    early, late = chip == 0, chip == 1
    giver = sp == 2
    partner, across = {"sp": chip * 2 + 1 - core}, {"sp": (1 - chip) * 2 + core}
    mine, theirs = core * ROWS, (1 - core) * ROWS
    kv_cols = KV * HEAD
    q_cols = GROUP * kv_cols

    def x_copy(r):
        return pltpu.make_async_copy(x.at[pl.ds(r * PIECE, PIECE)], xbuf.at[pl.ds(r * PIECE, PIECE)], x_sem.at[r])

    def w_copy(w, row, column, slot):
        return pltpu.make_async_copy(w.at[_rows(row, DEPTH), _rows(column, COLS)], wbuf.at[slot], w_sem.at[slot])

    def q_slot(c):
        return 4 + lax.rem(c, 3)

    def q_copy(c):
        return w_copy(wq, 0, core * q_cols + lax.rem(c, 4) * COLS, q_slot(c))

    def o_slot(u):
        return lax.rem(5 + u, SLOTS)

    def o_copy(u):
        return w_copy(wo, jnp.where(lax.rem(u, 2) == 0, core, 1 - core) * DEPTH, lax.div(lax.rem(u, 8), 2) * COLS, o_slot(u))

    def w_wait(slot):
        pltpu.make_async_copy(wq.at[pl.ds(0, DEPTH), pl.ds(0, COLS)], wbuf.at[slot], w_sem.at[slot]).wait()

    def remote(src, dst, out, got, device):
        return pltpu.make_async_remote_copy(src_ref=src, dst_ref=dst, send_sem=out, recv_sem=got, device_id=device, device_id_type=MESH)

    def swap(r):
        rows = a_loc.at[_rows(mine + r * PIECE, PIECE)]
        return remote(rows, rows, swap_out.at[r], swap_in.at[r], partner)

    def far_rows(c, r):
        return a_far.at[_rows((2 * r + c) * PIECE, PIECE)]

    def far(r):
        return remote(a_loc.at[_rows(mine + r * PIECE, PIECE)], far_rows(core, r), far_out.at[r], far_in.at[r], across)

    def hand(r):
        return remote(far_rows(core, r), far_rows(core, r), pass_out.at[r], pass_in.at[r], partner)

    def moved_rows(r):
        return a_loc.at[pl.ds(CHIP + r * PIECE, PIECE)]

    def back(r):
        return remote(a_loc.at[pl.ds(r * PIECE, PIECE)], moved_rows(r), back_out.at[r], back_in.at[r], {"sp": 0})

    def hand_moved(r):
        return remote(moved_rows(r), moved_rows(r), pass_out.at[r], pass_in.at[r], partner)

    def x_back(c):
        return remote(xbuf.at[pl.ds(c * PIECE, PIECE)], xm, xb_out.at[c], xb_in, {"sp": c})

    def y_back(c):
        return remote(ym, y.at[_rows(c * PIECE, PIECE)], yb_out, yb_in.at[c], {"sp": 2})

    def seen(i):
        return remote(a_loc.at[_rows(theirs + i * BQ, BQ)], a_far.at[pl.ds(i * BQ, BQ)], seen_out.at[i], seen_in.at[i], partner)

    def seen_more():
        rows = a_loc.at[_rows(jnp.where(early, CHIP + (1 - core) * PIECE, ROWS), PIECE)]
        return remote(rows, a_far.at[pl.ds(ROWS, PIECE)], seen_out.at[2], seen_in.at[2], partner)

    def x_share():
        return remote(xbuf.at[pl.ds(0, PIECE)], xm, xb_out.at[0], xb_in, {"sp": 2})

    def y_share(n):
        here = _rows(n * COLS, COLS)
        return remote(ym.at[:, here], y.at[pl.ds(0, PIECE), here], share_out.at[n], share_in.at[n], {"sp": 3})

    for r in range(4):
        x_copy(r).start()
    table_copy = pltpu.make_async_copy(table, tab, tab_sem)

    barrier = pltpu.get_barrier_semaphore()
    for other in range(1, 4):
        pl.semaphore_signal(barrier, inc=1, device_id={"sp": lax.rem(sp + other, 4)}, device_id_type=MESH)

    for r in range(4):
        x_copy(r).wait()
        if r == 1:
            w_copy(wk, 0, core * kv_cols, 0).start()
        if r == 3:
            table_copy.start()
            w_copy(wk, 0, core * kv_cols + COLS, 1).start()
        wide = xbuf[r * PIECE : (r + 1) * PIECE, :].astype(jnp.float32)
        scale = lax.rsqrt(jnp.mean(wide * wide, -1, keepdims=True) + 1e-6)
        a_loc[_rows(mine + r * PIECE, PIECE), :] = (wide * scale * gain[...].astype(jnp.float32)[None, :]).astype(a_loc.dtype)

    pl.semaphore_wait(barrier, 3)
    for r in range(4):
        pl.when(early)(far(r).start)
        swap(r).start()
        if r < 2:
            pl.when(giver)(back(r).start)
    for c in range(2):
        w_copy(wv, 0, core * kv_cols + c * COLS, 2 + c).start()
    table_copy.wait()
    pl.when(sp == 3)(x_share().start)

    @pl.when(giver)
    def _():
        for c in range(2):
            x_back(c).start()

    def turned(t, *places):
        rows = t.shape[0] // len(places)
        both = jnp.concatenate([tab[_rows(place, rows), :] for place in places], axis=0)
        back = pltpu.roll(both, HEAD // 2, 1)
        first = lax.broadcasted_iota(jnp.int32, both.shape, 1) < HEAD // 2
        cos, sin = jnp.where(first, both, back), jnp.where(first, -back, both)
        t = t.astype(q.dtype).astype(jnp.float32)
        for h in range(COLS // HEAD):
            part = t[:, h * HEAD : (h + 1) * HEAD]
            yield h, (part * cos + pltpu.roll(part, HEAD // 2, 1) * sin).astype(q.dtype)

    def project(a, row, slot, rows=BQ):
        return jnp.dot(a[_rows(row, rows), :], wbuf[slot], preferred_element_type=jnp.float32)

    def project_q(c, row):
        for h, t in turned(project(a_loc, row, q_slot(c)), chip * CHIP + row):
            q[lax.rem(c, 4) * 4 + h, _rows(row, BQ), :] = t

    def project_k(c, a, row, key, *places):
        for h, t in turned(project(a, row, c), *places):
            k[c * 4 + h, _rows(key, BQ), :] = t

    def project_v(c, a, row, key):
        t = project(a, row, 2 + c).astype(v.dtype)
        for h in range(COLS // HEAD):
            v[c * 4 + h, :, _rows(key, BQ)] = t[:, h * HEAD : (h + 1) * HEAD].T

    for c in range(2):
        w_wait(c)

    def local_kv(part, _):
        @pl.when(part == 1)
        def _():
            for r in range(4):
                swap(r).wait_recv()

        rows = [jnp.where(part == 0, mine, theirs) + b * BQ for b in range(2)]
        for c in range(2):
            for row in rows:
                project_k(c, a_loc, row, row, chip * CHIP + row)

        @pl.when(part == 0)
        def _():
            for c in range(2):
                w_wait(2 + c)
            for c in range(3):
                q_copy(c).start()

        for c in range(2):
            for row in rows:
                project_v(c, a_loc, row, row)

    lax.fori_loop(0, 2, local_kv, None)

    def local_q(c, _):
        w_wait(q_slot(c))

        @pl.when(early)
        def _():
            for b in range(CHIP // BQ):
                project_q(c, b * BQ)

        @pl.when(late)
        def _():
            for b in range(1, CHIP // BQ):
                project_q(c, b * BQ)

        pl.when((c == 0) | early)(q_copy(c + 3).start)

        @pl.when((c == 1) & (sp == 0))
        def _():
            for r in range(2):
                back(r).wait_recv()
                hand_moved(r).start()

    lax.fori_loop(0, 4, local_q, None)

    @pl.when(early)
    def _():
        @pl.when(core == 1)
        def _():
            for r in range(2):
                hand_moved(r).wait_recv()

        def moved_q(c, _):
            w_wait(q_slot(c))
            project_q(c, CHIP)
            pl.when(c == 4)(q_copy(7).start)

        lax.fori_loop(4, 8, moved_q, None)
        for c in range(2):
            project_k(c, a_loc, CHIP, CHIP, CHIP)
            project_v(c, a_loc, CHIP, CHIP)
        for u in range(2, 6):
            o_copy(u).start()

    for u in (0, 1, 6):
        o_copy(u).start()

    e = HEAD**-0.5 * LOG2E
    cols = GROUP * BQ

    def block(iq, state, at, size, ahead=None):
        here, queries = _rows(at, size), _rows(iq * BQ, BQ)
        ones = jnp.ones((8, size), v.dtype)
        begin = ahead is not None
        if begin:
            ok = lax.rem(lax.broadcasted_iota(jnp.int32, (size, cols), 1), BQ) + ahead >= lax.broadcasted_iota(jnp.int32, (size, cols), 0)

        def scores(h):
            return _dot(k[h, here, :], q[GROUP * h : GROUP * (h + 1), queries, :].reshape(cols, HEAD), 1, 1)

        def weights(h, s):
            if begin:
                s = jnp.where(ok, s, HIDDEN)
                new, keep = s.max(axis=0, keepdims=True), None
            else:
                old = top[state, h : h + 1, :]
                new = jnp.maximum(old, s.max(axis=0, keepdims=True))
                keep = jnp.exp2((old - new) * e)
            top[state, h : h + 1, :] = new
            return jnp.exp2((s - new) * e).astype(v.dtype), keep

        def add(h, p, keep):
            got = _dot(jnp.concatenate([v[h, :, here], ones], axis=0), p, 1, 0)
            mix[state, h] = got if begin else mix[state, h] * keep + got

        ready_s, ready_p = [scores(0), scores(1)], []
        for h in range(KV):
            if h + 2 < KV:
                ready_s.append(scores(h + 2))
            ready_p.append(weights(h, ready_s[h]))
            if h:
                add(h - 1, *ready_p[h - 1])
        add(KV - 1, *ready_p[-1])

    def finish(iq, state):
        for h in range(KV):
            out = (mix[state, h, :HEAD, :] * (1 / mix[state, h, HEAD : HEAD + 1, :])).astype(a_loc.dtype).T
            for n in range(GROUP):
                a_loc[_rows(iq * BQ, BQ), (GROUP * h + n) * HEAD : (GROUP * h + n + 1) * HEAD] = out[n * BQ : (n + 1) * BQ, :]

    def hand_on(r):
        @pl.when(late)
        def _():
            far(r).wait_recv()
            hand(r).start()

    def moved_output():
        seen_more().wait_recv()
        x_back(0).wait_recv()

        def output(n, _):
            u = 2 * n
            for i in range(2):
                w_wait(o_slot(u + i))
            t = project(a_loc, CHIP + core * PIECE, o_slot(u), PIECE) + project(a_far, ROWS, o_slot(u + 1), PIECE)
            here = _rows(n * COLS, COLS)
            ym[:, here] = (xm[:, here].astype(jnp.float32) + t).astype(ym.dtype)
            for i in range(2):
                o_copy(u + i + SLOTS).start()

        lax.fori_loop(0, 4, output, None)

    hand_on(0)

    def far_project(half):
        def part(i, _):
            r = 2 * half + i
            for at in range(4):
                pl.when(r == at)(hand(at).wait_recv)
            row = 2 * r * PIECE
            for n in range(2):
                project_k(n, a_far, row, CHIP + row, r * PIECE, ROWS + r * PIECE)
            pl.when(r == 2)(lambda: hand_on(3))
            for n in range(2):
                project_v(n, a_far, row, CHIP + row)

        lax.fori_loop(0, 2, part, None)

    def step(s, _):
        far_step = late & (s >= 3)
        half, i = lax.div(s, 3) - 1, lax.rem(s, 3)
        iq_early = jnp.where(s == 0, 4, lax.rem((1 - core) * 2 + s + 3, 4))
        iq_late = jnp.where(s < 3, s + 1, 1 + lax.rem(i + 1 - core, 3))
        iq = jnp.where(early, iq_early, iq_late)
        state = jnp.where(early, 0, iq - 1)
        p = lax.div(iq, 2)

        pl.when(far_step & (i == 0))(lambda: far_project(half))

        @pl.when(late & (s == 6))
        def _():
            for r in range(4):
                hand(r).wait_send()
            pl.semaphore_signal(ready, inc=1, device_id=partner, device_id_type=MESH)
            for u in range(2, 6):
                o_copy(u).start()

        @pl.when((late & (s == 6)) | (early & (s == 3)))
        def _():
            for r in range(4):
                swap(r).wait_send()
                pl.when(early)(far(r).wait_send)

        @pl.when(late & (s == 7))
        def _():
            pl.semaphore_wait(ready, 1)
            pl.when(core == 0)(seen(0).start)
            pl.when(core == 1)(seen(1).start)

        @pl.when(late & (s == 8))
        def _():
            pl.when(core == 0)(seen(1).start)
            pl.when(core == 1)(seen_more().start)

        even = lax.rem(iq, 2) == 0
        pl.when(jnp.logical_not(far_step) & even)(lambda: block(iq, state, p * BK, BQ, 0))
        pl.when(jnp.logical_not(far_step) & jnp.logical_not(even))(lambda: block(iq, state, p * BK, BK, BQ))

        @pl.when(early)
        def _():
            pl.when(s == 1)(seen_more().start)
            pl.when(s == 2)(seen(0).start)
            pl.when(s == 3)(seen(1).start)

        start = jnp.where(far_step, CHIP + half * BK, 0)
        lax.fori_loop(0, jnp.where(far_step, 1, p), lambda j, _: block(iq, state, start + j * BK, BK), None)

        @pl.when((s == 0) & (sp == 0))
        def _():
            for r in range(2):
                hand_moved(r).wait_send()

        pl.when(early | (s >= 6))(lambda: finish(iq, state))

        @pl.when(early)
        def _():
            pl.when(s == 1 + core)(moved_output)
            pl.when(s == 2 + core)(y_back(core).start)

        for at, r in ((1, 1), (3, 2)):
            pl.when(s == at)(functools.partial(hand_on, r))

    lax.fori_loop(0, jnp.where(early, 5, 9), step, None)

    pl.when(sp != 2)(seen(0).wait_recv)
    seen(1).wait_recv()

    @pl.when(sp == 2)
    def _():
        seen_more().wait_recv()
        x_share().wait_recv()

    begin = jnp.where(early, 8, 0)

    def output(n, _):
        u = begin + 2 * n
        for i in range(2):
            w_wait(o_slot(u + i))
        here = _rows(n * COLS, COLS)

        def both(own, other, rows):
            return project(a_loc, own, o_slot(u), rows) + project(a_far, other, o_slot(u + 1), rows)

        def part(row, rows):
            which = pl.ds(row, rows)
            y[which, here] = (xbuf[which, here].astype(jnp.float32) + both(mine + row, row, rows)).astype(y.dtype)

        @pl.when(early)
        def _():
            part(0, BQ)
            part(BQ, BQ)

        @pl.when(sp == 3)
        def _():
            part(PIECE, PIECE)
            part(BQ, BQ)

        @pl.when(sp == 2)
        def _():
            ym[:, here] = (xm[:, here].astype(jnp.float32) + both(ROWS, ROWS, PIECE)).astype(ym.dtype)
            y_share(n).start()
            part(BQ, BQ)

        pl.when(n == 0)(o_copy(u + SLOTS).start)

    lax.fori_loop(0, 4, output, None)
    pl.when(sp != 3)(seen(0).wait_send)
    seen(1).wait_send()
    pl.when(sp != 2)(seen_more().wait_send)
    pl.when(early)(y_back(core).wait_send)

    @pl.when(giver)
    def _():
        for c in range(2):
            back(c).wait_send()
            x_back(c).wait_send()
            y_back(c).wait_recv()
        for n in range(4):
            y_share(n).wait_send()

    @pl.when(sp == 3)
    def _():
        x_share().wait_send()
        for n in range(4):
            y_share(n).wait_recv()


def rotary():
    half = HEAD // 2
    places = np.arange(2 * CHIP, dtype=np.float32)
    angle = places[:, None] * (np.float32(THETA) ** (-np.arange(half, dtype=np.float32) / np.float32(half)))
    return np.concatenate([np.cos(angle.astype(np.float64)), np.sin(angle.astype(np.float64))], -1).astype(np.float32)


def solution(mesh):
    def step(x, gain, wq, wk, wv, wo):
        bf, f32 = jnp.bfloat16, jnp.float32
        dma = pltpu.SemaphoreType.DMA
        hbm = pl.BlockSpec(memory_space=pl.ANY)
        return pl.pallas_call(
            _kernel,
            out_shape=pltpu.VMEM(x.shape, x.dtype),
            in_specs=[hbm, pl.BlockSpec(memory_space=pltpu.VMEM), *[hbm] * 5],
            out_specs=pl.BlockSpec(memory_space=pltpu.VMEM),
            scratch_shapes=[
                pltpu.VMEM((CHIP + MOVED, DEPTH), bf),
                pltpu.VMEM((CHIP, DEPTH), bf),
                pltpu.VMEM((GROUP * KV, CHIP + MOVED, HEAD), bf),
                pltpu.VMEM((KV, 2 * CHIP, HEAD), bf),
                pltpu.VMEM((KV, HEAD, 2 * CHIP), bf),
                pltpu.VMEM((3, KV, GROUP * BQ), f32),
                pltpu.VMEM((3, KV, HEAD + 8, GROUP * BQ), f32),
                pltpu.VMEM((SLOTS, DEPTH, COLS), bf),
                pltpu.VMEM((ROWS, DEPTH), bf),
                pltpu.VMEM((2 * CHIP, HEAD), f32),
                pltpu.VMEM((PIECE, DEPTH), bf),
                pltpu.VMEM((PIECE, DEPTH), bf),
                dma((4,)), dma, dma((SLOTS,)),
                *[dma((4,))] * 6, dma((3,)), dma((3,)),
                dma((2,)), dma((2,)), dma((2,)), dma, dma, dma((2,)), dma((4,)), dma((4,)),
                pltpu.SemaphoreType.REGULAR,
            ],
            compiler_params=pltpu.CompilerParams(collective_id=0, has_side_effects=True, vmem_limit_bytes=VMEM),
            name="layer",
        )(x, gain, jnp.asarray(rotary()), wq, wk, wv, wo)

    tokens, whole = P(("dp", "sp"), None), P(None, None)
    return jax.shard_map(
        step,
        mesh=mesh,
        in_specs=(tokens, P(None), whole, whole, whole, whole),
        out_specs=tokens,
        check_vma=False,
    )
```

```python
import functools

import jax
import jax.numpy as jnp
import numpy as np
from jax import lax
from jax.experimental import pallas as pl
from jax.experimental.pallas import tpu as pltpu
from jax.sharding import PartitionSpec as P

HIDDEN = -jnp.inf
LOG2E = 1.4426950408889634
VMEM = 61 * 2**20
HEAD = 128
THETA = 10000

ROWS = 512
CHIP = 1024
DEPTH = 2048
COLS = 512
KV = 8
GROUP = 2
BQ = 256
BK = 512
PIECE = 128
MOVED = 256
SLOTS = 7

MESH = pl.DeviceIdType.MESH


def _dot(a, b, ca, cb):
    return lax.dot_general(a, b, (((ca,), (cb,)), ((), ())), preferred_element_type=jnp.float32)


def _rows(start, size):
    return pl.ds(pl.multiple_of(start, size), size)


def _kernel(x, gain, table, wq, wk, wv, wo, y, a_loc, a_far, q, k, v, top, mix, wbuf, xbuf, tab, xm, ym,
            x_sem, tab_sem, w_sem, swap_out, swap_in, far_out, far_in, pass_out, pass_in, seen_out, seen_in,
            back_out, back_in, xb_out, xb_in, yb_out, yb_in, share_out, share_in, ready):
    sp = lax.axis_index("sp")
    core, chip = lax.rem(sp, 2), lax.div(sp, 2)
    early, late = chip == 0, chip == 1
    giver = sp == 2
    partner, across = {"sp": chip * 2 + 1 - core}, {"sp": (1 - chip) * 2 + core}
    mine, theirs = core * ROWS, (1 - core) * ROWS
    kv_cols = KV * HEAD
    q_cols = GROUP * kv_cols

    def x_copy(r):
        return pltpu.make_async_copy(x.at[pl.ds(r * PIECE, PIECE)], xbuf.at[pl.ds(r * PIECE, PIECE)], x_sem.at[r])

    def w_copy(w, row, column, slot):
        return pltpu.make_async_copy(w.at[_rows(row, DEPTH), _rows(column, COLS)], wbuf.at[slot], w_sem.at[slot])

    def q_slot(c):
        return 4 + lax.rem(c, 3)

    def q_copy(c):
        return w_copy(wq, 0, core * q_cols + lax.rem(c, 4) * COLS, q_slot(c))

    def o_slot(u):
        return lax.rem(5 + u, SLOTS)

    def o_copy(u):
        return w_copy(wo, jnp.where(lax.rem(u, 2) == 0, core, 1 - core) * DEPTH, lax.div(lax.rem(u, 8), 2) * COLS, o_slot(u))

    def w_wait(slot):
        pltpu.make_async_copy(wq.at[pl.ds(0, DEPTH), pl.ds(0, COLS)], wbuf.at[slot], w_sem.at[slot]).wait()

    def remote(src, dst, out, got, device):
        return pltpu.make_async_remote_copy(src_ref=src, dst_ref=dst, send_sem=out, recv_sem=got, device_id=device, device_id_type=MESH)

    def swap(r):
        rows = a_loc.at[_rows(mine + r * PIECE, PIECE)]
        return remote(rows, rows, swap_out.at[r], swap_in.at[r], partner)

    def far_rows(c, r):
        return a_far.at[_rows((2 * r + c) * PIECE, PIECE)]

    def far(r):
        return remote(a_loc.at[_rows(mine + r * PIECE, PIECE)], far_rows(core, r), far_out.at[r], far_in.at[r], across)

    def hand(r):
        return remote(far_rows(core, r), far_rows(core, r), pass_out.at[r], pass_in.at[r], partner)

    def moved_rows(r):
        return a_loc.at[pl.ds(CHIP + r * PIECE, PIECE)]

    def back(r):
        return remote(a_loc.at[pl.ds(r * PIECE, PIECE)], moved_rows(r), back_out.at[r], back_in.at[r], {"sp": 0})

    def hand_moved(r):
        return remote(moved_rows(r), moved_rows(r), pass_out.at[r], pass_in.at[r], partner)

    def x_back(c):
        return remote(xbuf.at[pl.ds(c * PIECE, PIECE)], xm, xb_out.at[c], xb_in, {"sp": c})

    def y_back(c):
        return remote(ym, y.at[_rows(c * PIECE, PIECE)], yb_out, yb_in.at[c], {"sp": 2})

    def seen(i):
        return remote(a_loc.at[_rows(theirs + i * BQ, BQ)], a_far.at[pl.ds(i * BQ, BQ)], seen_out.at[i], seen_in.at[i], partner)

    def seen_more():
        rows = a_loc.at[_rows(jnp.where(early, CHIP + (1 - core) * PIECE, ROWS), PIECE)]
        return remote(rows, a_far.at[pl.ds(ROWS, PIECE)], seen_out.at[2], seen_in.at[2], partner)

    def x_share():
        return remote(xbuf.at[pl.ds(0, PIECE)], xm, xb_out.at[0], xb_in, {"sp": 2})

    def y_share(n):
        here = _rows(n * COLS, COLS)
        return remote(ym.at[:, here], y.at[pl.ds(0, PIECE), here], share_out.at[n], share_in.at[n], {"sp": 3})

    for r in range(4):
        x_copy(r).start()
    w_copy(wk, 0, core * kv_cols, 0).start()

    def table_copy(j):
        rows = _rows(lax.rem(sp + j, 4) * ROWS, ROWS)
        return pltpu.make_async_copy(table.at[rows], tab.at[rows], tab_sem.at[j])

    table_copy(0).start()

    barrier = pltpu.get_barrier_semaphore()
    for other in range(1, 4):
        pl.semaphore_signal(barrier, inc=1, device_id={"sp": lax.rem(sp + other, 4)}, device_id_type=MESH)

    for r in range(4):
        x_copy(r).wait()
        if r == 1:
            w_copy(wk, 0, core * kv_cols + COLS, 1).start()
        wide = xbuf[r * PIECE : (r + 1) * PIECE, :].astype(jnp.float32)
        scale = lax.rsqrt(jnp.mean(wide * wide, -1, keepdims=True) + 1e-6)
        a_loc[_rows(mine + r * PIECE, PIECE), :] = (wide * scale * gain[...].astype(jnp.float32)[None, :]).astype(a_loc.dtype)

    pl.semaphore_wait(barrier, 3)
    for r in range(4):
        pl.when(early)(far(r).start)
        swap(r).start()
        if r < 2:
            pl.when(giver)(back(r).start)
    for j in range(1, 4):
        table_copy(j).start()
    pl.when(sp == 3)(x_share().start)

    @pl.when(giver)
    def _():
        for c in range(2):
            x_back(c).start()

    def turned(t, *places):
        rows = t.shape[0] // len(places)
        both = jnp.concatenate([tab[_rows(place, rows), :] for place in places], axis=0)
        back = pltpu.roll(both, HEAD // 2, 1)
        first = lax.broadcasted_iota(jnp.int32, both.shape, 1) < HEAD // 2
        cos, sin = jnp.where(first, both, back), jnp.where(first, -back, both)
        t = t.astype(q.dtype).astype(jnp.float32)
        for h in range(COLS // HEAD):
            part = t[:, h * HEAD : (h + 1) * HEAD]
            yield h, (part * cos + pltpu.roll(part, HEAD // 2, 1) * sin).astype(q.dtype)

    def project(a, row, slot, rows=BQ):
        return jnp.dot(a[_rows(row, rows), :], wbuf[slot], preferred_element_type=jnp.float32)

    def project_q(c, row):
        for h, t in turned(project(a_loc, row, q_slot(c)), chip * CHIP + row):
            q[lax.rem(c, 4) * 4 + h, _rows(row, BQ), :] = t

    def project_k(c, a, row, key, *places):
        for h, t in turned(project(a, row, c), *places):
            k[c * 4 + h, _rows(key, BQ), :] = t

    def project_v(c, a, row, key):
        t = project(a, row, 2 + c).astype(v.dtype)
        for h in range(COLS // HEAD):
            v[c * 4 + h, :, _rows(key, BQ)] = t[:, h * HEAD : (h + 1) * HEAD].T

    table_copy(0).wait()
    w_wait(0)
    for c in range(2):
        w_copy(wv, 0, core * kv_cols + c * COLS, 2 + c).start()

    def local_kv(part, _):
        @pl.when(part == 1)
        def _():
            for r in range(4):
                swap(r).wait_recv()
            for j in range(1, 4):
                table_copy(j).wait()

        rows = [jnp.where(part == 0, mine, theirs) + b * BQ for b in range(2)]
        for c in range(2):
            if c:
                pl.when(part == 0)(lambda: w_wait(1))
            for row in rows:
                project_k(c, a_loc, row, row, chip * CHIP + row)

        @pl.when(part == 0)
        def _():
            for c in range(2):
                w_wait(2 + c)
            for c in range(3):
                q_copy(c).start()

        for c in range(2):
            for row in rows:
                project_v(c, a_loc, row, row)

    lax.fori_loop(0, 2, local_kv, None)

    def local_q(c, _):
        w_wait(q_slot(c))

        @pl.when(early)
        def _():
            for b in range(CHIP // BQ):
                project_q(c, b * BQ)

        @pl.when(late)
        def _():
            for b in range(1, CHIP // BQ):
                project_q(c, b * BQ)

        pl.when((c == 0) | early)(q_copy(c + 3).start)

        @pl.when((c == 1) & (sp == 0))
        def _():
            for r in range(2):
                back(r).wait_recv()
                hand_moved(r).start()

    lax.fori_loop(0, 4, local_q, None)

    @pl.when(early)
    def _():
        @pl.when(core == 1)
        def _():
            for r in range(2):
                hand_moved(r).wait_recv()

        def moved_q(c, _):
            w_wait(q_slot(c))
            project_q(c, CHIP)
            pl.when(c == 4)(q_copy(7).start)

        lax.fori_loop(4, 8, moved_q, None)
        for c in range(2):
            project_k(c, a_loc, CHIP, CHIP, CHIP)
            project_v(c, a_loc, CHIP, CHIP)
        for u in range(2, 6):
            o_copy(u).start()

    for u in (0, 1, 6):
        o_copy(u).start()

    e = HEAD**-0.5 * LOG2E
    cols = GROUP * BQ

    def block(iq, state, at, size, ahead=None):
        here, queries = _rows(at, size), _rows(iq * BQ, BQ)
        ones = jnp.ones((8, size), v.dtype)
        begin = ahead is not None
        if begin:
            ok = lax.rem(lax.broadcasted_iota(jnp.int32, (size, cols), 1), BQ) + ahead >= lax.broadcasted_iota(jnp.int32, (size, cols), 0)

        def scores(h):
            return _dot(k[h, here, :], q[GROUP * h : GROUP * (h + 1), queries, :].reshape(cols, HEAD), 1, 1)

        def weights(h, s):
            if begin:
                s = jnp.where(ok, s, HIDDEN)
                new, keep = s.max(axis=0, keepdims=True), None
            else:
                old = top[state, h : h + 1, :]
                new = jnp.maximum(old, s.max(axis=0, keepdims=True))
                keep = jnp.exp2((old - new) * e)
            top[state, h : h + 1, :] = new
            return jnp.exp2((s - new) * e).astype(v.dtype), keep

        def add(h, p, keep):
            got = _dot(jnp.concatenate([v[h, :, here], ones], axis=0), p, 1, 0)
            mix[state, h] = got if begin else mix[state, h] * keep + got

        ready_s, ready_p = [scores(0), scores(1)], []
        for h in range(KV):
            if h + 2 < KV:
                ready_s.append(scores(h + 2))
            ready_p.append(weights(h, ready_s[h]))
            if h:
                add(h - 1, *ready_p[h - 1])
        add(KV - 1, *ready_p[-1])

    def finish(iq, state):
        for h in range(KV):
            out = (mix[state, h, :HEAD, :] * (1 / mix[state, h, HEAD : HEAD + 1, :])).astype(a_loc.dtype).T
            for n in range(GROUP):
                a_loc[_rows(iq * BQ, BQ), (GROUP * h + n) * HEAD : (GROUP * h + n + 1) * HEAD] = out[n * BQ : (n + 1) * BQ, :]

    def hand_on(r):
        @pl.when(late)
        def _():
            far(r).wait_recv()
            hand(r).start()

    def moved_output():
        seen_more().wait_recv()
        x_back(0).wait_recv()

        def output(n, _):
            u = 2 * n
            for i in range(2):
                w_wait(o_slot(u + i))
            t = project(a_loc, CHIP + core * PIECE, o_slot(u), PIECE) + project(a_far, ROWS, o_slot(u + 1), PIECE)
            here = _rows(n * COLS, COLS)
            ym[:, here] = (xm[:, here].astype(jnp.float32) + t).astype(ym.dtype)
            for i in range(2):
                o_copy(u + i + SLOTS).start()

        lax.fori_loop(0, 4, output, None)

    hand_on(0)

    def far_project(half):
        def part(i, _):
            r = 2 * half + i
            for at in range(4):
                pl.when(r == at)(hand(at).wait_recv)
            row = 2 * r * PIECE

            def keys_and_values(between=None):
                for n in range(2):
                    project_k(n, a_far, row, CHIP + row, r * PIECE, ROWS + r * PIECE)
                if between is not None:
                    between()
                for n in range(2):
                    project_v(n, a_far, row, CHIP + row)

            pl.when(r != 2)(keys_and_values)
            pl.when(r == 2)(lambda: keys_and_values(lambda: hand_on(3)))

        lax.fori_loop(0, 2, part, None)

    def step(s, _):
        far_step = late & (s >= 3)
        half, i = lax.div(s, 3) - 1, lax.rem(s, 3)
        iq_early = jnp.where(s == 0, 4, lax.rem((1 - core) * 2 + s + 3, 4))
        iq_late = jnp.where(s < 3, s + 1, 1 + lax.rem(i + 1 - core, 3))
        iq = jnp.where(early, iq_early, iq_late)
        state = jnp.where(early, 0, iq - 1)
        p = lax.div(iq, 2)

        pl.when(far_step & (i == 0))(lambda: far_project(half))

        @pl.when(late & (s == 6))
        def _():
            for r in range(4):
                hand(r).wait_send()
            pl.semaphore_signal(ready, inc=1, device_id=partner, device_id_type=MESH)
            for u in range(2, 6):
                o_copy(u).start()

        @pl.when((late & (s == 6)) | (early & (s == 3)))
        def _():
            for r in range(4):
                swap(r).wait_send()
                pl.when(early)(far(r).wait_send)

        @pl.when(late & (s == 7))
        def _():
            pl.semaphore_wait(ready, 1)
            pl.when(core == 0)(seen(0).start)
            pl.when(core == 1)(seen(1).start)

        @pl.when(late & (s == 8))
        def _():
            pl.when(core == 0)(seen(1).start)
            pl.when(core == 1)(seen_more().start)

        even = lax.rem(iq, 2) == 0
        pl.when(jnp.logical_not(far_step) & even)(lambda: block(iq, state, p * BK, BQ, 0))
        pl.when(jnp.logical_not(far_step) & jnp.logical_not(even))(lambda: block(iq, state, p * BK, BK, BQ))

        @pl.when(early)
        def _():
            pl.when(s == 1)(seen_more().start)
            pl.when(s == 2)(seen(0).start)
            pl.when(s == 3)(seen(1).start)

        start = jnp.where(far_step, CHIP + half * BK, 0)
        lax.fori_loop(0, jnp.where(far_step, 1, p), lambda j, _: block(iq, state, start + j * BK, BK), None)

        @pl.when((s == 0) & (sp == 0))
        def _():
            for r in range(2):
                hand_moved(r).wait_send()

        pl.when(early | (s >= 6))(lambda: finish(iq, state))

        @pl.when(early)
        def _():
            pl.when(s == 1 + core)(moved_output)
            pl.when(s == 2 + core)(y_back(core).start)

        for at, r in ((1, 1), (3, 2)):
            pl.when(s == at)(functools.partial(hand_on, r))

    lax.fori_loop(0, jnp.where(early, 5, 9), step, None)

    pl.when(sp != 2)(seen(0).wait_recv)
    seen(1).wait_recv()

    @pl.when(sp == 2)
    def _():
        seen_more().wait_recv()
        x_share().wait_recv()

    begin = jnp.where(early, 8, 0)

    def output(n, _):
        u = begin + 2 * n
        for i in range(2):
            w_wait(o_slot(u + i))
        here = _rows(n * COLS, COLS)

        def both(own, other, rows):
            return project(a_loc, own, o_slot(u), rows) + project(a_far, other, o_slot(u + 1), rows)

        def part(row, rows):
            which = pl.ds(row, rows)
            y[which, here] = (xbuf[which, here].astype(jnp.float32) + both(mine + row, row, rows)).astype(y.dtype)

        @pl.when(early)
        def _():
            part(0, BQ)
            part(BQ, BQ)

        @pl.when(sp == 3)
        def _():
            part(PIECE, PIECE)
            part(BQ, BQ)

        @pl.when(sp == 2)
        def _():
            ym[:, here] = (xm[:, here].astype(jnp.float32) + both(ROWS, ROWS, PIECE)).astype(ym.dtype)
            y_share(n).start()
            part(BQ, BQ)

        pl.when(n == 0)(o_copy(u + SLOTS).start)

    lax.fori_loop(0, 4, output, None)
    pl.when(sp != 3)(seen(0).wait_send)
    seen(1).wait_send()
    pl.when(sp != 2)(seen_more().wait_send)
    pl.when(early)(y_back(core).wait_send)

    @pl.when(giver)
    def _():
        for c in range(2):
            back(c).wait_send()
            x_back(c).wait_send()
            y_back(c).wait_recv()
        for n in range(4):
            y_share(n).wait_send()

    @pl.when(sp == 3)
    def _():
        x_share().wait_send()
        for n in range(4):
            y_share(n).wait_recv()


def rotary():
    half = HEAD // 2
    places = np.arange(2 * CHIP, dtype=np.float32)
    angle = places[:, None] * (np.float32(THETA) ** (-np.arange(half, dtype=np.float32) / np.float32(half)))
    return np.concatenate([np.cos(angle.astype(np.float64)), np.sin(angle.astype(np.float64))], -1).astype(np.float32)


def solution(mesh):
    def step(x, gain, wq, wk, wv, wo):
        bf, f32 = jnp.bfloat16, jnp.float32
        dma = pltpu.SemaphoreType.DMA
        hbm = pl.BlockSpec(memory_space=pl.ANY)
        return pl.pallas_call(
            _kernel,
            out_shape=pltpu.VMEM(x.shape, x.dtype),
            in_specs=[hbm, pl.BlockSpec(memory_space=pltpu.VMEM), *[hbm] * 5],
            out_specs=pl.BlockSpec(memory_space=pltpu.VMEM),
            scratch_shapes=[
                pltpu.VMEM((CHIP + MOVED, DEPTH), bf),
                pltpu.VMEM((CHIP, DEPTH), bf),
                pltpu.VMEM((GROUP * KV, CHIP + MOVED, HEAD), bf),
                pltpu.VMEM((KV, 2 * CHIP, HEAD), bf),
                pltpu.VMEM((KV, HEAD, 2 * CHIP), bf),
                pltpu.VMEM((3, KV, GROUP * BQ), f32),
                pltpu.VMEM((3, KV, HEAD + 8, GROUP * BQ), f32),
                pltpu.VMEM((SLOTS, DEPTH, COLS), bf),
                pltpu.VMEM((ROWS, DEPTH), bf),
                pltpu.VMEM((2 * CHIP, HEAD), f32),
                pltpu.VMEM((PIECE, DEPTH), bf),
                pltpu.VMEM((PIECE, DEPTH), bf),
                dma((4,)), dma((4,)), dma((SLOTS,)),
                *[dma((4,))] * 6, dma((3,)), dma((3,)),
                dma((2,)), dma((2,)), dma((2,)), dma, dma, dma((2,)), dma((4,)), dma((4,)),
                pltpu.SemaphoreType.REGULAR,
            ],
            compiler_params=pltpu.CompilerParams(collective_id=0, has_side_effects=True, vmem_limit_bytes=VMEM),
            name="layer",
        )(x, gain, jnp.asarray(rotary()), wq, wk, wv, wo)

    tokens, whole = P(("dp", "sp"), None), P(None, None)
    return jax.shard_map(
        step,
        mesh=mesh,
        in_specs=(tokens, P(None), whole, whole, whole, whole),
        out_specs=tokens,
        check_vma=False,
    )
```

```python
import functools

import jax
import jax.numpy as jnp
import numpy as np
from jax import lax
from jax.experimental import pallas as pl
from jax.experimental.pallas import tpu as pltpu
from jax.sharding import PartitionSpec as P

HIDDEN = -jnp.inf
LOG2E = 1.4426950408889634
VMEM = 61 * 2**20
HEAD = 128
THETA = 10000

ROWS = 512
CHIP = 1024
DEPTH = 2048
COLS = 512
KV = 8
GROUP = 2
BQ = 256
BK = 512
PIECE = 128
MOVED = 256
SLOTS = 8
NEAR, FAR = 32, 64

MESH = pl.DeviceIdType.MESH


def _dot(a, b, ca, cb):
    return lax.dot_general(a, b, (((ca,), (cb,)), ((), ())), preferred_element_type=jnp.float32)


def _rows(start, size):
    return pl.ds(pl.multiple_of(start, size), size)


def _kernel(x, gain, table, wq, wk, wv, wo, y, a_loc, a_far, q, k, v, top, mix, wbuf, xbuf, tab, factors, xm, ym,
            x_sem, tab_sem, w_sem, swap_out, swap_in, far_out, far_in, pass_out, pass_in, seen_out, seen_in,
            back_out, back_in, xb_out, xb_in, yb_out, yb_in, share_out, share_in, ready):
    sp = lax.axis_index("sp")
    core, chip = lax.rem(sp, 2), lax.div(sp, 2)
    early, late = chip == 0, chip == 1
    giver = sp == 2
    partner, across = {"sp": chip * 2 + 1 - core}, {"sp": (1 - chip) * 2 + core}
    mine, theirs = core * ROWS, (1 - core) * ROWS
    kv_cols = KV * HEAD
    q_cols = GROUP * kv_cols

    def x_copy(r):
        return pltpu.make_async_copy(x.at[pl.ds(r * PIECE, PIECE)], xbuf.at[pl.ds(r * PIECE, PIECE)], x_sem.at[r])

    def w_copy(w, row, column, slot):
        return pltpu.make_async_copy(w.at[_rows(row, DEPTH), _rows(column, COLS)], wbuf.at[slot], w_sem.at[slot])

    def q_slot(c):
        return 4 + lax.rem(c, 4)

    def q_copy(c):
        return w_copy(wq, 0, core * q_cols + lax.rem(c, 4) * COLS, q_slot(c))

    def o_slot(u):
        return lax.rem(4 + u, SLOTS)

    def o_copy(u):
        return w_copy(wo, jnp.where(lax.rem(u, 2) == 0, core, 1 - core) * DEPTH, lax.div(lax.rem(u, 8), 2) * COLS, o_slot(u))

    def w_wait(slot):
        pltpu.make_async_copy(wq.at[pl.ds(0, DEPTH), pl.ds(0, COLS)], wbuf.at[slot], w_sem.at[slot]).wait()

    def remote(src, dst, out, got, device):
        return pltpu.make_async_remote_copy(src_ref=src, dst_ref=dst, send_sem=out, recv_sem=got, device_id=device, device_id_type=MESH)

    def swap(r):
        rows = a_loc.at[_rows(mine + r * PIECE, PIECE)]
        return remote(rows, rows, swap_out.at[r], swap_in.at[r], partner)

    def far_rows(c, r):
        return a_far.at[_rows((2 * r + c) * PIECE, PIECE)]

    def far(r):
        return remote(a_loc.at[_rows(mine + r * PIECE, PIECE)], far_rows(core, r), far_out.at[r], far_in.at[r], across)

    def hand(r):
        return remote(far_rows(core, r), far_rows(core, r), pass_out.at[r], pass_in.at[r], partner)

    def moved_rows(r):
        return a_loc.at[pl.ds(CHIP + r * PIECE, PIECE)]

    def back(r):
        return remote(a_loc.at[pl.ds(r * PIECE, PIECE)], moved_rows(r), back_out.at[r], back_in.at[r], {"sp": 0})

    def hand_moved(r):
        return remote(moved_rows(r), moved_rows(r), pass_out.at[r], pass_in.at[r], partner)

    def x_back(c):
        return remote(xbuf.at[pl.ds(c * PIECE, PIECE)], xm, xb_out.at[c], xb_in, {"sp": c})

    def y_back(c):
        return remote(ym, y.at[_rows(c * PIECE, PIECE)], yb_out, yb_in.at[c], {"sp": 2})

    def seen(i):
        return remote(a_loc.at[_rows(theirs + i * BQ, BQ)], a_far.at[pl.ds(i * BQ, BQ)], seen_out.at[i], seen_in.at[i], partner)

    def seen_more():
        rows = a_loc.at[_rows(jnp.where(early, CHIP + (1 - core) * PIECE, ROWS), PIECE)]
        return remote(rows, a_far.at[pl.ds(ROWS, PIECE)], seen_out.at[2], seen_in.at[2], partner)

    def x_share():
        return remote(xbuf.at[pl.ds(0, PIECE)], xm, xb_out.at[0], xb_in, {"sp": 2})

    def y_share(n):
        here = _rows(n * COLS, COLS)
        return remote(ym.at[:, here], y.at[pl.ds(0, PIECE), here], share_out.at[n], share_in.at[n], {"sp": 3})

    factor_copy = pltpu.make_async_copy(table, factors, tab_sem)
    factor_copy.start()
    for r in range(4):
        x_copy(r).start()
    w_copy(wk, 0, core * kv_cols, 0).start()

    barrier = pltpu.get_barrier_semaphore()
    for other in range(1, 4):
        pl.semaphore_signal(barrier, inc=1, device_id={"sp": lax.rem(sp + other, 4)}, device_id_type=MESH)

    factor_copy.wait()
    near_same, near_other = factors[2 * FAR : 2 * FAR + NEAR, :], factors[2 * FAR + NEAR :, :]
    for n in range(FAR):
        tab[n * NEAR : (n + 1) * NEAR, :] = factors[n : n + 1, :] * near_same + factors[FAR + n : FAR + n + 1, :] * near_other

    for r in range(4):
        x_copy(r).wait()
        if r == 1:
            w_copy(wk, 0, core * kv_cols + COLS, 1).start()
        wide = xbuf[r * PIECE : (r + 1) * PIECE, :].astype(jnp.float32)
        scale = lax.rsqrt(jnp.mean(wide * wide, -1, keepdims=True) + 1e-6)
        a_loc[_rows(mine + r * PIECE, PIECE), :] = (wide * scale * gain[...].astype(jnp.float32)[None, :]).astype(a_loc.dtype)

    pl.semaphore_wait(barrier, 3)
    for r in range(4):
        pl.when(early)(far(r).start)
        swap(r).start()
        if r < 2:
            pl.when(giver)(back(r).start)
    pl.when(sp == 3)(x_share().start)

    @pl.when(giver)
    def _():
        for c in range(2):
            x_back(c).start()

    def turned(t, *places):
        rows = t.shape[0] // len(places)
        both = jnp.concatenate([tab[_rows(place, rows), :] for place in places], axis=0)
        back = pltpu.roll(both, HEAD // 2, 1)
        first = lax.broadcasted_iota(jnp.int32, both.shape, 1) < HEAD // 2
        cos, sin = jnp.where(first, both, back), jnp.where(first, -back, both)
        t = t.astype(q.dtype).astype(jnp.float32)
        for h in range(COLS // HEAD):
            part = t[:, h * HEAD : (h + 1) * HEAD]
            yield h, (part * cos + pltpu.roll(part, HEAD // 2, 1) * sin).astype(q.dtype)

    def project(a, row, slot, rows=BQ):
        return jnp.dot(a[_rows(row, rows), :], wbuf[slot], preferred_element_type=jnp.float32)

    def project_q(c, row):
        for h, t in turned(project(a_loc, row, q_slot(c)), chip * CHIP + row):
            q[lax.rem(c, 4) * 4 + h, _rows(row, BQ), :] = t

    def project_k(c, a, row, key, *places):
        for h, t in turned(project(a, row, c), *places):
            k[c * 4 + h, _rows(key, BQ), :] = t

    def project_v(c, a, row, key):
        t = project(a, row, 2 + c).astype(v.dtype)
        for h in range(COLS // HEAD):
            v[c * 4 + h, :, _rows(key, BQ)] = t[:, h * HEAD : (h + 1) * HEAD].T

    w_wait(0)
    for c in range(2):
        w_copy(wv, 0, core * kv_cols + c * COLS, 2 + c).start()

    for part, start in enumerate((mine, theirs)):
        if part:
            for r in range(4):
                swap(r).wait_recv()
        rows = [start + b * BQ for b in range(2)]
        for c in range(2):
            if c and not part:
                w_wait(1)
            for row in rows:
                project_k(c, a_loc, row, row, chip * CHIP + row)
        if not part:
            for c in range(2):
                w_wait(2 + c)
            for c in range(4):
                q_copy(c).start()
        for c in range(2):
            for row in rows:
                project_v(c, a_loc, row, row)

    def local_q(i, _):
        c = 2 * i
        for n in range(2):
            w_wait(q_slot(c + n))

        @pl.when(early)
        def _():
            for n in range(2):
                for b in range(CHIP // BQ):
                    project_q(c + n, b * BQ)

        @pl.when(late)
        def _():
            for n in range(2):
                for b in range(1, CHIP // BQ):
                    project_q(c + n, b * BQ)

        @pl.when(early)
        def _():
            for n in range(2):
                q_copy(c + 4 + n).start()

        @pl.when((i == 0) & (sp == 0))
        def _():
            for r in range(2):
                back(r).wait_recv()
                hand_moved(r).start()

    lax.fori_loop(0, 2, local_q, None)

    @pl.when(early)
    def _():
        @pl.when(core == 1)
        def _():
            for r in range(2):
                hand_moved(r).wait_recv()

        def moved_q(c, _):
            w_wait(q_slot(c))
            project_q(c, CHIP)

        lax.fori_loop(4, 8, moved_q, None)
        for c in range(2):
            project_k(c, a_loc, CHIP, CHIP, CHIP)
            project_v(c, a_loc, CHIP, CHIP)
        for u in range(4, 8):
            o_copy(u).start()

    for u in range(4):
        o_copy(u).start()

    e = HEAD**-0.5 * LOG2E
    cols = GROUP * BQ

    def block(iq, state, at, size, ahead=None):
        here, queries = _rows(at, size), _rows(iq * BQ, BQ)
        ones = jnp.ones((8, size), v.dtype)
        begin = ahead is not None
        if begin:
            ok = lax.rem(lax.broadcasted_iota(jnp.int32, (size, cols), 1), BQ) + ahead >= lax.broadcasted_iota(jnp.int32, (size, cols), 0)

        def scores(h):
            return _dot(k[h, here, :], q[GROUP * h : GROUP * (h + 1), queries, :].reshape(cols, HEAD), 1, 1)

        def weights(h, s):
            if begin:
                s = jnp.where(ok, s, HIDDEN)
                new, keep = s.max(axis=0, keepdims=True), None
            else:
                old = top[state, h : h + 1, :]
                new = jnp.maximum(old, s.max(axis=0, keepdims=True))
                keep = jnp.exp2((old - new) * e)
            top[state, h : h + 1, :] = new
            return jnp.exp2((s - new) * e).astype(v.dtype), keep

        def add(h, p, keep):
            got = _dot(jnp.concatenate([v[h, :, here], ones], axis=0), p, 1, 0)
            mix[state, h] = got if begin else mix[state, h] * keep + got

        ready_s, ready_p = [scores(0), scores(1)], []
        for h in range(KV):
            if h + 2 < KV:
                ready_s.append(scores(h + 2))
            ready_p.append(weights(h, ready_s[h]))
            if h:
                add(h - 1, *ready_p[h - 1])
        add(KV - 1, *ready_p[-1])

    def finish(iq, state):
        for h in range(KV):
            out = (mix[state, h, :HEAD, :] * (1 / mix[state, h, HEAD : HEAD + 1, :])).astype(a_loc.dtype).T
            for n in range(GROUP):
                a_loc[_rows(iq * BQ, BQ), (GROUP * h + n) * HEAD : (GROUP * h + n + 1) * HEAD] = out[n * BQ : (n + 1) * BQ, :]

    def hand_on(r):
        @pl.when(late)
        def _():
            far(r).wait_recv()
            hand(r).start()

    def moved_output():
        seen_more().wait_recv()
        x_back(0).wait_recv()

        def output(n, _):
            u = 2 * n
            for i in range(2):
                w_wait(o_slot(u + i))
            t = project(a_loc, CHIP + core * PIECE, o_slot(u), PIECE) + project(a_far, ROWS, o_slot(u + 1), PIECE)
            here = _rows(n * COLS, COLS)
            ym[:, here] = (xm[:, here].astype(jnp.float32) + t).astype(ym.dtype)
            for i in range(2):
                o_copy(u + i + SLOTS).start()

        lax.fori_loop(0, 4, output, None)

    hand_on(0)

    def far_project(half):
        def part(i, _):
            r = 2 * half + i
            for at in range(4):
                pl.when(r == at)(hand(at).wait_recv)
            row = 2 * r * PIECE

            def keys_and_values(between=None):
                for n in range(2):
                    project_k(n, a_far, row, CHIP + row, r * PIECE, ROWS + r * PIECE)
                if between is not None:
                    between()
                for n in range(2):
                    project_v(n, a_far, row, CHIP + row)

            pl.when(r != 2)(keys_and_values)
            pl.when(r == 2)(lambda: keys_and_values(lambda: hand_on(3)))

        lax.fori_loop(0, 2, part, None)

    def step(s, _):
        far_step = late & (s >= 3)
        half, i = lax.div(s, 3) - 1, lax.rem(s, 3)
        iq_early = jnp.where(s == 0, 4, lax.rem((1 - core) * 2 + s + 3, 4))
        iq_late = jnp.where(s < 3, s + 1, 1 + lax.rem(i + 1 - core, 3))
        iq = jnp.where(early, iq_early, iq_late)
        state = jnp.where(early, 0, iq - 1)
        p = lax.div(iq, 2)

        pl.when(far_step & (i == 0))(lambda: far_project(half))

        @pl.when(late & (s == 6))
        def _():
            for r in range(4):
                hand(r).wait_send()
            pl.semaphore_signal(ready, inc=1, device_id=partner, device_id_type=MESH)
            for u in range(4, 8):
                o_copy(u).start()

        @pl.when((late & (s == 6)) | (early & (s == 3)))
        def _():
            for r in range(4):
                swap(r).wait_send()
                pl.when(early)(far(r).wait_send)

        @pl.when(late & (s == 7))
        def _():
            pl.semaphore_wait(ready, 1)
            pl.when(core == 0)(seen(0).start)
            pl.when(core == 1)(seen(1).start)

        @pl.when(late & (s == 8))
        def _():
            pl.when(core == 0)(seen(1).start)
            pl.when(core == 1)(seen_more().start)

        even = lax.rem(iq, 2) == 0
        pl.when(jnp.logical_not(far_step) & even)(lambda: block(iq, state, p * BK, BQ, 0))
        pl.when(jnp.logical_not(far_step) & jnp.logical_not(even))(lambda: block(iq, state, p * BK, BK, BQ))

        @pl.when(early)
        def _():
            pl.when(s == 1)(seen_more().start)
            pl.when(s == 2)(seen(0).start)
            pl.when(s == 3)(seen(1).start)

        start = jnp.where(far_step, CHIP + half * BK, 0)
        lax.fori_loop(0, jnp.where(far_step, 1, p), lambda j, _: block(iq, state, start + j * BK, BK), None)

        @pl.when((s == 0) & (sp == 0))
        def _():
            for r in range(2):
                hand_moved(r).wait_send()

        pl.when(early | (s >= 6))(lambda: finish(iq, state))

        @pl.when(early)
        def _():
            pl.when(s == 1 + core)(moved_output)
            pl.when(s == 2 + core)(y_back(core).start)

        for at, r in ((1, 1), (3, 2)):
            pl.when(s == at)(functools.partial(hand_on, r))

    lax.fori_loop(0, jnp.where(early, 5, 9), step, None)

    pl.when(sp != 2)(seen(0).wait_recv)
    seen(1).wait_recv()

    @pl.when(sp == 2)
    def _():
        seen_more().wait_recv()
        x_share().wait_recv()

    begin = jnp.where(early, 8, 0)

    def output(n, _):
        u = begin + 2 * n
        for i in range(2):
            w_wait(o_slot(u + i))
        here = _rows(n * COLS, COLS)

        def both(own, other, rows):
            return project(a_loc, own, o_slot(u), rows) + project(a_far, other, o_slot(u + 1), rows)

        def part(row, rows):
            which = pl.ds(row, rows)
            y[which, here] = (xbuf[which, here].astype(jnp.float32) + both(mine + row, row, rows)).astype(y.dtype)

        @pl.when(early)
        def _():
            part(0, BQ)
            part(BQ, BQ)

        @pl.when(sp == 3)
        def _():
            part(PIECE, PIECE)
            part(BQ, BQ)

        def share():
            ym[:, here] = (xm[:, here].astype(jnp.float32) + both(ROWS, ROWS, PIECE)).astype(ym.dtype)

        @pl.when((sp == 2) & (n < 3))
        def _():
            share()
            part(BQ, BQ)
            y_share(n).start()

        @pl.when((sp == 2) & (n == 3))
        def _():
            share()
            y_share(n).start()
            part(BQ, BQ)

    lax.fori_loop(0, 4, output, None)
    pl.when(sp != 3)(seen(0).wait_send)
    seen(1).wait_send()
    pl.when(sp != 2)(seen_more().wait_send)
    pl.when(early)(y_back(core).wait_send)

    @pl.when(giver)
    def _():
        for c in range(2):
            back(c).wait_send()
            x_back(c).wait_send()
            y_back(c).wait_recv()
        for n in range(4):
            y_share(n).wait_send()

    @pl.when(sp == 3)
    def _():
        x_share().wait_send()
        for n in range(4):
            y_share(n).wait_recv()


def rotary():
    half = HEAD // 2
    speed = np.float64(THETA) ** (-np.arange(half) / half)
    far, near = (np.arange(n)[:, None] * step * speed for n, step in ((FAR, NEAR), (NEAR, 1)))
    rows = ((np.cos(far), np.sin(far)), (np.sin(far), np.cos(far)), (np.cos(near), np.cos(near)), (-np.sin(near), np.sin(near)))
    return np.concatenate([np.concatenate(row, -1) for row in rows]).astype(np.float32)


def solution(mesh):
    def step(x, gain, wq, wk, wv, wo):
        bf, f32 = jnp.bfloat16, jnp.float32
        dma = pltpu.SemaphoreType.DMA
        hbm = pl.BlockSpec(memory_space=pl.ANY)
        return pl.pallas_call(
            _kernel,
            out_shape=pltpu.VMEM(x.shape, x.dtype),
            in_specs=[hbm, pl.BlockSpec(memory_space=pltpu.VMEM), *[hbm] * 5],
            out_specs=pl.BlockSpec(memory_space=pltpu.VMEM),
            scratch_shapes=[
                pltpu.VMEM((CHIP + MOVED, DEPTH), bf),
                pltpu.VMEM((CHIP, DEPTH), bf),
                pltpu.VMEM((GROUP * KV, CHIP + MOVED, HEAD), bf),
                pltpu.VMEM((KV, 2 * CHIP, HEAD), bf),
                pltpu.VMEM((KV, HEAD, 2 * CHIP), bf),
                pltpu.VMEM((3, KV, GROUP * BQ), f32),
                pltpu.VMEM((3, KV, HEAD + 8, GROUP * BQ), f32),
                pltpu.VMEM((SLOTS, DEPTH, COLS), bf),
                pltpu.VMEM((ROWS, DEPTH), bf),
                pltpu.VMEM((2 * CHIP, HEAD), f32),
                pltpu.VMEM((2 * FAR + 2 * NEAR, HEAD), f32),
                pltpu.VMEM((PIECE, DEPTH), bf),
                pltpu.VMEM((PIECE, DEPTH), bf),
                dma((4,)), dma, dma((SLOTS,)),
                *[dma((4,))] * 6, dma((3,)), dma((3,)),
                dma((2,)), dma((2,)), dma((2,)), dma, dma, dma((2,)), dma((4,)), dma((4,)),
                pltpu.SemaphoreType.REGULAR,
            ],
            compiler_params=pltpu.CompilerParams(collective_id=0, has_side_effects=True, vmem_limit_bytes=VMEM),
            name="layer",
        )(x, gain, jnp.asarray(rotary()), wq, wk, wv, wo)

    tokens, whole = P(("dp", "sp"), None), P(None, None)
    return jax.shard_map(
        step,
        mesh=mesh,
        in_specs=(tokens, P(None), whole, whole, whole, whole),
        out_specs=tokens,
        check_vma=False,
    )
```

```python
import functools

import jax
import jax.numpy as jnp
import numpy as np
from jax import lax
from jax.experimental import pallas as pl
from jax.experimental.pallas import tpu as pltpu
from jax.sharding import PartitionSpec as P

HIDDEN = -jnp.inf
LOG2E = 1.4426950408889634
VMEM = 61 * 2**20
HEAD = 128
THETA = 10000

ROWS = 512
CHIP = 1024
DEPTH = 2048
COLS = 512
KV = 8
GROUP = 2
BQ = 256
BK = 512
PIECE = 128
MOVED = 256
SLOTS = 8
NEAR, FAR = 32, 64

MESH = pl.DeviceIdType.MESH


def _dot(a, b, ca, cb):
    return lax.dot_general(a, b, (((ca,), (cb,)), ((), ())), preferred_element_type=jnp.float32)


def _rows(start, size):
    return pl.ds(pl.multiple_of(start, size), size)


def _kernel(x, gain, table, wq, wk, wv, wo, y, a_loc, a_far, q, k, v, top, mix, wbuf, xbuf, tab, factors, xm, ym,
            x_sem, tab_sem, w_sem, swap_out, swap_in, far_out, far_in, pass_out, pass_in, seen_out, seen_in,
            back_out, back_in, xb_out, xb_in, yb_out, yb_in, share_out, share_in, ready):
    sp = lax.axis_index("sp")
    core, chip = lax.rem(sp, 2), lax.div(sp, 2)
    early, late = chip == 0, chip == 1
    giver = sp == 2
    partner, across = {"sp": chip * 2 + 1 - core}, {"sp": (1 - chip) * 2 + core}
    mine, theirs = core * ROWS, (1 - core) * ROWS
    kv_cols = KV * HEAD
    q_cols = GROUP * kv_cols

    def x_copy(r):
        return pltpu.make_async_copy(x.at[pl.ds(r * PIECE, PIECE)], xbuf.at[pl.ds(r * PIECE, PIECE)], x_sem.at[r])

    def w_copy(w, row, column, slot):
        return pltpu.make_async_copy(w.at[_rows(row, DEPTH), _rows(column, COLS)], wbuf.at[slot], w_sem.at[slot])

    def q_slot(c):
        return 4 + lax.rem(c, 4)

    def q_copy(c):
        return w_copy(wq, 0, core * q_cols + lax.rem(c, 4) * COLS, q_slot(c))

    def o_slot(u):
        return lax.rem(4 + u, SLOTS)

    def o_copy(u):
        return w_copy(wo, jnp.where(lax.rem(u, 2) == 0, core, 1 - core) * DEPTH, lax.div(lax.rem(u, 8), 2) * COLS, o_slot(u))

    def w_wait(slot):
        pltpu.make_async_copy(wq.at[pl.ds(0, DEPTH), pl.ds(0, COLS)], wbuf.at[slot], w_sem.at[slot]).wait()

    def remote(src, dst, out, got, device):
        return pltpu.make_async_remote_copy(src_ref=src, dst_ref=dst, send_sem=out, recv_sem=got, device_id=device, device_id_type=MESH)

    def swap(r):
        rows = a_loc.at[_rows(mine + r * PIECE, PIECE)]
        return remote(rows, rows, swap_out.at[r], swap_in.at[r], partner)

    def far_rows(c, r):
        return a_far.at[_rows((2 * r + c) * PIECE, PIECE)]

    def far(r):
        return remote(a_loc.at[_rows(mine + r * PIECE, PIECE)], far_rows(core, r), far_out.at[r], far_in.at[r], across)

    def hand(r):
        return remote(far_rows(core, r), far_rows(core, r), pass_out.at[r], pass_in.at[r], partner)

    def moved_rows(r):
        return a_loc.at[pl.ds(CHIP + r * PIECE, PIECE)]

    def back(r):
        return remote(a_loc.at[pl.ds(r * PIECE, PIECE)], moved_rows(r), back_out.at[r], back_in.at[r], {"sp": 0})

    def hand_moved(r):
        return remote(moved_rows(r), moved_rows(r), pass_out.at[r], pass_in.at[r], partner)

    def x_back(c):
        return remote(xbuf.at[pl.ds(c * PIECE, PIECE)], xm, xb_out.at[c], xb_in, {"sp": c})

    def y_back(c):
        return remote(ym, y.at[_rows(c * PIECE, PIECE)], yb_out, yb_in.at[c], {"sp": 2})

    def seen(i):
        return remote(a_loc.at[_rows(theirs + i * BQ, BQ)], a_far.at[pl.ds(i * BQ, BQ)], seen_out.at[i], seen_in.at[i], partner)

    def seen_more():
        rows = a_loc.at[_rows(jnp.where(early, CHIP + (1 - core) * PIECE, ROWS), PIECE)]
        return remote(rows, a_far.at[pl.ds(ROWS, PIECE)], seen_out.at[2], seen_in.at[2], partner)

    def x_share():
        return remote(xbuf.at[pl.ds(0, PIECE)], xm, xb_out.at[0], xb_in, {"sp": 2})

    def y_share(n):
        here = _rows(n * COLS, COLS)
        return remote(ym.at[:, here], y.at[pl.ds(0, PIECE), here], share_out.at[n], share_in.at[n], {"sp": 3})

    factor_copy = pltpu.make_async_copy(table, factors, tab_sem)
    factor_copy.start()
    for r in range(4):
        x_copy(r).start()
    w_copy(wk, 0, core * kv_cols, 0).start()

    barrier = pltpu.get_barrier_semaphore()
    for other in range(1, 4):
        pl.semaphore_signal(barrier, inc=1, device_id={"sp": lax.rem(sp + other, 4)}, device_id_type=MESH)

    factor_copy.wait()
    near_same, near_other = factors[2 * FAR : 2 * FAR + NEAR, :], factors[2 * FAR + NEAR :, :]
    for n in range(FAR):
        tab[n * NEAR : (n + 1) * NEAR, :] = factors[n : n + 1, :] * near_same + factors[FAR + n : FAR + n + 1, :] * near_other

    for r in range(4):
        x_copy(r).wait()
        if r == 1:
            w_copy(wk, 0, core * kv_cols + COLS, 1).start()
        wide = xbuf[r * PIECE : (r + 1) * PIECE, :].astype(jnp.float32)
        scale = lax.rsqrt(jnp.mean(wide * wide, -1, keepdims=True) + 1e-6)
        a_loc[_rows(mine + r * PIECE, PIECE), :] = (wide * scale * gain[...].astype(jnp.float32)[None, :]).astype(a_loc.dtype)

    pl.semaphore_wait(barrier, 3)
    for r in range(4):
        pl.when(early)(far(r).start)
        swap(r).start()
        if r < 2:
            pl.when(giver)(back(r).start)
    pl.when(sp == 3)(x_share().start)

    @pl.when(giver)
    def _():
        for c in range(2):
            x_back(c).start()

    def turned(t, *places):
        rows = t.shape[0] // len(places)
        both = jnp.concatenate([tab[_rows(place, rows), :] for place in places], axis=0)
        back = pltpu.roll(both, HEAD // 2, 1)
        first = lax.broadcasted_iota(jnp.int32, both.shape, 1) < HEAD // 2
        cos, sin = jnp.where(first, both, back), jnp.where(first, -back, both)
        t = t.astype(q.dtype).astype(jnp.float32)
        for h in range(COLS // HEAD):
            part = t[:, h * HEAD : (h + 1) * HEAD]
            yield h, (part * cos + pltpu.roll(part, HEAD // 2, 1) * sin).astype(q.dtype)

    def project(a, row, slot, rows=BQ):
        return jnp.dot(a[_rows(row, rows), :], wbuf[slot], preferred_element_type=jnp.float32)

    def project_q(c, row):
        for h, t in turned(project(a_loc, row, q_slot(c)), chip * CHIP + row):
            q[lax.rem(c, 4) * 4 + h, _rows(row, BQ), :] = t

    def project_k(c, a, row, key, *places):
        for h, t in turned(project(a, row, c), *places):
            k[c * 4 + h, _rows(key, BQ), :] = t

    def project_v(c, a, row, key):
        t = project(a, row, 2 + c).astype(v.dtype)
        for h in range(COLS // HEAD):
            v[c * 4 + h, :, _rows(key, BQ)] = t[:, h * HEAD : (h + 1) * HEAD].T

    w_wait(0)
    for c in range(2):
        w_copy(wv, 0, core * kv_cols + c * COLS, 2 + c).start()

    for part, start in enumerate((mine, theirs)):
        if part:
            for r in range(4):
                swap(r).wait_recv()
        rows = [start + b * BQ for b in range(2)]
        for c in range(2):
            if c and not part:
                w_wait(1)
            for row in rows:
                project_k(c, a_loc, row, row, chip * CHIP + row)
        if not part:
            for c in range(2):
                w_wait(2 + c)
            for c in range(4):
                q_copy(c).start()
        for c in range(2):
            for row in rows:
                project_v(c, a_loc, row, row)

    def local_q(i, _):
        c = 2 * i
        for n in range(2):
            w_wait(q_slot(c + n))

        @pl.when(early)
        def _():
            for n in range(2):
                for b in range(CHIP // BQ):
                    project_q(c + n, b * BQ)

        @pl.when(late)
        def _():
            for n in range(2):
                for b in range(1, CHIP // BQ):
                    project_q(c + n, b * BQ)

        @pl.when(early)
        def _():
            for n in range(2):
                q_copy(c + 4 + n).start()

        @pl.when((i == 0) & (sp == 0))
        def _():
            for r in range(2):
                back(r).wait_recv()
                hand_moved(r).start()

    lax.fori_loop(0, 2, local_q, None)

    @pl.when(early)
    def _():
        @pl.when(core == 1)
        def _():
            for r in range(2):
                hand_moved(r).wait_recv()

        def moved_q(c, _):
            w_wait(q_slot(c))
            project_q(c, CHIP)

        lax.fori_loop(4, 8, moved_q, None)
        for c in range(2):
            project_k(c, a_loc, CHIP, CHIP, CHIP)
            project_v(c, a_loc, CHIP, CHIP)
        for u in range(4, 8):
            o_copy(u).start()

    for u in range(4):
        o_copy(u).start()

    e = HEAD**-0.5 * LOG2E
    cols = GROUP * BQ

    def block(iq, state, at, size, ahead=None):
        here, queries = _rows(at, size), _rows(iq * BQ, BQ)
        ones = jnp.ones((8, size), v.dtype)
        begin = ahead is not None
        if begin:
            ok = lax.rem(lax.broadcasted_iota(jnp.int32, (size, cols), 1), BQ) + ahead >= lax.broadcasted_iota(jnp.int32, (size, cols), 0)

        def scores(h):
            return _dot(k[h, here, :], q[GROUP * h : GROUP * (h + 1), queries, :].reshape(cols, HEAD), 1, 1)

        def weights(h, s):
            if begin:
                s = jnp.where(ok, s, HIDDEN)
                new, keep = s.max(axis=0, keepdims=True), None
            else:
                old = top[state, h : h + 1, :]
                new = jnp.maximum(old, s.max(axis=0, keepdims=True))
                keep = jnp.exp2((old - new) * e)
            top[state, h : h + 1, :] = new
            return jnp.exp2((s - new) * e).astype(v.dtype), keep

        def add(h, p, keep):
            got = _dot(jnp.concatenate([v[h, :, here], ones], axis=0), p, 1, 0)
            mix[state, h] = got if begin else mix[state, h] * keep + got

        ready_s, ready_p = [scores(0), scores(1)], []
        for h in range(KV):
            if h + 2 < KV:
                ready_s.append(scores(h + 2))
            ready_p.append(weights(h, ready_s[h]))
            if h:
                add(h - 1, *ready_p[h - 1])
        add(KV - 1, *ready_p[-1])

    def finish(iq, state):
        for h in range(KV):
            out = (mix[state, h, :HEAD, :] * (1 / mix[state, h, HEAD : HEAD + 1, :])).astype(a_loc.dtype).T
            for n in range(GROUP):
                a_loc[_rows(iq * BQ, BQ), (GROUP * h + n) * HEAD : (GROUP * h + n + 1) * HEAD] = out[n * BQ : (n + 1) * BQ, :]

    def hand_on(r):
        @pl.when(late)
        def _():
            far(r).wait_recv()
            hand(r).start()

    def moved_output():
        seen_more().wait_recv()
        x_back(0).wait_recv()

        def output(n, _):
            u = 2 * n
            for i in range(2):
                w_wait(o_slot(u + i))
            t = project(a_loc, CHIP + core * PIECE, o_slot(u), PIECE) + project(a_far, ROWS, o_slot(u + 1), PIECE)
            here = _rows(n * COLS, COLS)
            ym[:, here] = (xm[:, here].astype(jnp.float32) + t).astype(ym.dtype)
            for i in range(2):
                o_copy(u + i + SLOTS).start()

        lax.fori_loop(0, 4, output, None)

    hand_on(0)

    def far_project(half, iq, state):
        def part(i, _):
            r = 2 * half + i
            for at in range(4):
                pl.when(r == at)(hand(at).wait_recv)
            row = 2 * r * PIECE
            for n in range(2):
                project_k(n, a_far, row, CHIP + row, r * PIECE, ROWS + r * PIECE)
                project_v(n, a_far, row, CHIP + row)
            pl.when(r == 2)(lambda: hand_on(3))
            pl.when(half == 1)(lambda: block(iq, state, CHIP + row, BQ))

        lax.fori_loop(0, 2, part, None)

    def step(s, _):
        far_step = late & (s >= 3)
        half, i = lax.div(s, 3) - 1, lax.rem(s, 3)
        iq_early = jnp.where(s == 0, 4, lax.rem((1 - core) * 2 + s + 3, 4))
        iq_late = jnp.where(s < 3, s + 1, 1 + lax.rem(i + 1 - core, 3))
        iq = jnp.where(early, iq_early, iq_late)
        state = jnp.where(early, 0, iq - 1)
        p = lax.div(iq, 2)

        pl.when(far_step & (i == 0))(lambda: far_project(half, iq, state))

        @pl.when(late & (s == 6))
        def _():
            for r in range(4):
                hand(r).wait_send()
            pl.semaphore_signal(ready, inc=1, device_id=partner, device_id_type=MESH)
            for u in range(4, 8):
                o_copy(u).start()

        @pl.when((late & (s == 6)) | (early & (s == 3)))
        def _():
            for r in range(4):
                swap(r).wait_send()
                pl.when(early)(far(r).wait_send)

        @pl.when(late & (s == 7))
        def _():
            pl.semaphore_wait(ready, 1)
            pl.when(core == 0)(seen(0).start)
            pl.when(core == 1)(seen(1).start)

        @pl.when(late & (s == 8))
        def _():
            pl.when(core == 0)(seen(1).start)
            pl.when(core == 1)(seen_more().start)

        even = lax.rem(iq, 2) == 0
        pl.when(jnp.logical_not(far_step) & even)(lambda: block(iq, state, p * BK, BQ, 0))
        pl.when(jnp.logical_not(far_step) & jnp.logical_not(even))(lambda: block(iq, state, p * BK, BK, BQ))

        @pl.when(early)
        def _():
            pl.when(s == 1)(seen_more().start)
            pl.when(s == 2)(seen(0).start)
            pl.when(s == 3)(seen(1).start)

        start = jnp.where(far_step, CHIP + half * BK, 0)
        lax.fori_loop(0, jnp.where(far_step, jnp.where(s == 6, 0, 1), p), lambda j, _: block(iq, state, start + j * BK, BK), None)

        @pl.when((s == 0) & (sp == 0))
        def _():
            for r in range(2):
                hand_moved(r).wait_send()

        pl.when(early | (s >= 6))(lambda: finish(iq, state))

        @pl.when(early)
        def _():
            pl.when(s == 1 + core)(moved_output)
            pl.when(s == 2 + core)(y_back(core).start)

        for at, r in ((1, 1), (3, 2)):
            pl.when(s == at)(functools.partial(hand_on, r))

    lax.fori_loop(0, jnp.where(early, 5, 9), step, None)

    pl.when(sp != 2)(seen(0).wait_recv)
    seen(1).wait_recv()

    @pl.when(sp == 2)
    def _():
        seen_more().wait_recv()
        x_share().wait_recv()

    begin = jnp.where(early, 8, 0)

    def output(n, _):
        u = begin + 2 * n
        for i in range(2):
            w_wait(o_slot(u + i))
        here = _rows(n * COLS, COLS)

        def both(own, other, rows):
            return project(a_loc, own, o_slot(u), rows) + project(a_far, other, o_slot(u + 1), rows)

        def part(row, rows):
            which = pl.ds(row, rows)
            y[which, here] = (xbuf[which, here].astype(jnp.float32) + both(mine + row, row, rows)).astype(y.dtype)

        @pl.when(early)
        def _():
            part(0, BQ)
            part(BQ, BQ)

        @pl.when(sp == 3)
        def _():
            part(PIECE, PIECE)
            part(BQ, BQ)

        def share():
            ym[:, here] = (xm[:, here].astype(jnp.float32) + both(ROWS, ROWS, PIECE)).astype(ym.dtype)

        @pl.when((sp == 2) & (n < 3))
        def _():
            share()
            part(BQ, BQ)
            y_share(n).start()

        @pl.when((sp == 2) & (n == 3))
        def _():
            share()
            y_share(n).start()
            part(BQ, BQ)

    lax.fori_loop(0, 4, output, None)
    pl.when(sp != 3)(seen(0).wait_send)
    seen(1).wait_send()
    pl.when(sp != 2)(seen_more().wait_send)
    pl.when(early)(y_back(core).wait_send)

    @pl.when(giver)
    def _():
        for c in range(2):
            back(c).wait_send()
            x_back(c).wait_send()
            y_back(c).wait_recv()
        for n in range(4):
            y_share(n).wait_send()

    @pl.when(sp == 3)
    def _():
        x_share().wait_send()
        for n in range(4):
            y_share(n).wait_recv()


def rotary():
    half = HEAD // 2
    speed = np.float64(THETA) ** (-np.arange(half) / half)
    far, near = (np.arange(n)[:, None] * step * speed for n, step in ((FAR, NEAR), (NEAR, 1)))
    rows = ((np.cos(far), np.sin(far)), (np.sin(far), np.cos(far)), (np.cos(near), np.cos(near)), (-np.sin(near), np.sin(near)))
    return np.concatenate([np.concatenate(row, -1) for row in rows]).astype(np.float32)


def solution(mesh):
    def step(x, gain, wq, wk, wv, wo):
        bf, f32 = jnp.bfloat16, jnp.float32
        dma = pltpu.SemaphoreType.DMA
        hbm = pl.BlockSpec(memory_space=pl.ANY)
        return pl.pallas_call(
            _kernel,
            out_shape=pltpu.VMEM(x.shape, x.dtype),
            in_specs=[hbm, pl.BlockSpec(memory_space=pltpu.VMEM), *[hbm] * 5],
            out_specs=pl.BlockSpec(memory_space=pltpu.VMEM),
            scratch_shapes=[
                pltpu.VMEM((CHIP + MOVED, DEPTH), bf),
                pltpu.VMEM((CHIP, DEPTH), bf),
                pltpu.VMEM((GROUP * KV, CHIP + MOVED, HEAD), bf),
                pltpu.VMEM((KV, 2 * CHIP, HEAD), bf),
                pltpu.VMEM((KV, HEAD, 2 * CHIP), bf),
                pltpu.VMEM((3, KV, GROUP * BQ), f32),
                pltpu.VMEM((3, KV, HEAD + 8, GROUP * BQ), f32),
                pltpu.VMEM((SLOTS, DEPTH, COLS), bf),
                pltpu.VMEM((ROWS, DEPTH), bf),
                pltpu.VMEM((2 * CHIP, HEAD), f32),
                pltpu.VMEM((2 * FAR + 2 * NEAR, HEAD), f32),
                pltpu.VMEM((PIECE, DEPTH), bf),
                pltpu.VMEM((PIECE, DEPTH), bf),
                dma((4,)), dma, dma((SLOTS,)),
                *[dma((4,))] * 6, dma((3,)), dma((3,)),
                dma((2,)), dma((2,)), dma((2,)), dma, dma, dma((2,)), dma((4,)), dma((4,)),
                pltpu.SemaphoreType.REGULAR,
            ],
            compiler_params=pltpu.CompilerParams(collective_id=0, has_side_effects=True, vmem_limit_bytes=VMEM),
            name="layer",
        )(x, gain, jnp.asarray(rotary()), wq, wk, wv, wo)

    tokens, whole = P(("dp", "sp"), None), P(None, None)
    return jax.shard_map(
        step,
        mesh=mesh,
        in_specs=(tokens, P(None), whole, whole, whole, whole),
        out_specs=tokens,
        check_vma=False,
    )
```

```python
import functools

import jax
import jax.numpy as jnp
import numpy as np
from jax import lax
from jax.experimental import pallas as pl
from jax.experimental.pallas import tpu as pltpu
from jax.sharding import PartitionSpec as P

HIDDEN = -jnp.inf
LOG2E = 1.4426950408889634
VMEM = 61 * 2**20
HEAD = 128
THETA = 10000

ROWS = 512
CHIP = 1024
DEPTH = 2048
COLS = 512
KV = 8
GROUP = 2
BQ = 256
BK = 512
PIECE = 128
MOVED = 256
SLOTS = 8
NEAR, FAR = 32, 64

MESH = pl.DeviceIdType.MESH


def _dot(a, b, ca, cb):
    return lax.dot_general(a, b, (((ca,), (cb,)), ((), ())), preferred_element_type=jnp.float32)


def _rows(start, size):
    return pl.ds(pl.multiple_of(start, size), size)


def _kernel(x, gain, table, wq, wk, wv, wo, y, a_loc, a_far, q, k, v, top, mix, wbuf, xbuf, tab, factors, gains, xm, ym,
            x_sem, gain_sem, tab_sem, w_sem, swap_out, swap_in, far_out, far_in, pass_out, pass_in, seen_out, seen_in,
            back_out, back_in, xb_out, xb_in, yb_out, yb_in, share_out, share_in, ready):
    sp = lax.axis_index("sp")
    core, chip = lax.rem(sp, 2), lax.div(sp, 2)
    early, late = chip == 0, chip == 1
    giver = sp == 2
    partner, across = {"sp": chip * 2 + 1 - core}, {"sp": (1 - chip) * 2 + core}
    mine, theirs = core * ROWS, (1 - core) * ROWS
    kv_cols = KV * HEAD
    q_cols = GROUP * kv_cols

    def x_copy(r):
        return pltpu.make_async_copy(x.at[pl.ds(r * PIECE, PIECE)], xbuf.at[pl.ds(r * PIECE, PIECE)], x_sem.at[r])

    def w_copy(w, row, column, slot):
        return pltpu.make_async_copy(w.at[_rows(row, DEPTH), _rows(column, COLS)], wbuf.at[slot], w_sem.at[slot])

    def q_slot(c):
        return 4 + lax.rem(c, 4)

    def q_copy(c):
        return w_copy(wq, 0, core * q_cols + lax.rem(c, 4) * COLS, q_slot(c))

    def o_slot(u):
        return lax.rem(4 + u, SLOTS)

    def o_copy(u):
        return w_copy(wo, jnp.where(lax.rem(u, 2) == 0, core, 1 - core) * DEPTH, lax.div(lax.rem(u, 8), 2) * COLS, o_slot(u))

    def w_wait(slot):
        pltpu.make_async_copy(wq.at[pl.ds(0, DEPTH), pl.ds(0, COLS)], wbuf.at[slot], w_sem.at[slot]).wait()

    def remote(src, dst, out, got, device):
        return pltpu.make_async_remote_copy(src_ref=src, dst_ref=dst, send_sem=out, recv_sem=got, device_id=device, device_id_type=MESH)

    def swap(r):
        rows = a_loc.at[_rows(mine + r * PIECE, PIECE)]
        return remote(rows, rows, swap_out.at[r], swap_in.at[r], partner)

    def far_rows(c, r):
        return a_far.at[_rows((2 * r + c) * PIECE, PIECE)]

    def far(r):
        return remote(a_loc.at[_rows(mine + r * PIECE, PIECE)], far_rows(core, r), far_out.at[r], far_in.at[r], across)

    def hand(r):
        return remote(far_rows(core, r), far_rows(core, r), pass_out.at[r], pass_in.at[r], partner)

    def moved_rows(r):
        return a_loc.at[pl.ds(CHIP + r * PIECE, PIECE)]

    def back(r):
        return remote(a_loc.at[pl.ds(r * PIECE, PIECE)], moved_rows(r), back_out.at[r], back_in.at[r], {"sp": 0})

    def hand_moved(r):
        return remote(moved_rows(r), moved_rows(r), pass_out.at[r], pass_in.at[r], partner)

    def x_back(c):
        return remote(xbuf.at[pl.ds(c * PIECE, PIECE)], xm, xb_out.at[c], xb_in, {"sp": c})

    def y_back(c):
        return remote(ym, y.at[_rows(c * PIECE, PIECE)], yb_out, yb_in.at[c], {"sp": 2})

    def seen(i):
        return remote(a_loc.at[_rows(theirs + i * BQ, BQ)], a_far.at[pl.ds(i * BQ, BQ)], seen_out.at[i], seen_in.at[i], partner)

    def seen_more():
        rows = a_loc.at[_rows(jnp.where(early, CHIP + (1 - core) * PIECE, ROWS), PIECE)]
        return remote(rows, a_far.at[pl.ds(ROWS, PIECE)], seen_out.at[2], seen_in.at[2], partner)

    def x_share():
        return remote(xbuf.at[pl.ds(0, PIECE)], xm, xb_out.at[0], xb_in, {"sp": 2})

    def y_share(n):
        here = _rows(n * COLS, COLS)
        return remote(ym.at[:, here], y.at[pl.ds(0, PIECE), here], share_out.at[n], share_in.at[n], {"sp": 3})

    barrier = pltpu.get_barrier_semaphore()
    for other in range(1, 4):
        pl.semaphore_signal(barrier, inc=1, device_id={"sp": lax.rem(sp + other, 4)}, device_id_type=MESH)

    gain_copy = pltpu.make_async_copy(gain, gains, gain_sem)
    gain_copy.start()
    for r in range(4):
        x_copy(r).start()
    factor_copy = pltpu.make_async_copy(table, factors, tab_sem)
    factor_copy.start()
    w_copy(wk, 0, core * kv_cols, 0).start()

    gain_copy.wait()
    for r in range(4):
        x_copy(r).wait()
        if r == 1:
            w_copy(wk, 0, core * kv_cols + COLS, 1).start()
        wide = xbuf[r * PIECE : (r + 1) * PIECE, :].astype(jnp.float32)
        scale = lax.rsqrt(jnp.mean(wide * wide, -1, keepdims=True) + 1e-6)
        a_loc[_rows(mine + r * PIECE, PIECE), :] = (wide * scale * gains[...].astype(jnp.float32)[None, :]).astype(a_loc.dtype)

    pl.semaphore_wait(barrier, 3)
    for r in range(4):
        pl.when(early)(far(r).start)
        swap(r).start()
        if r < 2:
            pl.when(giver)(back(r).start)
    pl.when(sp == 3)(x_share().start)

    @pl.when(giver)
    def _():
        for c in range(2):
            x_back(c).start()

    factor_copy.wait()
    near_same, near_other = factors[2 * FAR : 2 * FAR + NEAR, :], factors[2 * FAR + NEAR :, :]
    for n in range(FAR):
        tab[n * NEAR : (n + 1) * NEAR, :] = factors[n : n + 1, :] * near_same + factors[FAR + n : FAR + n + 1, :] * near_other

    def turned(t, *places):
        rows = t.shape[0] // len(places)
        both = jnp.concatenate([tab[_rows(place, rows), :] for place in places], axis=0)
        back = pltpu.roll(both, HEAD // 2, 1)
        first = lax.broadcasted_iota(jnp.int32, both.shape, 1) < HEAD // 2
        cos, sin = jnp.where(first, both, back), jnp.where(first, -back, both)
        t = t.astype(q.dtype).astype(jnp.float32)
        for h in range(COLS // HEAD):
            part = t[:, h * HEAD : (h + 1) * HEAD]
            yield h, (part * cos + pltpu.roll(part, HEAD // 2, 1) * sin).astype(q.dtype)

    def project(a, row, slot, rows=BQ):
        return jnp.dot(a[_rows(row, rows), :], wbuf[slot], preferred_element_type=jnp.float32)

    def project_q(c, row):
        for h, t in turned(project(a_loc, row, q_slot(c)), chip * CHIP + row):
            q[lax.rem(c, 4) * 4 + h, _rows(row, BQ), :] = t

    def project_k(c, a, row, key, *places):
        for h, t in turned(project(a, row, c), *places):
            k[c * 4 + h, _rows(key, BQ), :] = t

    def project_v(c, a, row, key):
        t = project(a, row, 2 + c).astype(v.dtype)
        for h in range(COLS // HEAD):
            v[c * 4 + h, :, _rows(key, BQ)] = t[:, h * HEAD : (h + 1) * HEAD].T

    w_wait(0)
    for c in range(2):
        w_copy(wv, 0, core * kv_cols + c * COLS, 2 + c).start()

    for part, start in enumerate((mine, theirs)):
        if part:
            for r in range(4):
                swap(r).wait_recv()
        rows = [start + b * BQ for b in range(2)]
        for c in range(2):
            if c and not part:
                w_wait(1)
            for row in rows:
                project_k(c, a_loc, row, row, chip * CHIP + row)
        if not part:
            for c in range(2):
                w_wait(2 + c)
            for c in range(4):
                q_copy(c).start()
        for c in range(2):
            for row in rows:
                project_v(c, a_loc, row, row)

    def local_q(i, _):
        c = 2 * i
        for n in range(2):
            w_wait(q_slot(c + n))

        @pl.when(early)
        def _():
            for n in range(2):
                for b in range(CHIP // BQ):
                    project_q(c + n, b * BQ)

        @pl.when(late)
        def _():
            for n in range(2):
                for b in range(1, CHIP // BQ):
                    project_q(c + n, b * BQ)

        @pl.when(early)
        def _():
            for n in range(2):
                q_copy(c + 4 + n).start()

        @pl.when((i == 0) & (sp == 0))
        def _():
            for r in range(2):
                back(r).wait_recv()
                hand_moved(r).start()

    lax.fori_loop(0, 2, local_q, None)

    @pl.when(early)
    def _():
        @pl.when(core == 1)
        def _():
            for r in range(2):
                hand_moved(r).wait_recv()

        def moved_q(c, _):
            w_wait(q_slot(c))
            project_q(c, CHIP)

        lax.fori_loop(4, 8, moved_q, None)
        for c in range(2):
            project_k(c, a_loc, CHIP, CHIP, CHIP)
            project_v(c, a_loc, CHIP, CHIP)
        for u in range(4, 8):
            o_copy(u).start()

    for u in range(4):
        o_copy(u).start()

    e = HEAD**-0.5 * LOG2E
    cols = GROUP * BQ

    def block(iq, state, at, size, ahead=None):
        here, queries = _rows(at, size), _rows(iq * BQ, BQ)
        ones = jnp.ones((8, size), v.dtype)
        begin = ahead is not None
        if begin:
            ok = lax.rem(lax.broadcasted_iota(jnp.int32, (size, cols), 1), BQ) + ahead >= lax.broadcasted_iota(jnp.int32, (size, cols), 0)

        def scores(h):
            return _dot(k[h, here, :], q[GROUP * h : GROUP * (h + 1), queries, :].reshape(cols, HEAD), 1, 1)

        def weights(h, s):
            if begin:
                s = jnp.where(ok, s, HIDDEN)
                new, keep = s.max(axis=0, keepdims=True), None
            else:
                old = top[state, h : h + 1, :]
                new = jnp.maximum(old, s.max(axis=0, keepdims=True))
                keep = jnp.exp2((old - new) * e)
            top[state, h : h + 1, :] = new
            return jnp.exp2((s - new) * e).astype(v.dtype), keep

        def add(h, p, keep):
            got = _dot(jnp.concatenate([v[h, :, here], ones], axis=0), p, 1, 0)
            mix[state, h] = got if begin else mix[state, h] * keep + got

        ready_s, ready_p = [scores(0), scores(1)], []
        for h in range(KV):
            if h + 2 < KV:
                ready_s.append(scores(h + 2))
            ready_p.append(weights(h, ready_s[h]))
            if h:
                add(h - 1, *ready_p[h - 1])
        add(KV - 1, *ready_p[-1])

    def finish(iq, state):
        for h in range(KV):
            out = (mix[state, h, :HEAD, :] * (1 / mix[state, h, HEAD : HEAD + 1, :])).astype(a_loc.dtype).T
            for n in range(GROUP):
                a_loc[_rows(iq * BQ, BQ), (GROUP * h + n) * HEAD : (GROUP * h + n + 1) * HEAD] = out[n * BQ : (n + 1) * BQ, :]

    def hand_on(r):
        @pl.when(late)
        def _():
            far(r).wait_recv()
            hand(r).start()

    def moved_output():
        seen_more().wait_recv()
        x_back(0).wait_recv()

        def output(n, _):
            u = 2 * n
            for i in range(2):
                w_wait(o_slot(u + i))
            t = project(a_loc, CHIP + core * PIECE, o_slot(u), PIECE) + project(a_far, ROWS, o_slot(u + 1), PIECE)
            here = _rows(n * COLS, COLS)
            ym[:, here] = (xm[:, here].astype(jnp.float32) + t).astype(ym.dtype)
            for i in range(2):
                o_copy(u + i + SLOTS).start()

        lax.fori_loop(0, 4, output, None)

    hand_on(0)

    def far_project(half, iq, state):
        def part(i, _):
            r = 2 * half + i
            for at in range(4):
                pl.when(r == at)(hand(at).wait_recv)
            row = 2 * r * PIECE
            for n in range(2):
                project_k(n, a_far, row, CHIP + row, r * PIECE, ROWS + r * PIECE)
                project_v(n, a_far, row, CHIP + row)
            pl.when(r == 2)(lambda: hand_on(3))
            pl.when(half == 1)(lambda: block(iq, state, CHIP + row, BQ))

        lax.fori_loop(0, 2, part, None)

    def step(s, _):
        far_step = late & (s >= 3)
        half, i = lax.div(s, 3) - 1, lax.rem(s, 3)
        iq_early = jnp.where(s == 0, 4, lax.rem((1 - core) * 2 + s + 3, 4))
        iq_late = jnp.where(s < 3, s + 1, 1 + lax.rem(i + 1 - core, 3))
        iq = jnp.where(early, iq_early, iq_late)
        state = jnp.where(early, 0, iq - 1)
        p = lax.div(iq, 2)

        pl.when(far_step & (i == 0))(lambda: far_project(half, iq, state))

        @pl.when(late & (s == 6))
        def _():
            for r in range(4):
                hand(r).wait_send()
            pl.semaphore_signal(ready, inc=1, device_id=partner, device_id_type=MESH)
            for u in range(4, 8):
                o_copy(u).start()

        @pl.when((late & (s == 6)) | (early & (s == 3)))
        def _():
            for r in range(4):
                swap(r).wait_send()
                pl.when(early)(far(r).wait_send)

        @pl.when(late & (s == 7))
        def _():
            pl.semaphore_wait(ready, 1)
            pl.when(core == 0)(seen(0).start)
            pl.when(core == 1)(seen(1).start)

        @pl.when(late & (s == 8))
        def _():
            pl.when(core == 0)(seen(1).start)
            pl.when(core == 1)(seen_more().start)

        even = lax.rem(iq, 2) == 0
        pl.when(jnp.logical_not(far_step) & even)(lambda: block(iq, state, p * BK, BQ, 0))
        pl.when(jnp.logical_not(far_step) & jnp.logical_not(even))(lambda: block(iq, state, p * BK, BK, BQ))

        @pl.when(early)
        def _():
            pl.when(s == 1)(seen_more().start)
            pl.when(s == 2)(seen(0).start)
            pl.when(s == 3)(seen(1).start)

        start = jnp.where(far_step, CHIP + half * BK, 0)
        lax.fori_loop(0, jnp.where(far_step, jnp.where(s == 6, 0, 1), p), lambda j, _: block(iq, state, start + j * BK, BK), None)

        @pl.when((s == 0) & (sp == 0))
        def _():
            for r in range(2):
                hand_moved(r).wait_send()

        pl.when(early | (s >= 6))(lambda: finish(iq, state))

        @pl.when(early)
        def _():
            pl.when(s == 1 + core)(moved_output)
            pl.when(s == 2 + core)(y_back(core).start)

        for at, r in ((1, 1), (3, 2)):
            pl.when(s == at)(functools.partial(hand_on, r))

    lax.fori_loop(0, jnp.where(early, 5, 9), step, None)

    pl.when(sp != 2)(seen(0).wait_recv)
    seen(1).wait_recv()

    @pl.when(sp == 2)
    def _():
        seen_more().wait_recv()
        x_share().wait_recv()

    begin = jnp.where(early, 8, 0)

    def output(n, _):
        u = begin + 2 * n
        for i in range(2):
            w_wait(o_slot(u + i))
        here = _rows(n * COLS, COLS)

        def both(own, other, rows):
            return project(a_loc, own, o_slot(u), rows) + project(a_far, other, o_slot(u + 1), rows)

        def part(row, rows):
            which = pl.ds(row, rows)
            y[which, here] = (xbuf[which, here].astype(jnp.float32) + both(mine + row, row, rows)).astype(y.dtype)

        @pl.when(early)
        def _():
            part(0, BQ)
            part(BQ, BQ)

        @pl.when(sp == 3)
        def _():
            part(PIECE, PIECE)
            part(BQ, BQ)

        def share():
            ym[:, here] = (xm[:, here].astype(jnp.float32) + both(ROWS, ROWS, PIECE)).astype(ym.dtype)

        @pl.when((sp == 2) & (n < 3))
        def _():
            share()
            part(BQ, BQ)
            y_share(n).start()

        @pl.when((sp == 2) & (n == 3))
        def _():
            share()
            y_share(n).start()
            part(BQ, BQ)

    lax.fori_loop(0, 4, output, None)
    pl.when(sp != 3)(seen(0).wait_send)
    seen(1).wait_send()
    pl.when(sp != 2)(seen_more().wait_send)
    pl.when(early)(y_back(core).wait_send)

    @pl.when(giver)
    def _():
        for c in range(2):
            back(c).wait_send()
            x_back(c).wait_send()
            y_back(c).wait_recv()
        for n in range(4):
            y_share(n).wait_send()

    @pl.when(sp == 3)
    def _():
        x_share().wait_send()
        for n in range(4):
            y_share(n).wait_recv()


def rotary():
    half = HEAD // 2
    speed = np.float64(THETA) ** (-np.arange(half) / half)
    far, near = (np.arange(n)[:, None] * step * speed for n, step in ((FAR, NEAR), (NEAR, 1)))
    rows = ((np.cos(far), np.sin(far)), (np.sin(far), np.cos(far)), (np.cos(near), np.cos(near)), (-np.sin(near), np.sin(near)))
    return np.concatenate([np.concatenate(row, -1) for row in rows]).astype(np.float32)


def solution(mesh):
    def step(x, gain, wq, wk, wv, wo):
        bf, f32 = jnp.bfloat16, jnp.float32
        dma = pltpu.SemaphoreType.DMA
        hbm = pl.BlockSpec(memory_space=pl.ANY)
        return pl.pallas_call(
            _kernel,
            out_shape=pltpu.VMEM(x.shape, x.dtype),
            in_specs=[hbm] * 7,
            out_specs=pl.BlockSpec(memory_space=pltpu.VMEM),
            scratch_shapes=[
                pltpu.VMEM((CHIP + MOVED, DEPTH), bf),
                pltpu.VMEM((CHIP, DEPTH), bf),
                pltpu.VMEM((GROUP * KV, CHIP + MOVED, HEAD), bf),
                pltpu.VMEM((KV, 2 * CHIP, HEAD), bf),
                pltpu.VMEM((KV, HEAD, 2 * CHIP), bf),
                pltpu.VMEM((3, KV, GROUP * BQ), f32),
                pltpu.VMEM((3, KV, HEAD + 8, GROUP * BQ), f32),
                pltpu.VMEM((SLOTS, DEPTH, COLS), bf),
                pltpu.VMEM((ROWS, DEPTH), bf),
                pltpu.VMEM((2 * CHIP, HEAD), f32),
                pltpu.VMEM((2 * FAR + 2 * NEAR, HEAD), f32),
                pltpu.VMEM((DEPTH,), bf),
                pltpu.VMEM((PIECE, DEPTH), bf),
                pltpu.VMEM((PIECE, DEPTH), bf),
                dma((4,)), dma, dma, dma((SLOTS,)),
                *[dma((4,))] * 6, dma((3,)), dma((3,)),
                dma((2,)), dma((2,)), dma((2,)), dma, dma, dma((2,)), dma((4,)), dma((4,)),
                pltpu.SemaphoreType.REGULAR,
            ],
            compiler_params=pltpu.CompilerParams(collective_id=0, has_side_effects=True, vmem_limit_bytes=VMEM),
            name="layer",
        )(x, gain, jnp.asarray(rotary()), wq, wk, wv, wo)

    tokens, whole = P(("dp", "sp"), None), P(None, None)
    return jax.shard_map(
        step,
        mesh=mesh,
        in_specs=(tokens, P(None), whole, whole, whole, whole),
        out_specs=tokens,
        check_vma=False,
    )
```

```python
import functools

import jax
import jax.numpy as jnp
import numpy as np
from jax import lax
from jax.experimental import pallas as pl
from jax.experimental.pallas import tpu as pltpu
from jax.sharding import PartitionSpec as P

HIDDEN = -jnp.inf
LOG2E = 1.4426950408889634
VMEM = 61 * 2**20
HEAD = 128
THETA = 10000

ROWS = 512
CHIP = 1024
DEPTH = 2048
COLS = 512
KV = 8
GROUP = 2
BQ = 256
BK = 512
PIECE = 128
MOVED = 256
SLOTS = 8
NEAR, FAR = 32, 64

MESH = pl.DeviceIdType.MESH


def _dot(a, b, ca, cb):
    return lax.dot_general(a, b, (((ca,), (cb,)), ((), ())), preferred_element_type=jnp.float32)


def _rows(start, size):
    return pl.ds(pl.multiple_of(start, size), size)


def _kernel(x, gain, table, wq, wk, wv, wo, y, a_loc, a_far, q, k, v, top, mix, wbuf, xbuf, tab, factors, gains, xm, ym,
            x_sem, gain_sem, tab_sem, w_sem, swap_out, swap_in, far_out, far_in, pass_out, pass_in, seen_out, seen_in,
            back_out, back_in, xb_out, xb_in, yb_out, yb_in, share_out, share_in, ready):
    sp = lax.axis_index("sp")
    core, chip = lax.rem(sp, 2), lax.div(sp, 2)
    early, late = chip == 0, chip == 1
    giver = sp == 2
    partner, across = {"sp": chip * 2 + 1 - core}, {"sp": (1 - chip) * 2 + core}
    mine, theirs = core * ROWS, (1 - core) * ROWS
    kv_cols = KV * HEAD
    q_cols = GROUP * kv_cols

    def x_copy(r):
        return pltpu.make_async_copy(x.at[pl.ds(r * PIECE, PIECE)], xbuf.at[pl.ds(r * PIECE, PIECE)], x_sem.at[r])

    def w_copy(w, row, column, slot):
        return pltpu.make_async_copy(w.at[_rows(row, DEPTH), _rows(column, COLS)], wbuf.at[slot], w_sem.at[slot])

    def q_slot(c):
        return 4 + lax.rem(c, 4)

    def q_copy(c):
        return w_copy(wq, 0, core * q_cols + lax.rem(c, 4) * COLS, q_slot(c))

    def o_slot(u):
        return lax.rem(4 + u, SLOTS)

    def o_copy(u):
        return w_copy(wo, jnp.where(lax.rem(u, 2) == 0, core, 1 - core) * DEPTH, lax.div(lax.rem(u, 8), 2) * COLS, o_slot(u))

    def w_wait(slot):
        pltpu.make_async_copy(wq.at[pl.ds(0, DEPTH), pl.ds(0, COLS)], wbuf.at[slot], w_sem.at[slot]).wait()

    def remote(src, dst, out, got, device):
        return pltpu.make_async_remote_copy(src_ref=src, dst_ref=dst, send_sem=out, recv_sem=got, device_id=device, device_id_type=MESH)

    def swap(r):
        rows = a_loc.at[_rows(mine + r * PIECE, PIECE)]
        return remote(rows, rows, swap_out.at[r], swap_in.at[r], partner)

    def far_rows(c, r):
        return a_far.at[_rows((2 * r + c) * PIECE, PIECE)]

    def far(r):
        return remote(a_loc.at[_rows(mine + r * PIECE, PIECE)], far_rows(core, r), far_out.at[r], far_in.at[r], across)

    def hand(r):
        return remote(far_rows(core, r), far_rows(core, r), pass_out.at[r], pass_in.at[r], partner)

    def moved_rows(r):
        return a_loc.at[pl.ds(CHIP + r * PIECE, PIECE)]

    def back(r):
        return remote(a_loc.at[pl.ds(r * PIECE, PIECE)], moved_rows(r), back_out.at[r], back_in.at[r], {"sp": 0})

    def hand_moved(r):
        return remote(moved_rows(r), moved_rows(r), pass_out.at[r], pass_in.at[r], partner)

    def x_back(c):
        return remote(xbuf.at[pl.ds(c * PIECE, PIECE)], xm, xb_out.at[c], xb_in, {"sp": c})

    def y_back(c):
        return remote(ym, y.at[_rows(c * PIECE, PIECE)], yb_out, yb_in.at[c], {"sp": 2})

    def seen(i):
        return remote(a_loc.at[_rows(theirs + i * BQ, BQ)], a_far.at[pl.ds(i * BQ, BQ)], seen_out.at[i], seen_in.at[i], partner)

    def seen_more():
        rows = a_loc.at[_rows(jnp.where(early, CHIP + (1 - core) * PIECE, ROWS), PIECE)]
        return remote(rows, a_far.at[pl.ds(ROWS, PIECE)], seen_out.at[2], seen_in.at[2], partner)

    def x_share():
        return remote(xbuf.at[pl.ds(0, PIECE)], xm, xb_out.at[0], xb_in, {"sp": 2})

    def y_share(n):
        here = _rows(n * COLS, COLS)
        return remote(ym.at[:, here], y.at[pl.ds(0, PIECE), here], share_out.at[n], share_in.at[n], {"sp": 3})

    barrier = pltpu.get_barrier_semaphore()
    for other in range(1, 4):
        pl.semaphore_signal(barrier, inc=1, device_id={"sp": lax.rem(sp + other, 4)}, device_id_type=MESH)

    gain_copy = pltpu.make_async_copy(gain, gains, gain_sem)
    gain_copy.start()
    for r in range(4):
        x_copy(r).start()
    factor_copy = pltpu.make_async_copy(table, factors, tab_sem)
    factor_copy.start()
    w_copy(wk, 0, core * kv_cols, 0).start()

    gain_copy.wait()
    for r in range(4):
        x_copy(r).wait()
        if r == 1:
            w_copy(wk, 0, core * kv_cols + COLS, 1).start()
        wide = xbuf[r * PIECE : (r + 1) * PIECE, :].astype(jnp.float32)
        scale = lax.rsqrt(jnp.mean(wide * wide, -1, keepdims=True) + 1e-6)
        a_loc[_rows(mine + r * PIECE, PIECE), :] = (wide * scale * gains[...].astype(jnp.float32)[None, :]).astype(a_loc.dtype)

    pl.semaphore_wait(barrier, 3)
    for r in range(4):
        pl.when(early)(far(r).start)
        swap(r).start()
        if r < 2:
            pl.when(giver)(back(r).start)
    pl.when(sp == 3)(x_share().start)

    @pl.when(giver)
    def _():
        for c in range(2):
            x_back(c).start()

    factor_copy.wait()
    near_same, near_other = factors[2 * FAR : 2 * FAR + NEAR, :], factors[2 * FAR + NEAR :, :]
    for n in range(FAR):
        tab[n * NEAR : (n + 1) * NEAR, :] = factors[n : n + 1, :] * near_same + factors[FAR + n : FAR + n + 1, :] * near_other

    def turned(t, *places):
        rows = t.shape[0] // len(places)
        both = jnp.concatenate([tab[_rows(place, rows), :] for place in places], axis=0)
        back = pltpu.roll(both, HEAD // 2, 1)
        first = lax.broadcasted_iota(jnp.int32, both.shape, 1) < HEAD // 2
        cos, sin = jnp.where(first, both, back), jnp.where(first, -back, both)
        t = t.astype(q.dtype).astype(jnp.float32)
        for h in range(COLS // HEAD):
            part = t[:, h * HEAD : (h + 1) * HEAD]
            yield h, (part * cos + pltpu.roll(part, HEAD // 2, 1) * sin).astype(q.dtype)

    def project(a, row, slot, rows=BQ):
        return jnp.dot(a[_rows(row, rows), :], wbuf[slot], preferred_element_type=jnp.float32)

    def project_q(c, row):
        for h, t in turned(project(a_loc, row, q_slot(c)), chip * CHIP + row):
            q[lax.rem(c, 4) * 4 + h, _rows(row, BQ), :] = t

    def project_k(c, a, row, key, *places):
        for h, t in turned(project(a, row, c), *places):
            k[c * 4 + h, _rows(key, BQ), :] = t

    def project_v(c, a, row, key):
        t = project(a, row, 2 + c).astype(v.dtype)
        for h in range(COLS // HEAD):
            v[c * 4 + h, :, _rows(key, BQ)] = t[:, h * HEAD : (h + 1) * HEAD].T

    w_wait(0)
    for c in range(2):
        w_copy(wv, 0, core * kv_cols + c * COLS, 2 + c).start()

    for part, start in enumerate((mine, theirs)):
        if part:
            for r in range(4):
                swap(r).wait_recv()
        rows = [start + b * BQ for b in range(2)]
        for c in range(2):
            if c and not part:
                w_wait(1)
            for row in rows:
                project_k(c, a_loc, row, row, chip * CHIP + row)
        if not part:
            for c in range(2):
                w_wait(2 + c)
            for c in range(4):
                q_copy(c).start()
        for c in range(2):
            for row in rows:
                project_v(c, a_loc, row, row)

    def local_q(i, _):
        c = 2 * i
        for n in range(2):
            w_wait(q_slot(c + n))

        @pl.when(early)
        def _():
            for n in range(2):
                for b in range(CHIP // BQ):
                    project_q(c + n, b * BQ)

        @pl.when(late)
        def _():
            for n in range(2):
                for b in range(1, CHIP // BQ):
                    project_q(c + n, b * BQ)

        @pl.when(early)
        def _():
            for n in range(2):
                q_copy(c + 4 + n).start()

        @pl.when((i == 0) & (sp == 0))
        def _():
            for r in range(2):
                back(r).wait_recv()
                hand_moved(r).start()

    lax.fori_loop(0, 2, local_q, None)

    @pl.when(early)
    def _():
        @pl.when(core == 1)
        def _():
            for r in range(2):
                hand_moved(r).wait_recv()

        def moved_q(c, _):
            w_wait(q_slot(c))
            project_q(c, CHIP)

        lax.fori_loop(4, 8, moved_q, None)
        for c in range(2):
            project_k(c, a_loc, CHIP, CHIP, CHIP)
            project_v(c, a_loc, CHIP, CHIP)
        for u in range(4, 8):
            o_copy(u).start()

    for u in range(4):
        o_copy(u).start()

    e = HEAD**-0.5 * LOG2E
    cols = GROUP * BQ

    def block(iq, state, at, size, ahead=None):
        here, queries = _rows(at, size), _rows(iq * BQ, BQ)
        ones = jnp.ones((8, size), v.dtype)
        begin = ahead is not None
        if begin:
            ok = (lax.broadcasted_iota(jnp.int32, (1, cols), 1) & (BQ - 1)) + ahead >= lax.broadcasted_iota(jnp.int32, (size, 1), 0)

        def scores(h):
            return _dot(k[h, here, :], q[GROUP * h : GROUP * (h + 1), queries, :].reshape(cols, HEAD), 1, 1)

        def weights(h, s):
            if begin:
                s = jnp.where(ok, s, HIDDEN)
                new, keep = s.max(axis=0, keepdims=True), None
            else:
                old = top[state, h : h + 1, :]
                new = jnp.maximum(old, s.max(axis=0, keepdims=True))
                keep = jnp.exp2((old - new) * e)
            top[state, h : h + 1, :] = new
            return jnp.exp2((s - new) * e).astype(v.dtype), keep

        def add(h, p, keep):
            got = _dot(jnp.concatenate([v[h, :, here], ones], axis=0), p, 1, 0)
            mix[state, h] = got if begin else mix[state, h] * keep + got

        ready_s, ready_p = [scores(0), scores(1)], []
        for h in range(KV):
            if h + 2 < KV:
                ready_s.append(scores(h + 2))
            ready_p.append(weights(h, ready_s[h]))
            if h:
                add(h - 1, *ready_p[h - 1])
        add(KV - 1, *ready_p[-1])

    def finish(iq, state):
        for h in range(KV):
            out = (mix[state, h, :HEAD, :] * (1 / mix[state, h, HEAD : HEAD + 1, :])).astype(a_loc.dtype).T
            for n in range(GROUP):
                a_loc[_rows(iq * BQ, BQ), (GROUP * h + n) * HEAD : (GROUP * h + n + 1) * HEAD] = out[n * BQ : (n + 1) * BQ, :]

    def hand_on(r):
        @pl.when(late)
        def _():
            far(r).wait_recv()
            hand(r).start()

    def moved_output():
        seen_more().wait_recv()
        x_back(0).wait_recv()

        def output(n, _):
            u = 2 * n
            for i in range(2):
                w_wait(o_slot(u + i))
            t = project(a_loc, CHIP + core * PIECE, o_slot(u), PIECE) + project(a_far, ROWS, o_slot(u + 1), PIECE)
            here = _rows(n * COLS, COLS)
            ym[:, here] = (xm[:, here].astype(jnp.float32) + t).astype(ym.dtype)
            for i in range(2):
                o_copy(u + i + SLOTS).start()

        lax.fori_loop(0, 4, output, None)

    hand_on(0)

    def far_project(half, iq, state):
        def part(i, _):
            r = 2 * half + i
            for at in range(4):
                pl.when(r == at)(hand(at).wait_recv)
            row = 2 * r * PIECE
            for n in range(2):
                project_k(n, a_far, row, CHIP + row, r * PIECE, ROWS + r * PIECE)
                project_v(n, a_far, row, CHIP + row)
            pl.when(r == 2)(lambda: hand_on(3))
            pl.when(half == 1)(lambda: block(iq, state, CHIP + row, BQ))

        lax.fori_loop(0, 2, part, None)

    def step(s, _):
        far_step = late & (s >= 3)
        half, i = lax.div(s, 3) - 1, lax.rem(s, 3)
        iq_early = jnp.where(s == 0, 4, lax.rem((1 - core) * 2 + s + 3, 4))
        iq_late = jnp.where(s < 3, s + 1, 1 + lax.rem(i + 1 - core, 3))
        iq = jnp.where(early, iq_early, iq_late)
        state = jnp.where(early, 0, iq - 1)
        p = lax.div(iq, 2)

        pl.when(far_step & (i == 0))(lambda: far_project(half, iq, state))

        @pl.when(late & (s == 6))
        def _():
            for r in range(4):
                hand(r).wait_send()
            pl.semaphore_signal(ready, inc=1, device_id=partner, device_id_type=MESH)
            for u in range(4, 8):
                o_copy(u).start()

        @pl.when((late & (s == 6)) | (early & (s == 3)))
        def _():
            for r in range(4):
                swap(r).wait_send()
                pl.when(early)(far(r).wait_send)

        @pl.when(late & (s == 7))
        def _():
            pl.semaphore_wait(ready, 1)
            pl.when(core == 0)(seen(0).start)
            pl.when(core == 1)(seen(1).start)

        @pl.when(late & (s == 8))
        def _():
            pl.when(core == 0)(seen(1).start)
            pl.when(core == 1)(seen_more().start)

        even = lax.rem(iq, 2) == 0
        pl.when(jnp.logical_not(far_step) & even)(lambda: block(iq, state, p * BK, BQ, 0))
        pl.when(jnp.logical_not(far_step) & jnp.logical_not(even))(lambda: block(iq, state, p * BK, BK, BQ))

        @pl.when(early)
        def _():
            pl.when(s == 1)(seen_more().start)
            pl.when(s == 2)(seen(0).start)
            pl.when(s == 3)(seen(1).start)

        start = jnp.where(far_step, CHIP + half * BK, 0)
        lax.fori_loop(0, jnp.where(far_step, jnp.where(s == 6, 0, 1), p), lambda j, _: block(iq, state, start + j * BK, BK), None)

        @pl.when((s == 0) & (sp == 0))
        def _():
            for r in range(2):
                hand_moved(r).wait_send()

        pl.when(early | (s >= 6))(lambda: finish(iq, state))

        @pl.when(early)
        def _():
            pl.when(s == 1 + core)(moved_output)
            pl.when(s == 2 + core)(y_back(core).start)

        for at, r in ((1, 1), (3, 2)):
            pl.when(s == at)(functools.partial(hand_on, r))

    lax.fori_loop(0, jnp.where(early, 5, 9), step, None)

    pl.when(sp != 2)(seen(0).wait_recv)
    seen(1).wait_recv()

    @pl.when(sp == 2)
    def _():
        seen_more().wait_recv()
        x_share().wait_recv()

    begin = jnp.where(early, 8, 0)

    def output(n, _):
        u = begin + 2 * n
        for i in range(2):
            w_wait(o_slot(u + i))
        here = _rows(n * COLS, COLS)

        def both(own, other, rows):
            return project(a_loc, own, o_slot(u), rows) + project(a_far, other, o_slot(u + 1), rows)

        def part(row, rows):
            which = pl.ds(row, rows)
            y[which, here] = (xbuf[which, here].astype(jnp.float32) + both(mine + row, row, rows)).astype(y.dtype)

        @pl.when(early)
        def _():
            part(0, BQ)
            part(BQ, BQ)

        @pl.when(sp == 3)
        def _():
            part(PIECE, PIECE)
            part(BQ, BQ)

        def share():
            ym[:, here] = (xm[:, here].astype(jnp.float32) + both(ROWS, ROWS, PIECE)).astype(ym.dtype)

        @pl.when((sp == 2) & (n < 3))
        def _():
            share()
            part(BQ, BQ)
            y_share(n).start()

        @pl.when((sp == 2) & (n == 3))
        def _():
            share()
            y_share(n).start()
            part(BQ, BQ)

    lax.fori_loop(0, 4, output, None)
    pl.when(sp != 3)(seen(0).wait_send)
    seen(1).wait_send()
    pl.when(sp != 2)(seen_more().wait_send)
    pl.when(early)(y_back(core).wait_send)

    @pl.when(giver)
    def _():
        for c in range(2):
            back(c).wait_send()
            x_back(c).wait_send()
            y_back(c).wait_recv()
        for n in range(4):
            y_share(n).wait_send()

    @pl.when(sp == 3)
    def _():
        x_share().wait_send()
        for n in range(4):
            y_share(n).wait_recv()


def rotary():
    half = HEAD // 2
    speed = np.float64(THETA) ** (-np.arange(half) / half)
    far, near = (np.arange(n)[:, None] * step * speed for n, step in ((FAR, NEAR), (NEAR, 1)))
    rows = ((np.cos(far), np.sin(far)), (np.sin(far), np.cos(far)), (np.cos(near), np.cos(near)), (-np.sin(near), np.sin(near)))
    return np.concatenate([np.concatenate(row, -1) for row in rows]).astype(np.float32)


def solution(mesh):
    def step(x, gain, wq, wk, wv, wo):
        bf, f32 = jnp.bfloat16, jnp.float32
        dma = pltpu.SemaphoreType.DMA
        hbm = pl.BlockSpec(memory_space=pl.ANY)
        return pl.pallas_call(
            _kernel,
            out_shape=pltpu.VMEM(x.shape, x.dtype),
            in_specs=[hbm] * 7,
            out_specs=pl.BlockSpec(memory_space=pltpu.VMEM),
            scratch_shapes=[
                pltpu.VMEM((CHIP + MOVED, DEPTH), bf),
                pltpu.VMEM((CHIP, DEPTH), bf),
                pltpu.VMEM((GROUP * KV, CHIP + MOVED, HEAD), bf),
                pltpu.VMEM((KV, 2 * CHIP, HEAD), bf),
                pltpu.VMEM((KV, HEAD, 2 * CHIP), bf),
                pltpu.VMEM((3, KV, GROUP * BQ), f32),
                pltpu.VMEM((3, KV, HEAD + 8, GROUP * BQ), f32),
                pltpu.VMEM((SLOTS, DEPTH, COLS), bf),
                pltpu.VMEM((ROWS, DEPTH), bf),
                pltpu.VMEM((2 * CHIP, HEAD), f32),
                pltpu.VMEM((2 * FAR + 2 * NEAR, HEAD), f32),
                pltpu.VMEM((DEPTH,), bf),
                pltpu.VMEM((PIECE, DEPTH), bf),
                pltpu.VMEM((PIECE, DEPTH), bf),
                dma((4,)), dma, dma, dma((SLOTS,)),
                *[dma((4,))] * 6, dma((3,)), dma((3,)),
                dma((2,)), dma((2,)), dma((2,)), dma, dma, dma((2,)), dma((4,)), dma((4,)),
                pltpu.SemaphoreType.REGULAR,
            ],
            compiler_params=pltpu.CompilerParams(collective_id=0, has_side_effects=True, vmem_limit_bytes=VMEM),
            name="layer",
        )(x, gain, jnp.asarray(rotary()), wq, wk, wv, wo)

    tokens, whole = P(("dp", "sp"), None), P(None, None)
    return jax.shard_map(
        step,
        mesh=mesh,
        in_specs=(tokens, P(None), whole, whole, whole, whole),
        out_specs=tokens,
        check_vma=False,
    )
```
